128 devices in a mesh: rep: 2 (over core), fsdp: 64 (over z, y, x).
Axes of the slice: x: 4, y: 4, z: 4, core: 2. Of those that a mesh axis runs over, the one named last changes fastest.
Arguments:
- x_tokens: bfloat16 [768, 197, 1024], P(('rep', 'fsdp'))
- grad_z: bfloat16 [768, 197, 1024], P(('rep', 'fsdp'))
- w_qkv: float32 [1024, 3072], P('fsdp')
- b_qkv: float32 [3072], P('fsdp')
- w_out: float32 [1024, 1024], P('fsdp')
- w_up: float32 [1024, 4096], P('fsdp')
- b_up: float32 [4096], P('fsdp')
- w_down: float32 [4096, 1024], P('fsdp')
- vec_params: float32 [8, 1024], P(None, 'fsdp')
Outputs:
- output 1: bfloat16 [768, 197, 1024], P(('rep', 'fsdp'))
- output 2: bfloat16 [768, 197, 1024], P(('rep', 'fsdp'))
- output 3: float32 [1024, 3072], P('fsdp')
- output 4: float32 [3072], P('fsdp')
- output 5: float32 [1024, 1024], P('fsdp')
- output 6: float32 [1024, 4096], P('fsdp')
- output 7: float32 [4096], P('fsdp')
- output 8: float32 [4096, 1024], P('fsdp')
- output 9: float32 [8, 1024], P(None, 'fsdp')
All inputs are finite; a program needn't handle non-finite values.
Results may differ from the reference program's by a relative error of at most 0.02.
Values are sent between devices in bfloat16 or wider.
A program may use at most 1 GiB of HBM per device.

```python
import jax
import jax.numpy as jnp
from jax import lax

D = 1024
FF = 4096
SEQ = 197
HEADS = 16
SEQS_DEV = 6
DEVICES = 128
BATCH = SEQS_DEV * DEVICES
HEAD = D // HEADS
LN_EPS = 1e-5


def setup_inputs(seed: int = 0) -> dict:
    keys = jax.random.split(jax.random.key(seed), 12)
    seq_scale = jax.random.uniform(keys[0], (BATCH, 1, 1), minval=0.5, maxval=2.0)
    x_tokens = (jax.random.normal(keys[1], (BATCH, SEQ, D)) * seq_scale).astype(jnp.bfloat16)
    grad_scale = jax.random.uniform(keys[2], (BATCH, 1, 1), minval=0.25, maxval=2.0)
    grad_z = (jax.random.normal(keys[3], (BATCH, SEQ, D)) * grad_scale).astype(jnp.bfloat16)
    w_qkv = jax.random.normal(keys[4], (D, 3 * D)) * D ** -0.5
    b_qkv = 0.5 * jax.random.normal(keys[5], (3 * D,))
    w_out = jax.random.normal(keys[6], (D, D)) * D ** -0.5
    w_up = jax.random.normal(keys[7], (D, FF)) * D ** -0.5
    b_up = 0.5 * jax.random.normal(keys[8], (FF,))
    w_down = jax.random.normal(keys[9], (FF, D)) * FF ** -0.5
    is_scale = jnp.array([0.0, 0.0, 0.0, 1.0, 0.0, 0.0, 0.0, 1.0], jnp.float32)[:, None]
    row_offset = jnp.array([1.0, 0.0, 0.0, 0.0, 1.0, 0.0, 0.0, 0.0], jnp.float32)[:, None]
    normal_rows = row_offset + 0.25 * jax.random.normal(keys[10], (8, D))
    scale_rows = jax.random.uniform(keys[11], (8, D), minval=0.5, maxval=1.5)
    vec_params = is_scale * scale_rows + (1.0 - is_scale) * normal_rows
    return {"x_tokens": x_tokens, "grad_z": grad_z, "w_qkv": w_qkv, "b_qkv": b_qkv, "w_out": w_out,
            "w_up": w_up, "b_up": b_up, "w_down": w_down, "vec_params": vec_params}


def normalize(t):
    mean = jnp.mean(t, axis=-1, keepdims=True)
    centered = t - mean
    variance = jnp.mean(centered * centered, axis=-1, keepdims=True)
    return centered * lax.rsqrt(variance + LN_EPS)


def gelu_exact(t):
    return jax.nn.gelu(t, approximate=False)


def layer_pass(x_seq, dz_seq, matrices, bias_qkv, bias_up, vec_rows):
    w_qkv, w_out, w_up, w_down = matrices
    ln1_gain, ln1_bias, out_bias, scale_attn, ln2_gain, ln2_bias, down_bias, scale_mlp = vec_rows
    score_scale = HEAD ** -0.5
    x_float = x_seq.astype(jnp.float32)
    xhat_one, norm_one_back = jax.vjp(normalize, x_float)
    h_one = (xhat_one * ln1_gain + ln1_bias).astype(jnp.bfloat16)
    qkv_proj = (jnp.dot(h_one, w_qkv, preferred_element_type=jnp.float32) + bias_qkv).astype(jnp.bfloat16)
    qkv_heads = qkv_proj.reshape(SEQ, 3, HEADS, HEAD).astype(jnp.float32)
    q_heads = qkv_heads[:, 0]
    k_heads = qkv_heads[:, 1]
    v_heads = qkv_heads[:, 2]
    scores = jnp.einsum("qhe,khe->hqk", q_heads, k_heads) * score_scale
    attn_probs = jax.nn.softmax(scores, axis=-1)
    probs_bf = attn_probs.astype(jnp.bfloat16).astype(jnp.float32)
    head_out = jnp.einsum("hqk,khe->qhe", probs_bf, v_heads).astype(jnp.bfloat16).reshape(SEQ, D)
    att_out = jnp.dot(head_out, w_out, preferred_element_type=jnp.float32) + out_bias
    resid_mid = x_float + scale_attn * att_out
    xhat_two, norm_two_back = jax.vjp(normalize, resid_mid)
    h_two = (xhat_two * ln2_gain + ln2_bias).astype(jnp.bfloat16)
    pre_act = jnp.dot(h_two, w_up, preferred_element_type=jnp.float32) + bias_up
    act_float, gelu_back = jax.vjp(gelu_exact, pre_act)
    mlp_act = act_float.astype(jnp.bfloat16)
    mlp_out = jnp.dot(mlp_act, w_down, preferred_element_type=jnp.float32) + down_bias
    z_seq = (resid_mid + scale_mlp * mlp_out).astype(jnp.bfloat16)
    g_out = dz_seq.astype(jnp.float32)
    grad_scale_mlp = jnp.sum(g_out * mlp_out, axis=0)
    d_mlp = g_out * scale_mlp
    grad_down_bias = jnp.sum(d_mlp, axis=0)
    d_mlp_bf = d_mlp.astype(jnp.bfloat16)
    grad_w_down = jnp.dot(mlp_act.T, d_mlp_bf, preferred_element_type=jnp.float32)
    d_act = jnp.dot(d_mlp_bf, w_down.T, preferred_element_type=jnp.float32)
    d_pre = gelu_back(d_act)[0]
    grad_b_up = jnp.sum(d_pre, axis=0)
    d_pre_bf = d_pre.astype(jnp.bfloat16)
    grad_w_up = jnp.dot(h_two.T, d_pre_bf, preferred_element_type=jnp.float32)
    d_h_two = jnp.dot(d_pre_bf, w_up.T, preferred_element_type=jnp.float32)
    grad_ln2_gain = jnp.sum(d_h_two * xhat_two, axis=0)
    grad_ln2_bias = jnp.sum(d_h_two, axis=0)
    g_resid = g_out + norm_two_back(d_h_two * ln2_gain)[0]
    grad_scale_attn = jnp.sum(g_resid * att_out, axis=0)
    d_att = g_resid * scale_attn
    grad_out_bias = jnp.sum(d_att, axis=0)
    d_att_bf = d_att.astype(jnp.bfloat16)
    grad_w_out = jnp.dot(head_out.T, d_att_bf, preferred_element_type=jnp.float32)
    d_heads = jnp.dot(d_att_bf, w_out.T, preferred_element_type=jnp.float32).astype(jnp.bfloat16)
    d_heads = d_heads.reshape(SEQ, HEADS, HEAD).astype(jnp.float32)
    d_probs = jnp.einsum("qhe,khe->hqk", d_heads, v_heads)
    grad_v = jnp.einsum("hqk,qhe->khe", probs_bf, d_heads)
    d_scores = attn_probs * (d_probs - jnp.sum(d_probs * attn_probs, axis=-1, keepdims=True))
    d_scores_bf = (d_scores * score_scale).astype(jnp.bfloat16).astype(jnp.float32)
    grad_q = jnp.einsum("hqk,khe->qhe", d_scores_bf, k_heads)
    grad_k = jnp.einsum("hqk,qhe->khe", d_scores_bf, q_heads)
    d_qkv = jnp.stack([grad_q, grad_k, grad_v], axis=1).reshape(SEQ, 3 * D)
    grad_b_qkv = jnp.sum(d_qkv, axis=0)
    d_qkv_bf = d_qkv.astype(jnp.bfloat16)
    grad_w_qkv = jnp.dot(h_one.T, d_qkv_bf, preferred_element_type=jnp.float32)
    d_h_one = jnp.dot(d_qkv_bf, w_qkv.T, preferred_element_type=jnp.float32)
    grad_ln1_gain = jnp.sum(d_h_one * xhat_one, axis=0)
    grad_ln1_bias = jnp.sum(d_h_one, axis=0)
    dx_seq = (g_resid + norm_one_back(d_h_one * ln1_gain)[0]).astype(jnp.bfloat16)
    grad_vec = jnp.stack([grad_ln1_gain, grad_ln1_bias, grad_out_bias, grad_scale_attn,
                          grad_ln2_gain, grad_ln2_bias, grad_down_bias, grad_scale_mlp])
    return z_seq, dx_seq, (grad_w_qkv, grad_b_qkv, grad_w_out, grad_w_up, grad_b_up, grad_w_down, grad_vec)


def reference(x_tokens, grad_z, w_qkv, b_qkv, w_out, w_up, b_up, w_down, vec_params):
    matrices = (w_qkv.astype(jnp.bfloat16), w_out.astype(jnp.bfloat16),
                w_up.astype(jnp.bfloat16), w_down.astype(jnp.bfloat16))
    bias_qkv = b_qkv.astype(jnp.bfloat16).astype(jnp.float32)
    bias_up = b_up.astype(jnp.bfloat16).astype(jnp.float32)
    vec_rows = vec_params.astype(jnp.bfloat16).astype(jnp.float32)

    def step(running, pair):
        z_seq, dx_seq, seq_grads = layer_pass(pair[0], pair[1], matrices, bias_qkv, bias_up, vec_rows)
        return jax.tree.map(jnp.add, running, seq_grads), (z_seq, dx_seq)

    zero_grads = (jnp.zeros((D, 3 * D), jnp.float32), jnp.zeros((3 * D,), jnp.float32),
                  jnp.zeros((D, D), jnp.float32), jnp.zeros((D, FF), jnp.float32),
                  jnp.zeros((FF,), jnp.float32), jnp.zeros((FF, D), jnp.float32),
                  jnp.zeros((8, D), jnp.float32))
    totals, seq_outs = lax.scan(step, zero_grads, (x_tokens, grad_z))
    grad_w_qkv, grad_b_qkv, grad_w_out, grad_w_up, grad_b_up, grad_w_down, grad_vec = totals
    return (seq_outs[0], seq_outs[1], grad_w_qkv, grad_b_qkv, grad_w_out, grad_w_up, grad_b_up,
            grad_w_down, grad_vec)
```

```python
import jax
import jax.numpy as jnp
from jax import lax
from jax.experimental import pallas as pl
from jax.experimental.pallas import tpu as pltpu
from jax.sharding import PartitionSpec as P

HEADS = 16
LN_EPS = 1e-5


def normalize(t):
    mean = jnp.mean(t, axis=-1, keepdims=True)
    centered = t - mean
    variance = jnp.mean(centered * centered, axis=-1, keepdims=True)
    return centered * lax.rsqrt(variance + LN_EPS)


def gelu_exact(t):
    return jax.nn.gelu(t, approximate=False)


def layer_forward(x_loc, weights):
    w_qkv, b_qkv, w_out, w_up, b_up, w_down, vec_rows = weights
    ln1_gain, ln1_bias, out_bias, scale_attn, ln2_gain, ln2_bias, down_bias, scale_mlp = vec_rows
    num_seqs, tokens, width = x_loc.shape
    head_dim = width // HEADS
    score_scale = head_dim ** -0.5
    x_float = x_loc.astype(jnp.float32)
    h_one = (normalize(x_float) * ln1_gain + ln1_bias).astype(jnp.bfloat16)
    qkv_proj = jnp.einsum("std,de->ste", h_one, w_qkv, preferred_element_type=jnp.float32) + b_qkv
    qkv_heads = qkv_proj.astype(jnp.bfloat16).reshape(num_seqs, tokens, 3, HEADS, head_dim)
    q_heads = qkv_heads[:, :, 0]
    k_heads = qkv_heads[:, :, 1]
    v_heads = qkv_heads[:, :, 2]
    scores = jnp.einsum("sqhe,skhe->shqk", q_heads, k_heads, preferred_element_type=jnp.float32) * score_scale
    attn_probs = jax.nn.softmax(scores, axis=-1)
    probs_bf = attn_probs.astype(jnp.bfloat16)
    head_out = jnp.einsum("shqk,skhe->sqhe", probs_bf, v_heads, preferred_element_type=jnp.float32)
    head_out = head_out.astype(jnp.bfloat16).reshape(num_seqs, tokens, width)
    att_out = jnp.einsum("std,de->ste", head_out, w_out, preferred_element_type=jnp.float32) + out_bias
    resid_mid = x_float + scale_attn * att_out
    h_two = (normalize(resid_mid) * ln2_gain + ln2_bias).astype(jnp.bfloat16)
    pre_act = jnp.einsum("std,df->stf", h_two, w_up, preferred_element_type=jnp.float32) + b_up
    mlp_act = gelu_exact(pre_act).astype(jnp.bfloat16)
    mlp_out = jnp.einsum("stf,fd->std", mlp_act, w_down, preferred_element_type=jnp.float32) + down_bias
    z_loc = (resid_mid + scale_mlp * mlp_out).astype(jnp.bfloat16)
    saved = (h_one, qkv_heads, attn_probs, probs_bf, head_out, att_out, resid_mid, h_two, pre_act, mlp_act, mlp_out)
    return z_loc, saved


def layer_backward(x_loc, dz_loc, saved, weights):
    w_qkv, b_qkv, w_out, w_up, b_up, w_down, vec_rows = weights
    ln1_gain, ln1_bias, out_bias, scale_attn, ln2_gain, ln2_bias, down_bias, scale_mlp = vec_rows
    h_one, qkv_heads, attn_probs, probs_bf, head_out, att_out, resid_mid, h_two, pre_act, mlp_act, mlp_out = saved
    num_seqs, tokens, width = x_loc.shape
    head_dim = width // HEADS
    score_scale = head_dim ** -0.5
    g_out = dz_loc.astype(jnp.float32)
    grad_scale_mlp = jnp.sum(g_out * mlp_out, axis=(0, 1))
    d_mlp = g_out * scale_mlp
    grad_down_bias = jnp.sum(d_mlp, axis=(0, 1))
    d_mlp_bf = d_mlp.astype(jnp.bfloat16)
    grad_w_down = jnp.einsum("stf,std->fd", mlp_act, d_mlp_bf, preferred_element_type=jnp.float32)
    d_act = jnp.einsum("std,fd->stf", d_mlp_bf, w_down, preferred_element_type=jnp.float32)
    d_pre = jax.vjp(gelu_exact, pre_act)[1](d_act)[0]
    grad_b_up = jnp.sum(d_pre, axis=(0, 1))
    d_pre_bf = d_pre.astype(jnp.bfloat16)
    grad_w_up = jnp.einsum("std,stf->df", h_two, d_pre_bf, preferred_element_type=jnp.float32)
    d_h_two = jnp.einsum("stf,df->std", d_pre_bf, w_up, preferred_element_type=jnp.float32)
    array_b8, norm_two_back = jax.vjp(normalize, resid_mid)
    grad_ln2_gain = jnp.sum(d_h_two * array_b8, axis=(0, 1))
    grad_ln2_bias = jnp.sum(d_h_two, axis=(0, 1))
    g_resid = g_out + norm_two_back(d_h_two * ln2_gain)[0]
    grad_scale_attn = jnp.sum(g_resid * att_out, axis=(0, 1))
    d_att = g_resid * scale_attn
    grad_out_bias = jnp.sum(d_att, axis=(0, 1))
    d_att_bf = d_att.astype(jnp.bfloat16)
    grad_w_out = jnp.einsum("std,ste->de", head_out, d_att_bf, preferred_element_type=jnp.float32)
    d_heads = jnp.einsum("ste,de->std", d_att_bf, w_out, preferred_element_type=jnp.float32)
    d_heads = d_heads.astype(jnp.bfloat16).reshape(num_seqs, tokens, HEADS, head_dim)
    q_heads = qkv_heads[:, :, 0]
    k_heads = qkv_heads[:, :, 1]
    v_heads = qkv_heads[:, :, 2]
    d_probs = jnp.einsum("sqhe,skhe->shqk", d_heads, v_heads, preferred_element_type=jnp.float32)
    grad_v = jnp.einsum("shqk,sqhe->skhe", probs_bf, d_heads, preferred_element_type=jnp.float32)
    d_scores = attn_probs * (d_probs - jnp.sum(d_probs * attn_probs, axis=-1, keepdims=True))
    d_scores_bf = (d_scores * score_scale).astype(jnp.bfloat16)
    grad_q = jnp.einsum("shqk,skhe->sqhe", d_scores_bf, k_heads, preferred_element_type=jnp.float32)
    grad_k = jnp.einsum("shqk,sqhe->skhe", d_scores_bf, q_heads, preferred_element_type=jnp.float32)
    d_qkv = jnp.stack([grad_q, grad_k, grad_v], axis=2).reshape(num_seqs, tokens, 3 * width)
    grad_b_qkv = jnp.sum(d_qkv, axis=(0, 1))
    d_qkv_bf = d_qkv.astype(jnp.bfloat16)
    grad_w_qkv = jnp.einsum("std,ste->de", h_one, d_qkv_bf, preferred_element_type=jnp.float32)
    d_h_one = jnp.einsum("ste,de->std", d_qkv_bf, w_qkv, preferred_element_type=jnp.float32)
    value_a8, norm_one_back = jax.vjp(normalize, x_loc.astype(jnp.float32))
    grad_ln1_gain = jnp.sum(d_h_one * value_a8, axis=(0, 1))
    grad_ln1_bias = jnp.sum(d_h_one, axis=(0, 1))
    dx_loc = (g_resid + norm_one_back(d_h_one * ln1_gain)[0]).astype(jnp.bfloat16)
    grad_vec = jnp.stack([grad_ln1_gain, grad_ln1_bias, grad_out_bias, grad_scale_attn,
                          grad_ln2_gain, grad_ln2_bias, grad_down_bias, grad_scale_mlp])
    return dx_loc, (grad_w_qkv, grad_b_qkv, grad_w_out, grad_w_up, grad_b_up, grad_w_down, grad_vec)


MESH_ID = pl.DeviceIdType.MESH
ORDERS = ((2, 1, 0), (1, 0, 2), (0, 2, 1))
PIECE = 512


def my_place():
    rep = lax.axis_index("rep")
    flat = lax.axis_index("fsdp")
    return rep, (flat // 16, (flat // 4) % 4, flat % 4)


def along(place, dim, shift):
    moved = list(place)
    moved[dim] = (place[dim] + shift) % 4
    return tuple(moved)


def flat_of(place):
    return place[0] * 16 + place[1] * 4 + place[2]


def entry_barrier(rep, place):
    barrier = pltpu.get_barrier_semaphore()
    for dim in range(3):
        for shift in (1, 3):
            pl.semaphore_signal(barrier, inc=1, device_id=(rep, flat_of(along(place, dim, shift))),
                                device_id_type=MESH_ID)
    pl.semaphore_signal(barrier, inc=1, device_id=(1 - rep, flat_of(place)), device_id_type=MESH_ID)
    pl.semaphore_wait(barrier, 7)


def spot(place, order, upto, dim_index):
    index = [None, None, None]
    for k, dim in enumerate(order):
        index[dim] = slice(None) if k < upto else (dim_index if k == upto else place[dim])
    return tuple(index)


def gather_kernel(*refs):
    n_in, n_out = 5, 5
    shards, fulls = refs[:n_in], refs[n_in:n_in + n_out]
    own_sem, send_sem, recv_sem, pair_send, pair_recv = refs[n_in + n_out:]
    rep, place = my_place()
    entry_barrier(rep, place)
    lanes = []
    for item, (which, row, cols, base, order) in enumerate(gather_items()):
        lanes.append((item, which, row, cols, base, order))

    def window(which, row, cols, base, core):
        col = pl.multiple_of(core * base[0] + base[1], 128)
        return pl.ds(row, 16), pl.ds(col, cols)

    copies = {}

    def put(item, slot, src, dst, dim, shift):
        copy = pltpu.make_async_remote_copy(
            src_ref=src, dst_ref=dst, send_sem=send_sem.at[item, slot], recv_sem=recv_sem.at[item, slot],
            device_id=(rep, flat_of(along(place, dim, shift))), device_id_type=MESH_ID)
        copy.start()
        copies[item, slot] = copy

    def step(lane, level):
        item, which, row, cols, base, order = lane
        rows, columns = window(which, row, cols, base, rep)
        full = fulls[which]
        if level == 0:
            copies[item, "own"] = pltpu.make_async_copy(
                shards[which].at[rows, columns], full.at[place + (rows, columns)], own_sem.at[item])
            copies[item, "own"].start()
            for slot, shift in ((0, 1), (1, 3)):
                put(item, slot, shards[which].at[rows, columns], full.at[place + (rows, columns)], order[0], shift)
            return
        if level == 6:
            copies[item, 10].wait_recv()
            copies[item, 11].wait_recv()
            copy = pltpu.make_async_remote_copy(
                src_ref=full.at[:, :, :, rows, columns], dst_ref=full.at[:, :, :, rows, columns],
                send_sem=pair_send.at[item], recv_sem=pair_recv.at[item],
                device_id=(1 - rep, flat_of(place)), device_id_type=MESH_ID)
            copy.start()
            copies[item, "pair"] = copy
            return
        phase, second = level // 2, level % 2
        dim = order[phase]
        if second:
            for slot, shift, half in ((0, 1, 0), (1, 3, 8)):
                copies[item, 4 * phase + slot].wait_recv()
                from_index = (place[dim] + (4 - shift)) % 4
                where = spot(place, order, phase, from_index) + (pl.ds(row + half, 8), columns)
                put(item, 4 * phase + 2 + slot, full.at[where], full.at[where], dim, shift)
        else:
            if phase == 1:
                copies[item, "own"].wait()
            for slot in (2, 3):
                copies[item, 4 * (phase - 1) + slot].wait_recv()
            where = spot(place, order, phase, place[dim]) + (rows, columns)
            for slot, shift in ((0, 1), (1, 3)):
                put(item, 4 * phase + slot, full.at[where], full.at[where], dim, shift)

    stage_of = [0 if item < 4 else 1 + (item - 4) // 3 for item in range(len(lanes))]
    n_stage = max(stage_of) + 1
    for time in range(n_stage + 6):
        for stage in range(n_stage):
            level = time - stage
            if 0 <= level <= 6:
                for lane in lanes:
                    if stage_of[lane[0]] == stage:
                        step(lane, level)
    for lane in lanes:
        item = lane[0]
        copies[item, "pair"].wait_recv()
    for lane in lanes:
        item = lane[0]
        copies[item, "pair"].wait_send()
        for slot in range(12):
            copies[item, slot].wait_send()


def gather_items():
    items = [(0, 0, PIECE, (1536, PIECE * j), ORDERS[j]) for j in range(3)]
    items.append((4, 0, 128, (128, 0), ORDERS[0]))
    rest = [(1, 0, PIECE, (512, 0))]
    rest += [(2, 0, PIECE, (2048, PIECE * j)) for j in range(4)]
    rest += [(3, 16 * j, PIECE, (512, 0)) for j in range(4)]
    items += [piece + (ORDERS[k % 3],) for k, piece in enumerate(rest)]
    return items


def gather_call(shards):
    n = len(gather_items())
    bf = jnp.bfloat16
    outs = [jax.ShapeDtypeStruct((4, 4, 4) + s.shape, bf) for s in shards]
    return pl.pallas_call(
        gather_kernel, out_shape=outs,
        in_specs=[pl.BlockSpec(memory_space=pltpu.VMEM)] * 5,
        out_specs=[pl.BlockSpec(memory_space=pl.ANY)] * 5,
        scratch_shapes=[pltpu.SemaphoreType.DMA((n,)), pltpu.SemaphoreType.DMA((n, 12)),
                        pltpu.SemaphoreType.DMA((n, 12)), pltpu.SemaphoreType.DMA((n,)),
                        pltpu.SemaphoreType.DMA((n,))],
        compiler_params=pltpu.CompilerParams(collective_id=0, has_side_effects=True),
        name="gather_params",
    )(*shards)


def scatter_items():
    rest = [(3, 16 * j, PIECE, (512, 0)) for j in range(4)]
    rest += [(2, 0, PIECE, (2048, PIECE * j)) for j in range(4)]
    rest += [(1, 0, PIECE, (512, 0))]
    rest += [(0, 0, PIECE, (1536, PIECE * j)) for j in range(3)]
    items = [piece + (ORDERS[k % 3],) for k, piece in enumerate(rest)]
    items.append((4, 0, 128, (128, 0), ORDERS[0]))
    return items


def scatter_kernel(*refs):
    grads, outs = refs[:5], refs[5:10]
    pair_buf, pair_small = refs[10:12]
    (acc, acc_s, stage_buf, stage_s, half0, half1, half2, whole0, whole1, whole2,
     sh0, sh1, sh2, sw0, sw1, sw2,
     own_sem, stage_sem, pair_send, pair_recv, send_sem, recv_sem, out_sem, outr_send, outr_recv) = refs[12:]
    rep, place = my_place()
    items = scatter_items()
    n = len(items)
    small = n - 1
    copies = {}

    def window(item, core):
        which, row, cols, base, order = items[item]
        col = pl.multiple_of(core * base[0] + base[1], 128)
        return pl.ds(row, 16), pl.ds(col, cols)

    for item in range(n):
        which = items[item][0]
        rows, columns = window(item, rep)
        dst = acc_s if item == small else acc.at[item]
        copies[item, "own"] = pltpu.make_async_copy(grads[which].at[:, :, :, rows, columns], dst, own_sem.at[item])
        copies[item, "own"].start()
    entry_barrier(rep, place)
    for item in range(n):
        which = items[item][0]
        rows, columns = window(item, 1 - rep)
        dst = pair_small if item == small else pair_buf.at[item]
        copies[item, "pair"] = pltpu.make_async_remote_copy(
            src_ref=grads[which].at[:, :, :, rows, columns], dst_ref=dst,
            send_sem=pair_send.at[item], recv_sem=pair_recv.at[item],
            device_id=(1 - rep, flat_of(place)), device_id_type=MESH_ID)
        copies[item, "pair"].start()

    halves, wholes = (half0, half1, half2), (whole0, whole1, whole2)
    small_halves, small_wholes = (sh0, sh1, sh2), (sw0, sw1, sw2)

    def bufs(item, phase, second, side):
        if item == small:
            return (small_wholes if second else small_halves)[phase].at[side]
        return (wholes if second else halves)[phase].at[item, side]

    def total(item):
        return acc_s if item == small else acc.at[item]

    def left_over(order, phase):
        return sorted(order[phase + 1:])

    def index_of(order, phase, dim_index, i):
        index = list(place)
        index[order[phase]] = dim_index
        rest = left_over(order, phase)
        if len(rest) == 2:
            index[rest[0]], index[rest[1]] = i // 4, i % 4
        elif len(rest) == 1:
            index[rest[0]] = i
        sub = (i // 4, i % 4) if len(rest) == 2 else ((i,) if len(rest) == 1 else ())
        return tuple(index), sub

    def piece_of(order, phase, dim_index):
        index = list(place)
        index[order[phase]] = dim_index
        for dim in left_over(order, phase):
            index[dim] = slice(None)
        return tuple(index)

    def put(item, slot, src, dst, dim, shift):
        copy = pltpu.make_async_remote_copy(
            src_ref=src, dst_ref=dst, send_sem=send_sem.at[item, slot], recv_sem=recv_sem.at[item, slot],
            device_id=(rep, flat_of(along(place, dim, shift))), device_id_type=MESH_ID)
        copy.start()
        copies[item, slot] = copy

    def add(item, phase, dim_index, second, sides, row, rows):
        order = items[item][4]
        count = 4 ** (2 - phase)

        def body(i, carry):
            index, sub = index_of(order, phase, dim_index, i)
            target = total(item)
            value = target[index + (pl.ds(row, rows), slice(None))]
            for side in sides:
                value = value + bufs(item, phase, second, side)[sub + (slice(None), slice(None))]
            target[index + (pl.ds(row, rows), slice(None))] = value
            return carry

        lax.fori_loop(0, count, body, 0)

    def close_phase(item, phase):
        dim = items[item][4][phase]
        copies[item, 4 * phase + 2].wait_recv()
        copies[item, 4 * phase + 3].wait_recv()
        add(item, phase, place[dim], 1, (0, 1), 0, 16)

    def step(item, level):
        which, row, cols, base, order = items[item]
        if level == 0:
            copies[item, "pair"].wait_recv()
            stg = stage_s if item == small else stage_buf.at[item % 3]
            src = pair_small if item == small else pair_buf.at[item]
            load = pltpu.make_async_copy(src, stg, stage_sem.at[3 if item == small else item % 3])
            load.start()
            copies[item, "own"].wait()
            load.wait()

            def body(i, carry):
                z, y, x = i // 16, (i // 4) % 4, i % 4
                target = total(item)
                target[z, y, x] = target[z, y, x] + stg[z, y, x]
                return carry

            lax.fori_loop(0, 64, body, 0)
        if level in (2, 4, 6):
            close_phase(item, level // 2 - 1)
        if level == 6:
            rows, columns = window(item, rep)
            final = total(item).at[place]
            out_at = outs[which].at[rows, columns]
            copies[item, "out"] = pltpu.make_async_copy(final, out_at, out_sem.at[item])
            copies[item, "out"].start()
            copies[item, "outr"] = pltpu.make_async_remote_copy(
                src_ref=final, dst_ref=out_at, send_sem=outr_send.at[item], recv_sem=outr_recv.at[item],
                device_id=(1 - rep, flat_of(place)), device_id_type=MESH_ID)
            copies[item, "outr"].start()
            return
        phase, second = level // 2, level % 2
        dim = order[phase]
        for side, shift, half in ((0, 1, 0), (1, 3, 8)):
            slot = 4 * phase + 2 * second + side
            near = (place[dim] + shift) % 4
            if second:
                copies[item, 4 * phase + side].wait_recv()
                add(item, phase, near, 0, (side,), half, 8)
        for side, shift, half in ((0, 1, 0), (1, 3, 8)):
            slot = 4 * phase + 2 * second + side
            near, far = (place[dim] + shift) % 4, (place[dim] + 2) % 4
            if second:
                src = total(item).at[piece_of(order, phase, near)]
            else:
                src = total(item).at[piece_of(order, phase, far) + (pl.ds(half, 8), slice(None))]
            put(item, slot, src, bufs(item, phase, second, side), dim, shift)

    stage_of = [item // 3 if item < small else 3 for item in range(n)]
    n_stage = max(stage_of) + 1
    for time in range(n_stage + 6):
        for stage in range(n_stage):
            level = time - stage
            if 0 <= level <= 6:
                for item in range(n):
                    if stage_of[item] == stage:
                        step(item, level)
    for item in range(n):
        copies[item, "outr"].wait_recv()
        copies[item, "outr"].wait_send()
        copies[item, "out"].wait()
        copies[item, "pair"].wait_send()
        for slot in range(12):
            copies[item, slot].wait_send()


def scatter_call(grads):
    n = len(scatter_items())
    m = n - 1
    f32 = jnp.float32
    dma = pltpu.SemaphoreType.DMA
    outs = [jax.ShapeDtypeStruct(g.shape[3:], f32) for g in grads]
    outs += [jax.ShapeDtypeStruct((m, 4, 4, 4, 16, PIECE), f32), jax.ShapeDtypeStruct((4, 4, 4, 16, 128), f32)]
    results = pl.pallas_call(
        scatter_kernel, out_shape=outs,
        in_specs=[pl.BlockSpec(memory_space=pl.ANY)] * 5,
        out_specs=[pl.BlockSpec(memory_space=pl.ANY)] * 7,
        scratch_shapes=[
            pltpu.VMEM((m, 4, 4, 4, 16, PIECE), f32), pltpu.VMEM((4, 4, 4, 16, 128), f32),
            pltpu.VMEM((3, 4, 4, 4, 16, PIECE), f32), pltpu.VMEM((4, 4, 4, 16, 128), f32),
            pltpu.VMEM((m, 2, 4, 4, 8, PIECE), f32), pltpu.VMEM((m, 2, 4, 8, PIECE), f32), pltpu.VMEM((m, 2, 8, PIECE), f32),
            pltpu.VMEM((m, 2, 4, 4, 16, PIECE), f32), pltpu.VMEM((m, 2, 4, 16, PIECE), f32), pltpu.VMEM((m, 2, 16, PIECE), f32),
            pltpu.VMEM((2, 4, 4, 8, 128), f32), pltpu.VMEM((2, 4, 8, 128), f32), pltpu.VMEM((2, 8, 128), f32),
            pltpu.VMEM((2, 4, 4, 16, 128), f32), pltpu.VMEM((2, 4, 16, 128), f32), pltpu.VMEM((2, 16, 128), f32),
            dma((n,)), dma((4,)), dma((n,)), dma((n,)), dma((n, 12)), dma((n, 12)), dma((n,)), dma((n,)), dma((n,))],
        compiler_params=pltpu.CompilerParams(collective_id=1, has_side_effects=True, vmem_limit_bytes=67043328),
        name="scatter_grads",
    )(*grads)
    return results[:5]


def gather_weights(shards):
    w_qkv, b_qkv, w_out, w_up, b_up, w_down, vec_params = [s.astype(jnp.bfloat16) for s in shards]
    small = jnp.zeros((16, 256), jnp.bfloat16)
    small = small.at[0, 0:48].set(b_qkv).at[0, 48:112].set(b_up).at[0, 128:256].set(vec_params.reshape(128))
    qkv, out, up, down, table = gather_call((w_qkv, w_out, w_up, w_down, small))
    table = table.reshape(64, 16, 256)[:, 0].astype(jnp.float32)
    vec = table[:, 128:].reshape(64, 8, 16).transpose(1, 0, 2).reshape(8, 1024)
    return (qkv.reshape(1024, 3072), table[:, 0:48].reshape(3072), out.reshape(1024, 1024),
            up.reshape(1024, 4096), table[:, 48:112].reshape(4096), down.reshape(4096, 1024), vec)


def reduce_grads(local_grads):
    grad_w_qkv, grad_b_qkv, grad_w_out, grad_w_up, grad_b_up, grad_w_down, grad_vec = local_grads
    flat = jnp.concatenate([grad_b_qkv.reshape(64, 48), grad_b_up.reshape(64, 64), jnp.zeros((64, 16), jnp.float32),
                            grad_vec.reshape(8, 64, 16).transpose(1, 0, 2).reshape(64, 128)], axis=1)
    small = jnp.pad(flat[:, None, :], ((0, 0), (0, 15), (0, 0))).reshape(4, 4, 4, 16, 256)
    qkv, out, up, down, small = scatter_call((
        grad_w_qkv.reshape(4, 4, 4, 16, 3072), grad_w_out.reshape(4, 4, 4, 16, 1024),
        grad_w_up.reshape(4, 4, 4, 16, 4096), grad_w_down.reshape(4, 4, 4, 64, 1024), small))
    return qkv, small[0, 0:48], out, up, small[0, 48:112], down, small[0, 128:256].reshape(8, 16)


def solution(mesh):
    batch_spec = P(("rep", "fsdp"), None, None)
    row_spec = P("fsdp", None)
    flat_spec = P("fsdp")
    col_spec = P(None, "fsdp")
    param_specs = (row_spec, flat_spec, row_spec, row_spec, flat_spec, row_spec, col_spec)

    def device_step(x_loc, dz_loc, w_qkv, b_qkv, w_out, w_up, b_up, w_down, vec_params):
        weights = gather_weights((w_qkv, b_qkv, w_out, w_up, b_up, w_down, vec_params))
        z_loc, saved = layer_forward(x_loc, weights)
        dx_loc, local_grads = layer_backward(x_loc, dz_loc, saved, weights)
        return (z_loc, dx_loc) + reduce_grads(local_grads)

    return jax.shard_map(device_step, mesh=mesh, in_specs=(batch_spec, batch_spec) + param_specs,
                         out_specs=(batch_spec, batch_spec) + param_specs, check_vma=False)
```

```python
import jax
import jax.numpy as jnp
from jax import lax
from jax.experimental import pallas as pl
from jax.experimental.pallas import tpu as pltpu
from jax.sharding import PartitionSpec as P

LN_EPS = 1e-5

ALL = ...
FIRST, ONE = 0, 1
PACK, SHARDS, FLAT, LANES, SPAN, TRIPLE, TILE = 16, 64, 192, 128, 256, 384, 512
SUBS, RING = 8, 4
CUBE, BLOCK = (RING,) * 3, (2, SUBS, LANES)
AXES, SIDES = range(3), range(2)
ONCE = pl.Buffered(ONE)
ANYWHERE = pl.BlockSpec(memory_space=pl.ANY)
VM = pltpu.VMEM
KEEP = True
MIN = float("-inf")


def row(ref, k):
    return ref[k:k + ONE, :]


def other(rep):
    return ONE - rep


def iota(dims, axis):
    return lax.broadcasted_iota(jnp.int32, dims, axis)


def loop(count, body, start, **options):
    return lax.fori_loop(FIRST, count, body, start, **options)


def sum_rows(t):
    return jnp.sum(t, axis=FIRST, keepdims=KEEP)


def max_rows(t):
    return jnp.max(t, axis=FIRST, keepdims=KEEP)


def sum_lanes(t):
    return jnp.sum(t, axis=-ONE, keepdims=KEEP)


def max_lanes(t):
    return jnp.max(t, axis=-ONE, keepdims=KEEP)


def mean_lanes(t):
    return jnp.mean(t, axis=-ONE, keepdims=KEEP)


SEQS, TOKENS, PAD, WIDTH, HIDDEN = 6, 197, 208, 1024, 4096
ROWS = SEQS * PAD
BF, F32 = jnp.bfloat16, jnp.float32
VMEM_CAP = 67043328


def nn(a, b):
    return lax.dot_general(a, b, (((1,), (0,)), ((), ())), preferred_element_type=F32)


def nt(a, b):
    return lax.dot_general(a, b, (((1,), (1,)), ((), ())), preferred_element_type=F32)


def tn(a, b):
    return lax.dot_general(a, b, (((0,), (0,)), ((), ())), preferred_element_type=F32)


def row_stats(t):
    mean = mean_lanes(t)
    centered = t - mean
    variance = mean_lanes(centered * centered)
    return centered, lax.rsqrt(variance + LN_EPS)


def norm_back(dt, xhat, rstd):
    return rstd * (dt - mean_lanes(dt) - xhat * mean_lanes(dt * xhat))


def head_halves(width=LANES):
    lane = iota((1, width), 1)
    return lane < SHARDS


def stack_heads(dst, rows, low):
    zero = jnp.zeros_like(rows)
    dst[:PAD] = jnp.where(low, rows, zero)
    dst[SPAN:SPAN + PAD] = jnp.where(low, zero, rows)


def padded(dst, base, rows_ref, s):
    dst[base + FLAT:base + PAD] = jnp.zeros((PACK, WIDTH), dst.dtype)
    dst[base:base + TOKENS] = rows_ref[s].astype(dst.dtype)


MESH_ID = pl.DeviceIdType.MESH
ORDERS = ((2, 1, 0), (1, 0, 2), (0, 2, 1))
HOPS = (1, 2, 3)
GREETED = 10
FAR, NEAR, DIRECT = "far", "near", "direct"
EVERY = slice(None)


def my_place():
    rep, flat = lax.axis_index("rep"), lax.axis_index("fsdp")
    return rep, (flat // PACK, (flat // RING) % RING, flat % RING)


def along(place, dim, shift):
    moved = list(place)
    moved[dim] = (place[dim] + shift) % RING
    return tuple(moved)


def flat_of(place):
    return place[0] * PACK + place[1] * 4 + place[2]


def greet(sem, rep, place):
    pl.semaphore_signal(sem, inc=1, device_id=(other(rep), flat_of(place)), device_id_type=MESH_ID)
    for dim in AXES:
        for shift in HOPS:
            pl.semaphore_signal(sem, inc=1, device_id=(rep, flat_of(along(place, dim, shift))), device_id_type=MESH_ID)


def entry_barrier(rep, place):
    barrier = pltpu.get_barrier_semaphore()
    greet(barrier, rep, place)
    pl.semaphore_wait(barrier, GREETED)


def ring_scratch(slots, stages, parts):
    dma = pltpu.SemaphoreType.DMA
    block = BLOCK
    cube, square, line = CUBE, CUBE[1:], CUBE[2:]
    sides = (parts, 3)
    buffers = [(slots, parts) + cube + block, (parts,) + cube + block, (parts,) + cube + block,
               (stages, parts) + square + block,
               (slots,) + sides + square + block, (stages,) + sides + line + block, (stages,) + sides + block]
    sems = [(parts,)] * 2 + [(slots, parts, 5)] * 2 + [(stages, parts, 6)] * 2 + [(stages, parts, 2)] * 3
    regular = pltpu.SemaphoreType.REGULAR
    return [VM(b, F32) for b in buffers] + [dma(s) for s in sems] + [regular((slots,)), regular]


class Ring:
    def __init__(self, refs, slots, steps, window):
        (self.acc, self.inbox, self.outbox, self.rest, land0, land1, land2, self.pair_send, self.pair_recv,
         self.send, self.recv, self.rest_send, self.rest_recv, self.out_sem, self.out_send, self.out_recv,
         self.free, self.emptied) = refs
        self.landing = (land0, land1, land2)
        self.slots, self.steps, self.last = slots, steps, len(steps)
        self.window = window
        self.rep, self.place = my_place()
        self.partner = (other(self.rep), flat_of(self.place))

    def pair(self, part):
        return pltpu.make_async_remote_copy(
            src_ref=self.outbox.at[part], dst_ref=self.inbox.at[part], send_sem=self.pair_send.at[part],
            recv_sem=self.pair_recv.at[part], device_id=self.partner, device_id_type=MESH_ID)

    def axis(self, order, phase, index):
        at = {dim: EVERY for dim in order}
        for dim in order[:phase]:
            at[dim] = self.place[dim]
        at[order[phase]] = index
        if phase:
            del at[order[0]]
        return tuple(at[dim] for dim in sorted(at))

    def home(self, stage, part, phase):
        if phase:
            return self.rest, (stage, part), self.rest_send, self.rest_recv
        return self.acc, (stage % self.slots, part), self.send, self.recv

    def hops(self, stage, part, order, step):
        phase, kind = step
        dim = order[phase]
        memory, at, send, recv = self.home(stage, part, phase)
        found = []
        for side, shift in enumerate((1, 3) if kind != DIRECT else HOPS):
            number = side
            source, target, place = shift, 0, at + (side,)
            if kind == FAR:
                source, target = 2, shift
            if kind == NEAR:
                number = side + 2
            if phase == 2:
                number = side + 3
            src = at + self.axis(order, phase, (self.place[dim] + source) % RING)
            into = at + self.axis(order, phase, (self.place[dim] + target) % RING)
            if kind == FAR:
                src, into, place = src + (side,), into + (side,), at + (2,) + (EVERY, EVERY, side)
            copy = pltpu.make_async_remote_copy(
                src_ref=memory.at[src], dst_ref=self.landing[phase].at[place], send_sem=send.at[at + (number,)],
                recv_sem=recv.at[at + (number,)], device_id=(self.rep, flat_of(along(self.place, dim, shift))),
                device_id_type=MESH_ID)
            found.append((copy, into, place))
        return found

    def results(self, stage, part, order):
        copies = []
        for half in SIDES:
            at = (stage, part, half)
            src = self.rest.at[(stage, part) + tuple(self.place[dim] for dim in sorted(order[1:])) + (half,)]
            dst = self.window(stage, part, half)
            copies.append(pltpu.make_async_copy(src, dst, self.out_sem.at[at]))
            copies.append(pltpu.make_async_remote_copy(
                src_ref=src, dst_ref=dst, send_sem=self.out_send.at[at], recv_sem=self.out_recv.at[at],
                device_id=self.partner, device_id_type=MESH_ID))
        return copies

    def level(self, stage, level, orders, credit, refill):
        if level == 0:
            for part in orders:
                self.pair(part).wait()
                at = (stage % self.slots, part)
                for z in range(4):
                    self.acc[at + (z,)] = self.acc[at + (z,)] + self.inbox[part, z]

            @pl.when(stage >= self.slots)
            def _():
                pl.semaphore_wait(self.free.at[stage % self.slots], GREETED)

            @pl.when(refill)
            def _():
                pl.semaphore_signal(self.emptied, inc=1, device_id=self.partner, device_id_type=MESH_ID)
        else:
            step = self.steps[level - 1]
            phase, kind = step
            for part, order in orders.items():
                memory = self.home(stage, part, phase)[0]
                hops = self.hops(stage, part, order, step)
                for copy, _, _ in hops:
                    copy.wait_recv()
                if kind == FAR:
                    for _, into, place in hops:
                        memory[into] = memory[into] + self.landing[phase][place]
                    continue
                into = hops[0][1]
                total = memory[into]
                for _, _, place in hops:
                    total = total + self.landing[phase][place]
                if phase:
                    memory[into] = total
                else:
                    self.rest[stage, part] = total
            if phase == 0 and kind != FAR:
                self.sent(stage, orders, (0,))

                @pl.when(credit)
                def _():
                    greet(self.free.at[stage % self.slots], self.rep, self.place)
        for part, order in orders.items():
            if level < self.last:
                for copy, _, _ in self.hops(stage, part, order, self.steps[level]):
                    copy.start()
            else:
                for copy in self.results(stage, part, order):
                    copy.start()
        if level == self.last:
            self.sent(stage, orders, (1, 2))

    def sent(self, stage, orders, phases):
        for step in self.steps:
            if step[0] in phases:
                for part, order in orders.items():
                    for copy, _, _ in self.hops(stage, part, order, step):
                        copy.wait_send()

    def settle(self, stage, orders):
        for part, order in orders.items():
            for copy in self.results(stage, part, order):
                copy.wait()

    def reopen_box(self):
        pl.semaphore_wait(self.emptied, 1)


PIECE = TILE
QKV, OUT, UP, DOWN, SMALL = range(5)


def gather_items():
    rest = [(OUT, 0, 0, PIECE)]
    rest += [(UP, 0, PIECE * j, HIDDEN // 2) for j in range(4)]
    rest += [(DOWN, PACK * j, 0, PIECE) for j in range(4)]
    items = [(0, QKV, 0, PIECE * j, 3 * PIECE, ORDERS[j]) for j in AXES] + [(0, SMALL, 0, 0, 0, ORDERS[0])]
    return items + [(1 + k // 3,) + piece + (ORDERS[k % 3],) for k, piece in enumerate(rest)]


def small_rows(table, vec, b_qkv, b_up):
    lane = iota((SUBS, LANES), 1)

    def moved(f, half, shift):
        return pltpu.roll(table[f // PACK, f // RING % RING, f % RING, half], shift % LANES, 1)

    def fill(ref, tile, owners, half, width, first):
        total = jnp.zeros((SUBS, LANES), F32)
        for f in owners:
            start = width * f - LANES * tile
            here = jnp.logical_and(lane >= start, lane < start + width)
            total = jnp.where(here, moved(f, half, start - first), total)
        ref[:, tile * LANES:tile * LANES + LANES] = total[:ref.shape[0]]

    for tile in range(WIDTH // LANES):
        fill(vec, tile, range(SUBS * tile, SUBS * tile + SUBS), 0, PACK, 0)
    for tile in range(TILE // LANES):
        fill(b_up, tile, range(PACK * tile, PACK * tile + PACK), 1, SUBS, 0)
    for tile in range(3 * WIDTH // LANES):
        fill(b_qkv, tile, range(LANES * tile // 48, (LANES * tile + LANES - 1) // 48 + 1), 0, 48, PACK)


def placed(values, first):
    size = values.shape[ONE]
    lane = iota((size, LANES), 1)
    row = iota((size, LANES), 0)
    return nn(values.astype(BF), jnp.where(lane == row + first, 1.0, 0.0).astype(BF))


def first_kernel(x_ref, dz_ref, sq_ref, so_ref, su_ref, sd_ref, bq_ref, bu_ref, sv_ref,
                 h1_ref, qkv_ref, o_ref, a_ref, h2_ref, dm_ref, vec_ref, bup_ref, wq_hbm, wo_hbm, wu_hbm, wd_hbm,
                 wq, wo, su, sd, table, bias, xhat, kst, vst, xp,
                 own_sem, send_sem, recv_sem, pair_send, pair_recv, save_sem):
    t = pl.program_id(0)
    rep, place = my_place()
    partner = (other(rep), flat_of(place))
    items = gather_items()
    fulls = (wq, wo, wu_hbm, wd_hbm, table)

    def block(item, shards, half=None):
        _, array, row, first, step, _ = items[item]
        if array == SMALL:
            return table.at[shards + ((half,) if half is not None else ())]
        col, cols = rep * step + first, PIECE
        if half is not None:
            col, cols = col + half * (PIECE // 2), PIECE // 2
        return fulls[array].at[shards + (pl.ds(row, PACK), pl.ds(pl.multiple_of(col, LANES), cols))]

    def shard(item):
        _, array, row, first, step, _ = items[item]
        return (su, sd)[array - UP].at[pl.ds(row, PACK), pl.ds(pl.multiple_of(rep * step + first, LANES), PIECE)]

    def own(item):
        return pltpu.make_async_copy(shard(item), block(item, place), own_sem.at[item])

    def pair(item):
        everywhere = block(item, (EVERY,) * 3)
        return pltpu.make_async_remote_copy(
            src_ref=everywhere, dst_ref=everywhere, send_sem=pair_send.at[item], recv_sem=pair_recv.at[item],
            device_id=partner, device_id_type=MESH_ID)

    def hops(item, level):
        array, order = items[item][1], items[item][-1]
        phase, second = level // 2, level % 2
        dim = order[phase]
        found = []
        for side, shift in enumerate((1, 3)):
            at = [EVERY] * 3
            for later in order[phase:]:
                at[later] = place[later]
            if second:
                at[dim] = (place[dim] + 4 - shift) % RING
            dst = block(item, tuple(at), side if second else None)
            src = shard(item) if level == 0 and array in (UP, DOWN) else dst
            number = 2 * level + side
            found.append(pltpu.make_async_remote_copy(
                src_ref=src, dst_ref=dst, send_sem=send_sem.at[item, number], recv_sem=recv_sem.at[item, number],
                device_id=(rep, flat_of(along(place, dim, shift))), device_id_type=MESH_ID))
        return found

    def advance(*todo):
        for stage, level in todo:
            for item in range(len(items)):
                if items[item][0] != stage:
                    continue
                if level:
                    for copy in hops(item, level - 1):
                        copy.wait_recv()
                if level == 2 and items[item][1] in (UP, DOWN):
                    own(item).wait()
                if level == 6:
                    if items[item][1] != SMALL:
                        pair(item).start()
                else:
                    for copy in hops(item, level):
                        copy.start()

    def arrived(*arrays):
        for item in range(len(items)):
            if items[item][1] in arrays:
                pair(item).wait_recv()

    def saves():
        return (pltpu.make_async_copy(wq, wq_hbm, save_sem.at[FIRST]), pltpu.make_async_copy(wo, wo_hbm, save_sem.at[1]))

    @pl.when(t == FIRST)
    def _():
        for full, piece, half in ((wq, sq_ref, 3 * PIECE), (wo, so_ref, PIECE)):
            cols = pl.ds(pl.multiple_of(rep * half, LANES), half)
            full[place + (EVERY, cols)] = piece[:, cols].astype(BF)
        su[ALL] = su_ref[ALL].astype(BF)
        sd[ALL] = sd_ref[ALL].astype(BF)
        first_row = iota((SUBS, 48), 0) == 0
        table[place + (0,)] = placed(sv_ref[ALL], 0) + placed(jnp.where(first_row, bq_ref[ALL], 0.0), PACK)
        table[place + (1,)] = placed(bu_ref[ALL], 0)
        entry_barrier(rep, place)
        advance((0, 0))
        for item in range(len(items)):
            if items[item][1] in (UP, DOWN):
                own(item).start()
        for s in range(SEQS):
            base = s * PAD
            xp[FLAT:PAD] = jnp.zeros((PACK, WIDTH), BF)
            xp[:TOKENS] = x_ref[s]
            centered, rstd = row_stats(xp[ALL].astype(F32))
            xhat[base:base + PAD] = centered * rstd
            level = s + 1
            if s < 5:
                advance(*((stage, level - stage) for stage in range(min(level, 3) + 1)))
        advance((0, 6))
        small_rows(table, vec_ref, bias, bup_ref)
        h1_ref[ALL] = (xhat[ALL] * vec_ref[:1, :] + row(vec_ref, 1)).astype(BF)
        for s in range(SEQS):
            h1_ref[s * PAD + FLAT:s * PAD + PAD] = jnp.where(
                iota((PACK, 1), 0) < TOKENS - FLAT, h1_ref[s * PAD + FLAT:s * PAD + PAD], jnp.zeros((), BF))
        arrived(QKV)
        saves()[0].start()
        kst[ALL] = jnp.zeros_like(kst)
        vst[ALL] = jnp.zeros_like(vst)

    @pl.when(t > FIRST)
    def _():
        base = pl.multiple_of((t - 1) * (2 * PAD), PACK)

        def qkv_tile(n, carry):
            cols = pl.ds(pl.multiple_of(n * PIECE, PIECE), PIECE)
            weights = wq[:, :, :, :, cols].reshape(WIDTH, PIECE)
            qkv_ref[:, cols] = (nn(h1_ref[pl.ds(base, 2 * PAD), :], weights) + bias[:, cols]).astype(BF)
            return carry

        loop(6, qkv_tile, 0)

    @pl.when(t == 1)
    def _():
        advance((1, 5), (2, 4), (3, 3))

    @pl.when(t == 2)
    def _():
        advance((3, 6))

    low = head_halves()
    visible = iota((1, SPAN), 1) < TOKENS

    def head_pair(p, carry):
        def cols(third):
            return pl.ds(pl.multiple_of(third * WIDTH + p * LANES, LANES), LANES)

        for s in SIDES:
            rows = pl.ds(s * PAD, PAD)
            stack_heads(kst.at[s], qkv_ref[rows, cols(1)], low)
            stack_heads(vst.at[s], qkv_ref[rows, cols(2)], low)
        for s in SIDES:
            rows = pl.ds(s * PAD, PAD)
            scores = nt(qkv_ref[rows, cols(0)], kst[s])
            probs = []
            for half in SIDES:
                part = jnp.where(visible, scores[:, half * SPAN:half * SPAN + SPAN], -jnp.inf)
                top = max_lanes(part)
                e = jnp.exp((part - top) * 0.125)
                probs.append((e * (1.0 / sum_lanes(e))).astype(BF))
            o_ref[rows, pl.ds(pl.multiple_of(p * LANES, LANES), LANES)] = nn(jnp.concatenate(probs, axis=1), vst[s]).astype(BF)
        return carry

    @pl.when(t > FIRST)
    def _():
        loop(4, head_pair, 0, unroll=4)

    @pl.when(t == 1)
    def _():
        advance((1, 6), (2, 5), (3, 4))

    @pl.when(t > FIRST)
    def _():
        lax.fori_loop(4, SUBS, head_pair, 0, unroll=4)

    @pl.when(t == 1)
    def _():
        advance((2, 6), (3, 5))
        arrived(OUT)
        saves()[1].start()

    @pl.when(t > FIRST)
    def _():
        for s in SIDES:
            padded(xp, 0, x_ref, 2 * (t - 1) + s)
            xhat[s * PAD:s * PAD + PAD] = xp[ALL].astype(F32)
            dm_ref[s * PAD + FLAT:s * PAD + PAD] = jnp.zeros((PACK, WIDTH), BF)
            dm_ref[s * PAD:s * PAD + TOKENS] = (dz_ref[s].astype(F32) * row(vec_ref, 7)).astype(BF)
        a_ref[ALL] = nn(o_ref[ALL], wo[ALL].reshape(WIDTH, WIDTH)) + row(vec_ref, 2)

        def rows(i, carry):
            at = pl.ds(pl.multiple_of(i * 32, 32), 32)
            y = xhat[at, :] + row(vec_ref, 3) * a_ref[at, :]
            centered, rstd = row_stats(y)
            h2_ref[at, :] = (centered * rstd * row(vec_ref, 4) + row(vec_ref, 5)).astype(BF)
            return carry

        loop(2 * PAD // 32, rows, 0, unroll=13)

    @pl.when(t == 3)
    def _():
        arrived(UP, DOWN)
        for item in range(len(items)):
            if items[item][1] != SMALL:
                pair(item).wait_send()
            for level in range(6):
                for copy in hops(item, level):
                    copy.wait_send()
        for copy in saves():
            copy.wait()


def first(x, dz, shards, small):
    whole = lambda dims: pl.BlockSpec(dims, lambda t: (0,) * len(dims), pipeline_mode=ONCE)
    pair = lambda t: jnp.maximum(t - 1, 0)
    rows = lambda width: pl.BlockSpec((2 * PAD, width), lambda t: (pair(t), 0))
    anywhere = ANYWHERE
    shape, vmem, dma = jax.ShapeDtypeStruct, VM, pltpu.SemaphoreType.DMA
    n = len(gather_items())
    cube = CUBE
    return pl.pallas_call(
        first_kernel, grid=(4,),
        out_shape=[shape((ROWS, WIDTH), BF), shape((ROWS, 3 * WIDTH), BF), shape((ROWS, WIDTH), BF), shape((ROWS, WIDTH), F32),
                   shape((ROWS, WIDTH), BF), shape((ROWS, WIDTH), BF), shape((SUBS, WIDTH), F32), shape((SUBS, TILE), F32)]
        + [shape(cube + s.shape, BF) for s in shards],
        in_specs=[whole((SEQS, TOKENS, WIDTH)), pl.BlockSpec((2, TOKENS, WIDTH), lambda t: (pair(t), 0, 0))]
        + [whole(s.shape) for s in shards + small],
        out_specs=[whole((ROWS, WIDTH)), rows(3 * WIDTH), rows(WIDTH), rows(WIDTH), rows(WIDTH), rows(WIDTH),
                   whole((SUBS, WIDTH)), whole((SUBS, TILE))] + [anywhere] * 4,
        scratch_shapes=[vmem(cube + shards[QKV].shape, BF), vmem(cube + shards[OUT].shape, BF), vmem(shards[UP].shape, BF),
                        vmem(shards[DOWN].shape, BF), vmem(cube + (2, SUBS, LANES), F32), vmem((1, 3 * WIDTH), F32),
                        vmem((ROWS, WIDTH), F32), vmem((2, PIECE, LANES), BF), vmem((2, PIECE, LANES), BF),
                        vmem((PAD, WIDTH), BF),
                        dma((n,)), dma((n, 12)), dma((n, 12)), dma((n,)), dma((n,)), dma((2,))],
        compiler_params=pltpu.CompilerParams(vmem_limit_bytes=VMEM_CAP, collective_id=0, has_side_effects=True),
        name="first",
    )(x, dz, *shards, *small)


CHUNK = 624
TILES = HIDDEN // TILE
MLP_SLOTS, MLP_PARTS = 3, 4
MLP_STEPS = ((0, FAR), (0, NEAR), (1, DIRECT), (2, DIRECT))


def gelu_and_slope(u):
    cdf = 0.5 * (1.0 + lax.erf(u * (2.0 ** -0.5)))
    pdf = jnp.exp(u * u * -0.5) * ((2.0 * jnp.pi) ** -0.5)
    return u * cdf, cdf + u * pdf


def mlp_kernel(h_ref, dm_ref, w1_ref, w2_ref, b1_ref, x_ref, dz_ref, a_ref, wo_ref, vec_ref,
               gw1_ref, gw2_ref, gb_ref, z_ref, gr_ref, da_ref, do_ref, gv_ref,
               m_acc, dh_acc, act, dpre, turned, xp, zp, zo, *ring_refs):
    j = pl.program_id(0)

    def window(stage, part, half):
        if part < 2:
            col = rep * TILE + (part * 2 + half) * LANES
            return gw2_ref.at[pl.ds(pl.multiple_of(stage * SUBS, SUBS), SUBS), pl.ds(pl.multiple_of(col, LANES), LANES)]
        col = stage * TILE + rep * SPAN + (part - 2) * LANES
        return gw1_ref.at[pl.ds(half * SUBS, SUBS), pl.ds(pl.multiple_of(col, LANES), LANES)]

    ring = Ring(ring_refs, MLP_SLOTS, MLP_STEPS, window)
    rep = ring.rep
    every_part = range(MLP_PARTS)

    def run(lag, level):
        stage = j - lag
        for turn in AXES:
            orders = {part: ORDERS[(turn + part) % 3] for part in every_part}

            @pl.when(jnp.logical_and(jnp.logical_and(stage >= 0, stage < TILES), stage % 3 == turn))
            def _(orders=orders):
                ring.level(stage, level, orders, stage < TILES - MLP_SLOTS, stage < TILES - 1)

    @pl.when(j == FIRST)
    def _():
        entry_barrier(rep, ring.place)
        m_acc[ALL] = jnp.zeros_like(m_acc)
        dh_acc[ALL] = jnp.zeros_like(dh_acc)
        turned[ALL] = jnp.transpose(h_ref[ALL])

    def chunk(i, total):
        at = pl.ds(i * CHUNK, CHUNK)
        w1, w2 = w1_ref[ALL], w2_ref[ALL].reshape(TILE, WIDTH)
        u = nn(h_ref[at, :], w1) + b1_ref[pl.ds(j, 1), :]
        value, slope = gelu_and_slope(u)
        act[at, :] = value.astype(BF)
        d = nt(dm_ref[at, :], w2) * slope
        dpre[at, :] = d.astype(BF)
        m_acc[at, :] += nn(act[at, :], w2)
        dh_acc[at, :] += nt(dpre[at, :], w1)
        return sum_rows(d) + total

    def grads(core, target):
        cols = pl.ds(pl.multiple_of(core * TILE, TILE), TILE)
        g = tn(act[ALL], dm_ref[:, cols])
        for part in SIDES:
            for half in SIDES:
                first = (part * 2 + half) * LANES
                target(part, half, g[:, first:first + LANES].reshape(CUBE + BLOCK[1:]))

    def grads_up(core, target):
        g = nn(turned[ALL], dpre[:, pl.ds(pl.multiple_of(core * SPAN, SPAN), SPAN)])
        for part in SIDES:
            target(part + 2, EVERY, g[:, part * LANES:part * LANES + LANES].reshape(CUBE + BLOCK))

    @pl.when(j < TILES)
    def _():
        gb_ref[pl.ds(j, 1), :] = chunk(1, chunk(0, 0.0))

    @pl.when(j == TILES)
    def _():
        gv_ref[ALL] = jnp.zeros_like(gv_ref)

    @pl.when(j >= TILES)
    def _():
        padded(xp, 0, x_ref, 0)
        padded(zp, 0, dz_ref, 0)
        s1, g2, b2, s2 = (vec_ref[k:k + 1, :] for k in (3, 4, 6, 7))
        here = pl.ds(pl.multiple_of((j - TILES) * PAD, PACK), PAD)
        a = a_ref[ALL]
        y = xp[ALL].astype(F32) + s1 * a
        mlp_out = m_acc[here, :] + b2
        g_out = zp[ALL].astype(F32)
        zo[ALL] = (y + s2 * mlp_out).astype(BF)
        centered, rstd = row_stats(y)
        xhat = centered * rstd
        dh = dh_acc[here, :]
        g_resid = g_out + norm_back(dh * g2, xhat, rstd)
        d_att = g_resid * s1
        gr_ref[ALL] = g_resid
        da_ref[ALL] = d_att.astype(BF)
        for k, total in enumerate((d_att, g_resid * a, dh * xhat, dh, g_out * s2, g_out * mlp_out)):
            gv_ref[2 + k:3 + k, :] += sum_rows(total)
        z_ref[0] = zo[:TOKENS]
        do_ref[ALL] = nt(da_ref[ALL], wo_ref[ALL]).astype(BF)

    for lag in range(ring.last + 1, 0, -1):
        run(lag, lag - 1)

    @pl.when(j < TILES)
    def _():
        slot = j % MLP_SLOTS

        def out(part, half, value):
            ring.outbox[part, :, :, :, half] = value

        def own(part, half, value):
            ring.acc[slot, part, :, :, :, half] = value

        grads(other(rep), out)
        grads_up(other(rep), out)

        @pl.when(j >= 1)
        def _():
            ring.reopen_box()

        for part in every_part:
            ring.pair(part).start()
        grads(rep, own)
        grads_up(rep, own)

    @pl.when(j == TILES + SEQS - 1)
    def _():
        for stage in range(TILES):
            ring.settle(stage, {part: ORDERS[(stage + part) % 3] for part in every_part})


def mlp(h, dm, w1, b1, w2, x, dz, a, w_out, vec):
    whole = lambda shape: pl.BlockSpec(shape, lambda j: (0, 0), pipeline_mode=ONCE)
    tile = lambda j: jnp.minimum(j, TILES - 1)
    seq = lambda j: jnp.maximum(j - TILES, 0)
    b1_spec = whole((SUBS, TILE))
    seqs = pl.BlockSpec((1, TOKENS, WIDTH), lambda j: (seq(j), 0, 0))
    rows = pl.BlockSpec((PAD, WIDTH), lambda j: (seq(j), 0))
    anywhere = ANYWHERE
    shape = jax.ShapeDtypeStruct
    return pl.pallas_call(
        mlp_kernel, grid=(TILES + SEQS,),
        out_shape=[shape((PACK, HIDDEN), F32), shape((SHARDS, WIDTH), F32), shape((SUBS, TILE), F32),
                   shape((SEQS, TOKENS, WIDTH), BF), shape((ROWS, WIDTH), F32), shape((ROWS, WIDTH), BF),
                   shape((ROWS, WIDTH), BF), shape((8, WIDTH), F32)],
        in_specs=[whole((ROWS, WIDTH)), whole((ROWS, WIDTH)), pl.BlockSpec((WIDTH, TILE), lambda j: (0, tile(j))),
                  pl.BlockSpec((SHARDS, SUBS, WIDTH), lambda j: (0, tile(j), 0)), b1_spec, seqs, seqs, rows,
                  whole((WIDTH, WIDTH)), whole((8, WIDTH))],
        out_specs=[anywhere, anywhere, whole((SUBS, TILE)), seqs, rows, rows, rows, whole((8, WIDTH))],
        scratch_shapes=[VM((ROWS, WIDTH), F32), VM((ROWS, WIDTH), F32), VM((ROWS, TILE), BF),
                        VM((ROWS, TILE), BF), VM((WIDTH, ROWS), BF), VM((PAD, WIDTH), BF),
                        VM((PAD, WIDTH), BF), VM((PAD, WIDTH), BF)] + ring_scratch(MLP_SLOTS, TILES, MLP_PARTS),
        compiler_params=pltpu.CompilerParams(vmem_limit_bytes=VMEM_CAP, collective_id=1, has_side_effects=True),
        name="mlp",
    )(h, dm, w1, w2.reshape(SHARDS, SHARDS, WIDTH), b1, x, dz, a, w_out, vec)


GROUP = SPAN
GROUPS = WIDTH // GROUP
THIRDS = 3
ATT_SLOTS, ATT_STAGES, ATT_PARTS = 2, GROUPS + 1, 4
ATT_STEPS = tuple((phase, DIRECT) for phase in AXES)


def small_blocks(target, vec, b_qkv, b_up):
    lane = iota((SUBS, LANES), 1)

    def turned(ref, tile, first, to):
        return pltpu.roll(ref[:, tile * LANES:tile * LANES + LANES], (to - first) % LANES, 1)

    for f in range(SHARDS):
        tile, first = divmod(48 * f, LANES)
        bias = turned(b_qkv, tile, first, PACK)
        if first + 48 > LANES:
            bias = jnp.where(lane[:1] < PACK + LANES - first, bias, turned(b_qkv, tile + 1, first, PACK))
        rows = turned(vec, f // SUBS, PACK * (f % SUBS), 0)
        up = turned(b_up, f // PACK, SUBS * (f % PACK), SHARDS)
        target[f // PACK, f // RING % RING, f % RING] = jnp.where(lane < PACK, rows, jnp.where(lane < SHARDS, bias, up))


def attn_bwd_kernel(q_ref, k_ref, v_ref, do_ref, h_ref, wq_ref, wk_ref, wv_ref, o_ref, da_ref, x_ref, gr_ref, vec_ref,
                    gvin_ref, gbup_ref, gw_ref, gwo_ref, dx_ref, small_ref,
                    dh, grads, by_core, turned, qst, dst, xp, dxp, sums, biases, blocks, from_x, from_y, from_z, from_pair,
                    small_send, small_recv, *ring_refs):
    g = pl.program_id(0)

    def window(stage, part, half):
        rows = pl.ds(half * SUBS, SUBS)
        if isinstance(stage, int) and stage == 0:
            return gwo_ref.at[rows, pl.ds(pl.multiple_of(rep * TILE + part * LANES, LANES), LANES)]
        col = part * WIDTH + (stage - 1) * GROUP + rep * LANES
        return gw_ref.at[rows, pl.ds(pl.multiple_of(col, LANES), LANES)]

    ring = Ring(ring_refs, ATT_SLOTS, ATT_STEPS, window)
    rep, place = ring.rep, ring.place
    first_orders = {part: ORDERS[part % 3] for part in range(ATT_PARTS)}
    orders = {part: ORDERS[part] for part in range(THIRDS)}

    def level(stage, which, at):
        ring.level(stage, at, which, stage < ATT_STAGES - ATT_SLOTS, stage < ATT_STAGES - 1)

    def poll(todo):
        for lag, at in todo:
            @pl.when(g - lag >= 1)
            def _(lag=lag, at=at):
                level(g - lag, orders, at)

            @pl.when(g == lag)
            def _(at=at):
                level(0, first_orders, at)

    @pl.when(g == FIRST)
    def _():
        entry_barrier(rep, place)
        dh[ALL] = jnp.zeros_like(dh)
        qst[ALL] = jnp.zeros_like(qst)
        dst[ALL] = jnp.zeros_like(dst)
        turned[ALL] = jnp.transpose(h_ref[ALL])
        for core, box in ((other(rep), ring.outbox), (rep, ring.acc.at[FIRST])):
            w = tn(o_ref[ALL], da_ref[:, pl.ds(pl.multiple_of(core * TILE, TILE), TILE)])
            for part in range(ATT_PARTS):
                box[part] = w[:, part * LANES:part * LANES + LANES].reshape(CUBE + BLOCK)
            if box is ring.outbox:
                for part in range(ATT_PARTS):
                    ring.pair(part).start()

    poll(((2, 2),))
    low = head_halves()
    low_rows = iota((LANES, 1), 0) < SHARDS
    hidden = iota((PAD, 1), 0) >= TOKENS

    def seq(s, sums):
        rows = pl.ds(pl.multiple_of(s * PAD, PACK), PAD)
        out = []
        for p in SIDES:
            cols = slice(p * LANES, p * LANES + LANES)
            qs, ds = qst.at[p], dst.at[p]
            k_rows, v_rows = k_ref[rows, cols], v_ref[rows, cols]
            stack_heads(qs, q_ref[rows, cols], low)
            stack_heads(ds, do_ref[rows, cols], low)
            scores = jnp.where(hidden, -jnp.inf, nt(k_rows, qs[ALL]))
            top = max_rows(scores)
            e = jnp.exp((scores - top) * 0.125)
            probs = e * (1.0 / sum_rows(e))
            d_probs = nt(v_rows, ds[ALL])
            inner = sum_rows(d_probs * probs)
            d_scores = (probs * (d_probs - inner) * 0.125).astype(BF)
            grad_v = nn(probs.astype(BF), ds[ALL])
            grad_k = nn(d_scores, qs[ALL])
            folded = nn(jnp.transpose(k_rows), d_scores)
            grad_q = jnp.transpose(jnp.where(low_rows, folded[:, 0:SPAN], folded[:, SPAN:TILE]))[:PAD]
            for third, value in enumerate((grad_q, grad_k, grad_v)):
                rounded = value.astype(BF)
                grads[third, rows, cols] = rounded
                by_core[rows, p * TRIPLE + third * LANES:p * TRIPLE + third * LANES + LANES] = rounded
                out.append(sum_rows(value))
        return tuple(t + n for t, n in zip(sums, out))

    zero = jnp.zeros((ONE, LANES), F32)
    bias_sums = loop(SEQS, seq, (zero,) * 6, unroll=SEQS)
    for p in SIDES:
        for third in range(THIRDS):
            at = pl.multiple_of(third * WIDTH + g * GROUP + p * LANES, LANES)
            biases[:, pl.ds(at, LANES)] = bias_sums[3 * p + third]
    poll(((2, 3), (1, 1), (0, 0)))
    stage = g + 1

    ring.reopen_box()

    w = nn(turned[ALL], by_core[ALL])
    for part in range(THIRDS):
        both = [w[:, at:at + LANES].reshape(CUBE + BLOCK) for at in (part * LANES, TRIPLE + part * LANES)]
        ring.outbox[part] = jnp.where(rep == 0, both[1], both[0])
        ring.acc[stage % ATT_SLOTS, part] = jnp.where(rep == 0, both[0], both[1])
    for part in range(THIRDS):
        ring.pair(part).start()

    def chunk(i, carry):
        at = pl.ds(pl.multiple_of(i * CHUNK, PACK), CHUNK)
        dh[at, :] += nt(grads[0, at, :], wq_ref[ALL]) + nt(grads[1, at, :], wk_ref[ALL]) + nt(grads[2, at, :], wv_ref[ALL])
        return carry

    loop(ROWS // CHUNK, chunk, 0)

    def exchange(dim, landing, at, number):
        copies = []
        for hops in range(1, 4):
            index = list(at)
            index[dim] = (place[dim] + hops) % RING
            copies.append(pltpu.make_async_remote_copy(
                src_ref=blocks.at[tuple(index)], dst_ref=landing.at[hops - 1], send_sem=small_send.at[number + hops],
                recv_sem=small_recv.at[number + hops], device_id=(rep, flat_of(along(place, dim, hops))),
                device_id_type=MESH_ID))
        return copies

    def start(copies):
        for copy in copies:
            copy.start()
        return copies

    def collect(copies, dim, landing, at):
        for copy in copies:
            copy.wait()
        index = list(at)
        index[dim] = place[dim]
        index = tuple(index)
        blocks[index] = blocks[index] + landing[0] + landing[1] + landing[2]

    @pl.when(g == GROUPS - 1)
    def _():
        def tail(*todo):
            for stage, at in todo:
                level(stage, orders, at)

        gain = vec_ref[:1, :]
        tail((2, 2), (3, 1), (4, 0))
        sums[ALL] = gvin_ref[ALL]
        for s in range(SEQS):
            padded(xp, 0, x_ref, s)
            here = pl.ds(s * PAD, PAD)
            centered, rstd = row_stats(xp[ALL])
            xhat = centered * rstd
            d = dh[here, :]
            dxp[ALL] = (gr_ref[here, :] + norm_back(d * gain, xhat, rstd)).astype(BF)
            for k, value in enumerate((d * xhat, d)):
                sums[k:k + 1, :] += sum_rows(value)
            dx_ref[s] = dxp[:TOKENS]
            if s == 3:
                tail((2, 3), (3, 2))
        small_blocks(blocks, sums, biases, gbup_ref)
        at = [EVERY] * 3
        number = 0
        for dim, landing, todo in ((2, from_x, ((4, 1),)), (1, from_y, ((3, 3),)), (0, from_z, ((4, 2),))):
            copies = start(exchange(dim, landing, at, number))
            tail(*todo)
            collect(copies, dim, landing, at)
            at[dim] = place[dim]
            number += 3
        last = pltpu.make_async_remote_copy(
            src_ref=blocks.at[place], dst_ref=from_pair, send_sem=small_send.at[FIRST], recv_sem=small_recv.at[FIRST],
            device_id=ring.partner, device_id_type=MESH_ID)
        last.start()
        tail((4, 3))
        last.wait()
        small_ref[ALL] = blocks[place] + from_pair[ALL]
        ring.settle(0, first_orders)
        for stage in range(1, ATT_STAGES):
            ring.settle(stage, orders)


def attn_bwd(qkv, do, h, w_qkv, o, da, x, gr, vec, gvin, gbup):
    one = lambda shape: pl.BlockSpec(shape, lambda g: (0,) * len(shape), pipeline_mode=ONCE)
    third = lambda t: pl.BlockSpec((ROWS, GROUP), lambda g: (0, t * GROUPS + g))
    wthird = lambda t: pl.BlockSpec((WIDTH, GROUP), lambda g: (0, t * GROUPS + g))
    col = pl.BlockSpec((ROWS, GROUP), lambda g: (0, g))
    anywhere = ANYWHERE
    shape = jax.ShapeDtypeStruct
    rows = (SUBS, LANES)
    vmem, dma = VM, pltpu.SemaphoreType.DMA
    return pl.pallas_call(
        attn_bwd_kernel, grid=(GROUPS,),
        out_shape=[shape((PACK, 3 * WIDTH), F32), shape((PACK, WIDTH), F32), shape((SEQS, TOKENS, WIDTH), BF), shape(rows, F32)],
        in_specs=[third(0), third(1), third(2), col, one((ROWS, WIDTH)), wthird(0), wthird(1), wthird(2),
                  one((ROWS, WIDTH)), one((ROWS, WIDTH)), one((SEQS, TOKENS, WIDTH)), one((ROWS, WIDTH)),
                  one((SUBS, WIDTH)), one((SUBS, WIDTH)), one((SUBS, TILE))],
        out_specs=[anywhere, anywhere, one((SEQS, TOKENS, WIDTH)), one(rows)],
        scratch_shapes=[vmem((ROWS, WIDTH), F32), vmem((THIRDS, ROWS, GROUP), BF), vmem((ROWS, 3 * GROUP), BF),
                        vmem((WIDTH, ROWS), BF), vmem((2, TILE, LANES), BF), vmem((2, TILE, LANES), BF),
                        vmem((PAD, WIDTH), F32), vmem((PAD, WIDTH), BF), vmem((SUBS, WIDTH), F32), vmem((1, 3 * WIDTH), F32),
                        vmem(CUBE + rows, F32), vmem((3, 4, 4) + rows, F32), vmem((3, 4) + rows, F32),
                        vmem((3,) + rows, F32), vmem(rows, F32), dma((10,)), dma((10,))]
        + ring_scratch(ATT_SLOTS, ATT_STAGES, ATT_PARTS),
        compiler_params=pltpu.CompilerParams(vmem_limit_bytes=VMEM_CAP, collective_id=2, has_side_effects=True),
        name="attn_bwd",
    )(qkv, qkv, qkv, do, h, w_qkv, w_qkv, w_qkv, o, da, x, gr, vec, gvin, gbup)


def tiled(t, inner):
    rows = t.shape[0]
    return t.reshape(rows, -1, inner, SUBS).swapaxes(1, 2).reshape(rows, HIDDEN)


def layer(x, dz, w_qkv, b_qkv, w_out, w_up, b_up, w_down, vec_params):
    h1, qkv, o, a, h2, dm, vec, b_up, w_qkv, w_out, w_up, w_down = first(
        x, dz, (w_qkv, w_out, tiled(w_up, SUBS), w_down), (b_qkv[None], b_up.reshape(SUBS, SUBS), vec_params))
    w_qkv, w_out, w_up = (w.reshape(WIDTH, -1) for w in (w_qkv, w_out, w_up))
    gw_up, gw_down, gb_up, z, gr, da, do, gvec = mlp(h2, dm, w_up, b_up, w_down, x, dz, a, w_out, vec)
    gw_qkv, gw_out, dx, small = attn_bwd(qkv, do, h1, w_qkv, o, da, x, gr, vec, gvec, gb_up)
    return (z, dx, gw_qkv, small[0, 16:SHARDS], gw_out, tiled(gw_up, SHARDS), small[:, 64:72].reshape(SHARDS), gw_down,
            small[:, 0:PACK])


def solution(mesh):
    batch = P(("rep", "fsdp"), None, None)
    rows, flat = P("fsdp", None), P("fsdp")
    params = (rows, flat, rows, rows, flat, rows, P(None, "fsdp"))
    return jax.shard_map(layer, mesh=mesh, in_specs=(batch, batch) + params, out_specs=(batch, batch) + params, check_vma=False)
```

```python
import jax
import jax.numpy as jnp
from jax import lax
from jax.experimental import pallas as pl
from jax.experimental.pallas import tpu as pltpu
from jax.sharding import PartitionSpec as P

LN_EPS = 1e-5

ALL = ...
FIRST, ONE = 0, 1
PACK, SHARDS, FLAT, LANES, SPAN, TRIPLE, TILE = 16, 64, 192, 128, 256, 384, 512
SUBS, RING = 8, 4
CUBE, BLOCK = (RING,) * 3, (2, SUBS, LANES)
AXES, SIDES = range(3), range(2)
ONCE = pl.Buffered(ONE)
ANYWHERE = pl.BlockSpec(memory_space=pl.ANY)
VM = pltpu.VMEM
KEEP = True
MIN = float("-inf")


def row(ref, k):
    return ref[k:k + ONE, :]


def other(rep):
    return ONE - rep


def iota(dims, axis):
    return lax.broadcasted_iota(jnp.int32, dims, axis)


def loop(count, body, start, **options):
    return lax.fori_loop(FIRST, count, body, start, **options)


def sum_rows(t):
    return jnp.sum(t, axis=FIRST, keepdims=KEEP)


def max_rows(t):
    return jnp.max(t, axis=FIRST, keepdims=KEEP)


def sum_lanes(t):
    return jnp.sum(t, axis=-ONE, keepdims=KEEP)


def max_lanes(t):
    return jnp.max(t, axis=-ONE, keepdims=KEEP)


def mean_lanes(t):
    return jnp.mean(t, axis=-ONE, keepdims=KEEP)


SEQS, TOKENS, PAD, WIDTH, HIDDEN = 6, 197, 208, 1024, 4096
ROWS = SEQS * PAD
BF, F32 = jnp.bfloat16, jnp.float32
VMEM_CAP = 67043328


def nn(a, b):
    return lax.dot_general(a, b, (((1,), (0,)), ((), ())), preferred_element_type=F32)


def nt(a, b):
    return lax.dot_general(a, b, (((1,), (1,)), ((), ())), preferred_element_type=F32)


def tn(a, b):
    return lax.dot_general(a, b, (((0,), (0,)), ((), ())), preferred_element_type=F32)


def row_stats(t):
    mean = mean_lanes(t)
    centered = t - mean
    variance = mean_lanes(centered * centered)
    return centered, lax.rsqrt(variance + LN_EPS)


def norm_back(dt, xhat, rstd):
    return rstd * (dt - mean_lanes(dt) - xhat * mean_lanes(dt * xhat))


def head_halves(width=LANES):
    lane = iota((1, width), 1)
    return lane < SHARDS


def stack_heads(dst, rows, low):
    zero = jnp.zeros_like(rows)
    dst[:PAD] = jnp.where(low, rows, zero)
    dst[SPAN:SPAN + PAD] = jnp.where(low, zero, rows)


def padded(dst, base, rows_ref, s):
    dst[base + FLAT:base + PAD] = jnp.zeros((PACK, WIDTH), dst.dtype)
    dst[base:base + TOKENS] = rows_ref[s].astype(dst.dtype)


MESH_ID = pl.DeviceIdType.MESH
ORDERS = ((2, 1, 0), (1, 0, 2), (0, 2, 1))
HOPS = (1, 2, 3)
GREETED = 10
FAR, NEAR, DIRECT = "far", "near", "direct"
EVERY = slice(None)


def my_place():
    rep, flat = lax.axis_index("rep"), lax.axis_index("fsdp")
    return rep, (flat // PACK, (flat // RING) % RING, flat % RING)


def along(place, dim, shift):
    moved = list(place)
    moved[dim] = (place[dim] + shift) % RING
    return tuple(moved)


def flat_of(place):
    return place[0] * PACK + place[1] * 4 + place[2]


def greet(sem, rep, place):
    pl.semaphore_signal(sem, inc=1, device_id=(other(rep), flat_of(place)), device_id_type=MESH_ID)
    for dim in AXES:
        for shift in HOPS:
            pl.semaphore_signal(sem, inc=1, device_id=(rep, flat_of(along(place, dim, shift))), device_id_type=MESH_ID)


def entry_barrier(rep, place):
    barrier = pltpu.get_barrier_semaphore()
    greet(barrier, rep, place)
    pl.semaphore_wait(barrier, GREETED)


def ring_scratch(slots, stages, parts):
    dma = pltpu.SemaphoreType.DMA
    block = BLOCK
    cube, square, line = CUBE, CUBE[1:], CUBE[2:]
    sides = (parts, 3)
    buffers = [(slots, parts) + cube + block, (parts,) + cube + block, (parts,) + cube + block,
               (stages, parts) + square + block,
               (slots,) + sides + square + block, (stages,) + sides + line + block, (stages,) + sides + block]
    sems = [(parts,)] * 2 + [(slots, parts, 5)] * 2 + [(stages, parts, 6)] * 2 + [(stages, parts)] * 3
    regular = pltpu.SemaphoreType.REGULAR
    return [VM(b, F32) for b in buffers] + [dma(s) for s in sems] + [regular((slots,)), regular]


class Ring:
    def __init__(self, refs, slots, steps, window):
        (self.acc, self.inbox, self.outbox, self.rest, land0, land1, land2, self.pair_send, self.pair_recv,
         self.send, self.recv, self.rest_send, self.rest_recv, self.out_sem, self.out_send, self.out_recv,
         self.free, self.emptied) = refs
        self.landing = (land0, land1, land2)
        self.slots, self.steps, self.last = slots, steps, len(steps)
        self.window = window
        self.rep, self.place = my_place()
        self.partner = (other(self.rep), flat_of(self.place))

    def pair(self, part):
        return pltpu.make_async_remote_copy(
            src_ref=self.outbox.at[part], dst_ref=self.inbox.at[part], send_sem=self.pair_send.at[part],
            recv_sem=self.pair_recv.at[part], device_id=self.partner, device_id_type=MESH_ID)

    def axis(self, order, phase, index):
        at = {dim: EVERY for dim in order}
        for dim in order[:phase]:
            at[dim] = self.place[dim]
        at[order[phase]] = index
        if phase:
            del at[order[0]]
        return tuple(at[dim] for dim in sorted(at))

    def home(self, stage, part, phase):
        if phase:
            return self.rest, (stage, part), self.rest_send, self.rest_recv
        return self.acc, (stage % self.slots, part), self.send, self.recv

    def hops(self, stage, part, order, step):
        phase, kind = step
        dim = order[phase]
        memory, at, send, recv = self.home(stage, part, phase)
        found = []
        for side, shift in enumerate((1, 3) if kind != DIRECT else HOPS):
            number = side
            source, target, place = shift, 0, at + (side,)
            if kind == FAR:
                source, target = 2, shift
            if kind == NEAR:
                number = side + 2
            if phase == 2:
                number = side + 3
            src = at + self.axis(order, phase, (self.place[dim] + source) % RING)
            into = at + self.axis(order, phase, (self.place[dim] + target) % RING)
            if kind == FAR:
                src, into, place = src + (side,), into + (side,), at + (2,) + (EVERY, EVERY, side)
            copy = pltpu.make_async_remote_copy(
                src_ref=memory.at[src], dst_ref=self.landing[phase].at[place], send_sem=send.at[at + (number,)],
                recv_sem=recv.at[at + (number,)], device_id=(self.rep, flat_of(along(self.place, dim, shift))),
                device_id_type=MESH_ID)
            found.append((copy, into, place))
        return found

    def results(self, stage, part, order):
        at = (stage, part)
        src = self.rest.at[at + tuple(self.place[dim] for dim in sorted(order[1:]))]
        dst = self.window(stage, part)
        return (pltpu.make_async_copy(src, dst, self.out_sem.at[at]),
                pltpu.make_async_remote_copy(
                    src_ref=src, dst_ref=dst, send_sem=self.out_send.at[at], recv_sem=self.out_recv.at[at],
                    device_id=self.partner, device_id_type=MESH_ID))

    def level(self, stage, level, orders, credit, refill):
        if level == 0:
            for part in orders:
                self.pair(part).wait()
                at = (stage % self.slots, part)
                for z in range(4):
                    self.acc[at + (z,)] = self.acc[at + (z,)] + self.inbox[part, z]

            @pl.when(stage >= self.slots)
            def _():
                pl.semaphore_wait(self.free.at[stage % self.slots], GREETED)

            @pl.when(refill)
            def _():
                pl.semaphore_signal(self.emptied, inc=1, device_id=self.partner, device_id_type=MESH_ID)
        else:
            step = self.steps[level - 1]
            phase, kind = step
            for part, order in orders.items():
                memory = self.home(stage, part, phase)[0]
                hops = self.hops(stage, part, order, step)
                for copy, _, _ in hops:
                    copy.wait_recv()
                if kind == FAR:
                    for _, into, place in hops:
                        memory[into] = memory[into] + self.landing[phase][place]
                    continue
                into = hops[0][1]
                total = memory[into]
                for _, _, place in hops:
                    total = total + self.landing[phase][place]
                if phase:
                    memory[into] = total
                else:
                    self.rest[stage, part] = total
            if phase == 0 and kind != FAR:
                self.sent(stage, orders, (0,))

                @pl.when(credit)
                def _():
                    greet(self.free.at[stage % self.slots], self.rep, self.place)
        for part, order in orders.items():
            if level < self.last:
                for copy, _, _ in self.hops(stage, part, order, self.steps[level]):
                    copy.start()
            else:
                for copy in self.results(stage, part, order):
                    copy.start()
        if level == self.last:
            self.sent(stage, orders, (1, 2))

    def sent(self, stage, orders, phases):
        for step in self.steps:
            if step[0] in phases:
                for part, order in orders.items():
                    for copy, _, _ in self.hops(stage, part, order, step):
                        copy.wait_send()

    def settle(self, stage, orders):
        for part, order in orders.items():
            for copy in self.results(stage, part, order):
                copy.wait()

    def reopen_box(self):
        pl.semaphore_wait(self.emptied, 1)


PIECE = TILE
QKV, OUT, UP, DOWN, SMALL = range(5)


def gather_items():
    rest = [(OUT, 0, 0, PIECE)]
    rest += [(UP, 0, PIECE * j, HIDDEN // 2) for j in range(4)]
    rest += [(DOWN, PACK * j, 0, PIECE) for j in range(4)]
    items = [(0, QKV, 0, PIECE * j, 3 * PIECE, ORDERS[j]) for j in AXES] + [(0, SMALL, 0, 0, 0, ORDERS[0])]
    return items + [(1 + k // 3,) + piece + (ORDERS[k % 3],) for k, piece in enumerate(rest)]


def small_rows(table, vec, b_qkv, b_up):
    lane = iota((SUBS, LANES), 1)

    def moved(f, half, shift):
        return pltpu.roll(table[f // PACK, f // RING % RING, f % RING, half], shift % LANES, 1)

    def fill(ref, tile, owners, half, width, first):
        total = jnp.zeros((SUBS, LANES), F32)
        for f in owners:
            start = width * f - LANES * tile
            here = jnp.logical_and(lane >= start, lane < start + width)
            total = jnp.where(here, moved(f, half, start - first), total)
        ref[:, tile * LANES:tile * LANES + LANES] = total[:ref.shape[0]]

    for tile in range(WIDTH // LANES):
        fill(vec, tile, range(SUBS * tile, SUBS * tile + SUBS), 0, PACK, 0)
    for tile in range(TILE // LANES):
        fill(b_up, tile, range(PACK * tile, PACK * tile + PACK), 1, SUBS, 0)
    for tile in range(3 * WIDTH // LANES):
        fill(b_qkv, tile, range(LANES * tile // 48, (LANES * tile + LANES - 1) // 48 + 1), 0, 48, PACK)


def placed(values, first, period=LANES):
    size = values.shape[ONE]
    lane = iota((size, LANES), 1)
    row = iota((size, LANES), 0)
    return nn(values.astype(BF), jnp.where(lane == row % period + first, 1.0, 0.0).astype(BF))


def unit_columns(j):
    column = iota((WIDTH, LANES), 1)
    row = iota((WIDTH, LANES), 0)
    taken = row == SHARDS * (column // SUBS) + SUBS * j + column % SUBS
    return jnp.where(taken, 1.0, 0.0).astype(BF)


def first_kernel(x_ref, dz_ref, sq_ref, so_ref, su_ref, sd_ref, bq_ref, bu_ref, sv_ref,
                 h1_ref, qkv_ref, o_ref, a_ref, h2_ref, dm_ref, vec_ref, bup_ref, wq_hbm, wo_hbm, wu_hbm, wd_hbm,
                 wq, wo, su, sd, packed, table, bias, xhat, kst, vst, xp,
                 own_sem, send_sem, recv_sem, pair_send, pair_recv, save_sem):
    t = pl.program_id(0)
    rep, place = my_place()
    partner = (other(rep), flat_of(place))
    items = gather_items()
    fulls = (wq, wo, wu_hbm, wd_hbm, table)

    def block(item, shards, half=None):
        _, array, row, first, step, _ = items[item]
        if array == SMALL:
            return table.at[shards + ((half,) if half is not None else ())]
        col, cols = rep * step + first, PIECE
        if half is not None:
            col, cols = col + half * (PIECE // 2), PIECE // 2
        return fulls[array].at[shards + (pl.ds(row, PACK), pl.ds(pl.multiple_of(col, LANES), cols))]

    def shard(item):
        _, array, row, first, step, _ = items[item]
        return (su, sd)[array - UP].at[pl.ds(row, PACK), pl.ds(pl.multiple_of(rep * step + first, LANES), PIECE)]

    def own(item):
        return pltpu.make_async_copy(shard(item), block(item, place), own_sem.at[item])

    def pair(item):
        everywhere = block(item, (EVERY,) * 3)
        return pltpu.make_async_remote_copy(
            src_ref=everywhere, dst_ref=everywhere, send_sem=pair_send.at[item], recv_sem=pair_recv.at[item],
            device_id=partner, device_id_type=MESH_ID)

    def hops(item, level):
        array, order = items[item][1], items[item][-1]
        phase, second = level // 2, level % 2
        dim = order[phase]
        found = []
        for side, shift in enumerate((1, 3)):
            at = [EVERY] * 3
            for later in order[phase:]:
                at[later] = place[later]
            if second:
                at[dim] = (place[dim] + 4 - shift) % RING
            dst = block(item, tuple(at), side if second else None)
            src = shard(item) if level == 0 and array in (UP, DOWN) else dst
            number = 2 * level + side
            found.append(pltpu.make_async_remote_copy(
                src_ref=src, dst_ref=dst, send_sem=send_sem.at[item, number], recv_sem=recv_sem.at[item, number],
                device_id=(rep, flat_of(along(place, dim, shift))), device_id_type=MESH_ID))
        return found

    def advance(*todo):
        for stage, level in todo:
            for item in range(len(items)):
                if items[item][0] != stage:
                    continue
                if level:
                    for copy in hops(item, level - 1):
                        copy.wait_recv()
                if level == 2 and items[item][1] in (UP, DOWN):
                    own(item).wait()
                if level == 6:
                    if items[item][1] != SMALL:
                        pair(item).start()
                else:
                    for copy in hops(item, level):
                        copy.start()

    def arrived(*arrays):
        for item in range(len(items)):
            if items[item][1] in arrays:
                pair(item).wait_recv()

    def saves():
        return (pltpu.make_async_copy(wq, wq_hbm, save_sem.at[FIRST]), pltpu.make_async_copy(wo, wo_hbm, save_sem.at[1]))

    @pl.when(t == FIRST)
    def _():
        for full, piece, half in ((wq, sq_ref, 3 * PIECE), (wo, so_ref, PIECE)):
            cols = pl.ds(pl.multiple_of(rep * half, LANES), half)
            full[place + (EVERY, cols)] = piece[:, cols].astype(BF)
        for b in range(4):
            packed[b * 16:b * PACK + PACK] = su_ref[:, b * WIDTH:b * WIDTH + WIDTH].astype(BF)
        sd[ALL] = sd_ref[ALL].astype(BF)
        first_row = iota((SUBS, 48), 0) == 0
        table[place + (0,)] = placed(sv_ref[ALL], 0) + placed(jnp.where(first_row, bq_ref[ALL], 0.0), PACK)
        unit = iota((SUBS, SHARDS), 1) // SUBS == iota((SUBS, SHARDS), 0)
        table[place + (1,)] = placed(jnp.where(unit, bu_ref[ALL], 0.0), 0, SUBS)
        entry_barrier(rep, place)
        advance((0, 0))
        for j in range(SUBS):
            turned = nn(packed[ALL], unit_columns(j)).astype(BF)
            for b in range(4):
                su[:, j * TILE + b * LANES:j * TILE + b * LANES + LANES] = turned[b * 16:b * PACK + PACK]
        for item in range(len(items)):
            if items[item][1] in (UP, DOWN):
                own(item).start()
        for s in range(SEQS):
            base = s * PAD
            xp[FLAT:PAD] = jnp.zeros((PACK, WIDTH), BF)
            xp[:TOKENS] = x_ref[s]
            centered, rstd = row_stats(xp[ALL].astype(F32))
            xhat[base:base + PAD] = centered * rstd
            level = s + 1
            if s < 5:
                advance(*((stage, level - stage) for stage in range(min(level, 3) + 1)))
        advance((0, 6))
        small_rows(table, vec_ref, bias, bup_ref)
        real = iota((PAD, 1), 0) < TOKENS

        def scaled(s, carry):
            here = pl.ds(pl.multiple_of(s * PAD, PACK), PAD)
            h1_ref[here, :] = jnp.where(real, xhat[here, :] * vec_ref[:1, :] + row(vec_ref, 1), 0.0).astype(BF)
            return carry

        loop(SEQS, scaled, 0)
        kst[ALL] = jnp.zeros_like(kst)
        vst[ALL] = jnp.zeros_like(vst)

    @pl.when(t > FIRST)
    def _():
        base = pl.multiple_of((t - 1) * (2 * PAD), PACK)

        def qkv_tile(n, carry):
            cols = pl.ds(pl.multiple_of((rep * 3 + n) % 6 * PIECE, PIECE), PIECE)
            weights = wq[:, :, :, :, cols].reshape(WIDTH, PIECE)
            qkv_ref[:, cols] = (nn(h1_ref[pl.ds(base, 2 * PAD), :], weights) + bias[:, cols]).astype(BF)
            return carry

        loop(3, qkv_tile, 0)

        @pl.when(t == 1)
        def _():
            arrived(QKV)
            saves()[0].start()

        lax.fori_loop(3, 6, qkv_tile, 0)

    @pl.when(t == 1)
    def _():
        advance((1, 5), (2, 4), (3, 3))

    low = head_halves()
    visible = iota((1, SPAN), 1) < TOKENS

    def head_pair(p, carry):
        def cols(third):
            return pl.ds(pl.multiple_of(third * WIDTH + p * LANES, LANES), LANES)

        for s in SIDES:
            rows = pl.ds(s * PAD, PAD)
            stack_heads(kst.at[s], qkv_ref[rows, cols(1)], low)
            stack_heads(vst.at[s], qkv_ref[rows, cols(2)], low)
        for s in SIDES:
            rows = pl.ds(s * PAD, PAD)
            scores = nt(qkv_ref[rows, cols(0)], kst[s])
            probs = []
            for half in SIDES:
                part = jnp.where(visible, scores[:, half * SPAN:half * SPAN + SPAN], -jnp.inf)
                top = max_lanes(part)
                e = jnp.exp((part - top) * 0.125)
                probs.append((e * (1.0 / sum_lanes(e))).astype(BF))
            o_ref[rows, pl.ds(pl.multiple_of(p * LANES, LANES), LANES)] = nn(jnp.concatenate(probs, axis=1), vst[s]).astype(BF)
        return carry

    def two_pairs(i, carry):
        head_pair(2 * i, carry)
        head_pair(2 * i + 1, carry)
        for step, turn, todo in ((1, 0, ((1, 6),)), (2, 1, ((3, 5),)), (1, 2, ((2, 5), (3, 4))), (2, 3, ((3, 6),))):
            @pl.when(jnp.logical_and(t == step, i == turn))
            def _(todo=todo):
                advance(*todo)

        return carry

    @pl.when(t > FIRST)
    def _():
        loop(4, two_pairs, 0)

    @pl.when(t == 1)
    def _():
        arrived(OUT)
        saves()[1].start()

    @pl.when(t > FIRST)
    def _():
        for s in SIDES:
            padded(xp, 0, x_ref, 2 * (t - 1) + s)
            xhat[s * PAD:s * PAD + PAD] = xp[ALL].astype(F32)
            dm_ref[s * PAD + FLAT:s * PAD + PAD] = jnp.zeros((PACK, WIDTH), BF)
            dm_ref[s * PAD:s * PAD + TOKENS] = (dz_ref[s].astype(F32) * row(vec_ref, 7)).astype(BF)
        a_ref[ALL] = nn(o_ref[ALL], wo[ALL].reshape(WIDTH, WIDTH)) + row(vec_ref, 2)

        def rows(i, carry):
            at = pl.ds(pl.multiple_of(i * 32, 32), 32)
            y = xhat[at, :] + row(vec_ref, 3) * a_ref[at, :]
            centered, rstd = row_stats(y)
            h2_ref[at, :] = (centered * rstd * row(vec_ref, 4) + row(vec_ref, 5)).astype(BF)
            return carry

        loop(2 * PAD // 32, rows, 0, unroll=13)

    @pl.when(t == 1)
    def _():
        advance((2, 6))

    @pl.when(t == 3)
    def _():
        arrived(UP, DOWN)
        for item in range(len(items)):
            if items[item][1] != SMALL:
                pair(item).wait_send()
            for level in range(6):
                for copy in hops(item, level):
                    copy.wait_send()
        for copy in saves():
            copy.wait()


def first(x, dz, shards, small):
    whole = lambda dims: pl.BlockSpec(dims, lambda t: (0,) * len(dims), pipeline_mode=ONCE)
    pair = lambda t: jnp.maximum(t - 1, 0)
    rows = lambda width: pl.BlockSpec((2 * PAD, width), lambda t: (pair(t), 0))
    anywhere = ANYWHERE
    shape, vmem, dma = jax.ShapeDtypeStruct, VM, pltpu.SemaphoreType.DMA
    n = len(gather_items())
    cube = CUBE
    return pl.pallas_call(
        first_kernel, grid=(4,),
        out_shape=[shape((ROWS, WIDTH), BF), shape((ROWS, 3 * WIDTH), BF), shape((ROWS, WIDTH), BF), shape((ROWS, WIDTH), F32),
                   shape((ROWS, WIDTH), BF), shape((ROWS, WIDTH), BF), shape((SUBS, WIDTH), F32), shape((SUBS, TILE), F32)]
        + [shape(cube + s.shape, BF) for s in shards],
        in_specs=[whole((SEQS, TOKENS, WIDTH)), pl.BlockSpec((2, TOKENS, WIDTH), lambda t: (pair(t), 0, 0))]
        + [whole(s.shape) for s in shards + small],
        out_specs=[whole((ROWS, WIDTH)), rows(3 * WIDTH), rows(WIDTH), rows(WIDTH), rows(WIDTH), rows(WIDTH),
                   whole((SUBS, WIDTH)), whole((SUBS, TILE))] + [anywhere] * 4,
        scratch_shapes=[vmem(cube + shards[QKV].shape, BF), vmem(cube + shards[OUT].shape, BF), vmem(shards[UP].shape, BF),
                        vmem(shards[DOWN].shape, BF), vmem((SHARDS, WIDTH), BF), vmem(cube + (2, SUBS, LANES), F32), vmem((1, 3 * WIDTH), F32),
                        vmem((ROWS, WIDTH), F32), vmem((2, PIECE, LANES), BF), vmem((2, PIECE, LANES), BF),
                        vmem((PAD, WIDTH), BF),
                        dma((n,)), dma((n, 12)), dma((n, 12)), dma((n,)), dma((n,)), dma((2,))],
        compiler_params=pltpu.CompilerParams(vmem_limit_bytes=VMEM_CAP, collective_id=0, has_side_effects=True),
        name="first",
    )(x, dz, *shards, *small)


CHUNK = 624
TILES = HIDDEN // TILE
MLP_SLOTS, MLP_PARTS = 3, 4
MLP_STEPS = ((0, FAR), (0, NEAR), (1, DIRECT), (2, DIRECT))


def gelu_and_slope(u):
    cdf = 0.5 * (1.0 + lax.erf(u * (2.0 ** -0.5)))
    pdf = jnp.exp(u * u * -0.5) * ((2.0 * jnp.pi) ** -0.5)
    return u * cdf, cdf + u * pdf


def mlp_kernel(h_ref, dm_ref, w1_ref, w2_ref, b1_ref, x_ref, dz_ref, a_ref, wo_ref, vec_ref,
               gw1_ref, gw2_ref, gb_ref, z_ref, gr_ref, da_ref, do_ref, gv_ref,
               m_acc, dh_acc, act, dpre, turned, xp, zp, zo, *ring_refs):
    j = pl.program_id(0)

    def window(stage, part):
        if part < 2:
            return gw2_ref.at[stage, pl.ds(rep * 4 + part * 2, 2)]
        return gw1_ref.at[:, stage * 4 + rep * 2 + part - 2]

    ring = Ring(ring_refs, MLP_SLOTS, MLP_STEPS, window)
    rep = ring.rep
    every_part = range(MLP_PARTS)

    def run(lag, level):
        stage = j - lag
        for turn in AXES:
            orders = {part: ORDERS[(turn + part) % 3] for part in every_part}

            @pl.when(jnp.logical_and(jnp.logical_and(stage >= 0, stage < TILES), stage % 3 == turn))
            def _(orders=orders):
                ring.level(stage, level, orders, stage < TILES - MLP_SLOTS, stage < TILES - 1)

    @pl.when(j == FIRST)
    def _():
        entry_barrier(rep, ring.place)
        m_acc[ALL] = jnp.zeros_like(m_acc)
        dh_acc[ALL] = jnp.zeros_like(dh_acc)
        turned[ALL] = jnp.transpose(h_ref[ALL])

    def chunk(i, total):
        at = pl.ds(pl.multiple_of(i * CHUNK, PACK), CHUNK)
        w1, w2 = w1_ref[ALL], w2_ref[ALL].reshape(TILE, WIDTH)
        u = nn(h_ref[at, :], w1) + b1_ref[pl.ds(j, 1), :]
        value, slope = gelu_and_slope(u)
        act[at, :] = value.astype(BF)
        d = nt(dm_ref[at, :], w2) * slope
        dpre[at, :] = d.astype(BF)
        m_acc[at, :] += nn(act[at, :], w2)
        dh_acc[at, :] += nt(dpre[at, :], w1)
        return sum_rows(d) + total

    def grads(core, target):
        cols = pl.ds(pl.multiple_of(core * TILE, TILE), TILE)
        g = tn(act[ALL], dm_ref[:, cols])
        for part in SIDES:
            for half in SIDES:
                first = (part * 2 + half) * LANES
                target(part, half, g[:, first:first + LANES].reshape(CUBE + BLOCK[1:]))

    def grads_up(core, target):
        g = nn(turned[ALL], dpre[:, pl.ds(pl.multiple_of(core * SPAN, SPAN), SPAN)])
        for part in SIDES:
            target(part + 2, EVERY, g[:, part * LANES:part * LANES + LANES].reshape(CUBE + BLOCK))

    @pl.when(j < TILES)
    def _():
        gb_ref[pl.ds(j, 1), :] = loop(ROWS // CHUNK, chunk, jnp.zeros((1, TILE), F32))

    @pl.when(j == TILES)
    def _():
        gv_ref[ALL] = jnp.zeros_like(gv_ref)

    @pl.when(j >= TILES)
    def _():
        padded(xp, 0, x_ref, 0)
        padded(zp, 0, dz_ref, 0)
        s1, g2, b2, s2 = (vec_ref[k:k + 1, :] for k in (3, 4, 6, 7))
        here = pl.ds(pl.multiple_of((j - TILES) * PAD, PACK), PAD)
        a = a_ref[ALL]
        y = xp[ALL].astype(F32) + s1 * a
        mlp_out = m_acc[here, :] + b2
        g_out = zp[ALL].astype(F32)
        zo[ALL] = (y + s2 * mlp_out).astype(BF)
        centered, rstd = row_stats(y)
        xhat = centered * rstd
        dh = dh_acc[here, :]
        g_resid = g_out + norm_back(dh * g2, xhat, rstd)
        d_att = g_resid * s1
        gr_ref[ALL] = g_resid
        da_ref[ALL] = d_att.astype(BF)
        for k, total in enumerate((d_att, g_resid * a, dh * xhat, dh, g_out * s2, g_out * mlp_out)):
            gv_ref[2 + k:3 + k, :] += sum_rows(total)
        z_ref[0] = zo[:TOKENS]
        do_ref[ALL] = nt(da_ref[ALL], wo_ref[ALL]).astype(BF)

    for lag in range(ring.last + 1, 0, -1):
        run(lag, lag - 1)

    @pl.when(j < TILES)
    def _():
        slot = j % MLP_SLOTS

        def out(part, half, value):
            ring.outbox[part, :, :, :, half] = value

        def own(part, half, value):
            ring.acc[slot, part, :, :, :, half] = value

        grads(other(rep), out)
        grads_up(other(rep), out)

        @pl.when(j >= 1)
        def _():
            ring.reopen_box()

        for part in every_part:
            ring.pair(part).start()
        grads(rep, own)
        grads_up(rep, own)

    @pl.when(j == TILES + SEQS - 1)
    def _():
        for stage in range(TILES):
            ring.settle(stage, {part: ORDERS[(stage + part) % 3] for part in every_part})


def mlp(h, dm, w1, b1, w2, x, dz, a, w_out, vec):
    whole = lambda shape: pl.BlockSpec(shape, lambda j: (0, 0), pipeline_mode=ONCE)
    tile = lambda j: jnp.minimum(j, TILES - 1)
    seq = lambda j: jnp.maximum(j - TILES, 0)
    b1_spec = whole((SUBS, TILE))
    seqs = pl.BlockSpec((1, TOKENS, WIDTH), lambda j: (seq(j), 0, 0))
    rows = pl.BlockSpec((PAD, WIDTH), lambda j: (seq(j), 0))
    anywhere = ANYWHERE
    shape = jax.ShapeDtypeStruct
    return pl.pallas_call(
        mlp_kernel, grid=(TILES + SEQS,),
        out_shape=[shape((2, HIDDEN // LANES, SUBS, LANES), F32), shape((SUBS, SUBS, SUBS, LANES), F32), shape((SUBS, TILE), F32),
                   shape((SEQS, TOKENS, WIDTH), BF), shape((ROWS, WIDTH), F32), shape((ROWS, WIDTH), BF),
                   shape((ROWS, WIDTH), BF), shape((8, WIDTH), F32)],
        in_specs=[whole((ROWS, WIDTH)), whole((ROWS, WIDTH)), pl.BlockSpec((WIDTH, TILE), lambda j: (0, tile(j))),
                  pl.BlockSpec((SHARDS, SUBS, WIDTH), lambda j: (0, tile(j), 0)), b1_spec, seqs, seqs, rows,
                  whole((WIDTH, WIDTH)), whole((8, WIDTH))],
        out_specs=[anywhere, anywhere, whole((SUBS, TILE)), seqs, rows, rows, rows, whole((8, WIDTH))],
        scratch_shapes=[VM((ROWS, WIDTH), F32), VM((ROWS, WIDTH), F32), VM((ROWS, TILE), BF),
                        VM((ROWS, TILE), BF), VM((WIDTH, ROWS), BF), VM((PAD, WIDTH), BF),
                        VM((PAD, WIDTH), BF), VM((PAD, WIDTH), BF)] + ring_scratch(MLP_SLOTS, TILES, MLP_PARTS),
        compiler_params=pltpu.CompilerParams(vmem_limit_bytes=VMEM_CAP, collective_id=1, has_side_effects=True),
        name="mlp",
    )(h, dm, w1, w2.reshape(SHARDS, SHARDS, WIDTH), b1, x, dz, a, w_out, vec)


GROUP = SPAN
GROUPS = WIDTH // GROUP
THIRDS = 3
ATT_SLOTS, ATT_STAGES, ATT_PARTS = 2, GROUPS + 1, 4
ATT_STEPS = tuple((phase, DIRECT) for phase in AXES)


def small_blocks(target, vec, b_qkv, b_up):
    lane = iota((SUBS, LANES), 1)

    def turned(ref, tile, first, to):
        return pltpu.roll(ref[:, tile * LANES:tile * LANES + LANES], (to - first) % LANES, 1)

    for f in range(SHARDS):
        tile, first = divmod(48 * f, LANES)
        bias = turned(b_qkv, tile, first, PACK)
        if first + 48 > LANES:
            bias = jnp.where(lane[:1] < PACK + LANES - first, bias, turned(b_qkv, tile + 1, first, PACK))
        rows = turned(vec, f // SUBS, PACK * (f % SUBS), 0)
        up = turned(b_up, f // PACK, SUBS * (f % PACK), SHARDS)
        target[f // PACK, f // RING % RING, f % RING] = jnp.where(lane < PACK, rows, jnp.where(lane < SHARDS, bias, up))


def attn_bwd_kernel(q_ref, k_ref, v_ref, do_ref, h_ref, wq_ref, wk_ref, wv_ref, o_ref, da_ref, x_ref, gr_ref, vec_ref,
                    gvin_ref, gbup_ref, gup_ref, gw_ref, gwo_ref, dx_ref, small_ref, up_ref,
                    dh, grads, by_core, turned, qst, dst, xp, dxp, sums, biases, blocks, from_x, from_y, from_z, from_pair,
                    small_send, small_recv, *ring_refs):
    g = pl.program_id(0)

    def window(stage, part):
        if isinstance(stage, int) and stage == 0:
            return gwo_ref.at[:, rep * 4 + part]
        return gw_ref.at[:, part * SUBS + (stage - 1) * 2 + rep]

    ring = Ring(ring_refs, ATT_SLOTS, ATT_STEPS, window)
    rep, place = ring.rep, ring.place
    first_orders = {part: ORDERS[part % 3] for part in range(ATT_PARTS)}
    orders = {part: ORDERS[part] for part in range(THIRDS)}

    def level(stage, which, at):
        ring.level(stage, at, which, stage < ATT_STAGES - ATT_SLOTS, stage < ATT_STAGES - 1)

    def poll(todo):
        for lag, at in todo:
            @pl.when(g - lag >= 1)
            def _(lag=lag, at=at):
                level(g - lag, orders, at)

            @pl.when(g == lag)
            def _(at=at):
                level(0, first_orders, at)

    @pl.when(g == FIRST)
    def _():
        entry_barrier(rep, place)
        dh[ALL] = jnp.zeros_like(dh)
        qst[ALL] = jnp.zeros_like(qst)
        dst[ALL] = jnp.zeros_like(dst)
        turned[ALL] = jnp.transpose(h_ref[ALL])
        for core, box in ((other(rep), ring.outbox), (rep, ring.acc.at[FIRST])):
            w = tn(o_ref[ALL], da_ref[:, pl.ds(pl.multiple_of(core * TILE, TILE), TILE)])
            for part in range(ATT_PARTS):
                box[part] = w[:, part * LANES:part * LANES + LANES].reshape(CUBE + BLOCK)
            if box is ring.outbox:
                for part in range(ATT_PARTS):
                    ring.pair(part).start()

    poll(((2, 2),))
    low = head_halves()
    low_rows = iota((LANES, 1), 0) < SHARDS
    hidden = iota((PAD, 1), 0) >= TOKENS

    def seq(s, sums):
        rows = pl.ds(pl.multiple_of(s * PAD, PACK), PAD)
        out = []
        for p in SIDES:
            cols = slice(p * LANES, p * LANES + LANES)
            qs, ds = qst.at[p], dst.at[p]
            k_rows, v_rows = k_ref[rows, cols], v_ref[rows, cols]
            stack_heads(qs, q_ref[rows, cols], low)
            stack_heads(ds, do_ref[rows, cols], low)
            scores = jnp.where(hidden, -jnp.inf, nt(k_rows, qs[ALL]))
            top = max_rows(scores)
            e = jnp.exp((scores - top) * 0.125)
            probs = e * (1.0 / sum_rows(e))
            d_probs = nt(v_rows, ds[ALL])
            inner = sum_rows(d_probs * probs)
            d_scores = (probs * (d_probs - inner) * 0.125).astype(BF)
            grad_v = nn(probs.astype(BF), ds[ALL])
            grad_k = nn(d_scores, qs[ALL])
            folded = nn(jnp.transpose(k_rows), d_scores)
            grad_q = jnp.transpose(jnp.where(low_rows, folded[:, 0:SPAN], folded[:, SPAN:TILE]))[:PAD]
            for third, value in enumerate((grad_q, grad_k, grad_v)):
                rounded = value.astype(BF)
                grads[third, rows, cols] = rounded
                by_core[rows, p * TRIPLE + third * LANES:p * TRIPLE + third * LANES + LANES] = rounded
                out.append(sum_rows(value))
        return tuple(t + n for t, n in zip(sums, out))

    zero = jnp.zeros((ONE, LANES), F32)
    bias_sums = loop(SEQS, seq, (zero,) * 6, unroll=2)
    for p in SIDES:
        for third in range(THIRDS):
            at = pl.multiple_of(third * WIDTH + g * GROUP + p * LANES, LANES)
            biases[:, pl.ds(at, LANES)] = bias_sums[3 * p + third]
    poll(((2, 3), (1, 1), (0, 0)))
    stage = g + 1

    ring.reopen_box()

    w = nn(turned[ALL], by_core[ALL])
    for part in range(THIRDS):
        both = [w[:, at:at + LANES].reshape(CUBE + BLOCK) for at in (part * LANES, TRIPLE + part * LANES)]
        ring.outbox[part] = jnp.where(rep == 0, both[1], both[0])
        ring.acc[stage % ATT_SLOTS, part] = jnp.where(rep == 0, both[0], both[1])
    for part in range(THIRDS):
        ring.pair(part).start()

    def chunk(i, carry):
        at = pl.ds(pl.multiple_of(i * CHUNK, PACK), CHUNK)
        dh[at, :] += nt(grads[0, at, :], wq_ref[ALL]) + nt(grads[1, at, :], wk_ref[ALL]) + nt(grads[2, at, :], wv_ref[ALL])
        return carry

    loop(ROWS // CHUNK, chunk, 0)

    def exchange(dim, landing, at, number):
        copies = []
        for hops in range(1, 4):
            index = list(at)
            index[dim] = (place[dim] + hops) % RING
            copies.append(pltpu.make_async_remote_copy(
                src_ref=blocks.at[tuple(index)], dst_ref=landing.at[hops - 1], send_sem=small_send.at[number + hops],
                recv_sem=small_recv.at[number + hops], device_id=(rep, flat_of(along(place, dim, hops))),
                device_id_type=MESH_ID))
        return copies

    def start(copies):
        for copy in copies:
            copy.start()
        return copies

    def collect(copies, dim, landing, at):
        for copy in copies:
            copy.wait()
        index = list(at)
        index[dim] = place[dim]
        index = tuple(index)
        blocks[index] = blocks[index] + landing[0] + landing[1] + landing[2]

    @pl.when(g == GROUPS - 1)
    def _():
        def tail(*todo):
            for stage, at in todo:
                level(stage, orders, at)

        gain = vec_ref[:1, :]
        tail((2, 2), (3, 1), (4, 0))
        sums[ALL] = gvin_ref[ALL]
        def norm_one(s, carry):
            padded(xp, 0, x_ref, s)
            here = pl.ds(pl.multiple_of(s * PAD, PACK), PAD)
            centered, rstd = row_stats(xp[ALL])
            xhat = centered * rstd
            d = dh[here, :]
            dxp[ALL] = (gr_ref[here, :] + norm_back(d * gain, xhat, rstd)).astype(BF)
            for k, value in enumerate((d * xhat, d)):
                sums[k:k + 1, :] += sum_rows(value)
            dx_ref[s] = dxp[:TOKENS]

            @pl.when(s == 3)
            def _():
                tail((2, 3), (3, 2))

            return carry

        loop(SEQS, norm_one, 0)
        small_blocks(blocks, sums, biases, gbup_ref)
        at = [EVERY] * 3
        number = 0
        def shard_order():
            for j in range(SUBS):
                turned[:, j * LANES:j * LANES + LANES] = unit_columns(j)
                for b in range(4):
                    for h in SIDES:
                        xp[b * PACK + h * SUBS:b * PACK + h * SUBS + SUBS, j * LANES:j * LANES + LANES] = gup_ref[h, j * 4 + b]
            left = xp[:SHARDS]
            total = jnp.zeros_like(left)
            for _ in AXES:
                piece = left.astype(BF)
                total = total + nt(piece, turned[:, 0:WIDTH])
                left = left - piece.astype(F32)
            for b in range(4):
                up_ref[:, b * WIDTH:b * WIDTH + WIDTH] = total[b * 16:b * PACK + PACK]

        for dim, landing, todo in ((2, from_x, ((4, 1),)), (1, from_y, ((3, 3),)), (0, from_z, ((4, 2),))):
            copies = start(exchange(dim, landing, at, number))
            if dim == 1:
                shard_order()
            tail(*todo)
            collect(copies, dim, landing, at)
            at[dim] = place[dim]
            number += 3
        last = pltpu.make_async_remote_copy(
            src_ref=blocks.at[place], dst_ref=from_pair, send_sem=small_send.at[FIRST], recv_sem=small_recv.at[FIRST],
            device_id=ring.partner, device_id_type=MESH_ID)
        last.start()
        tail((4, 3))
        last.wait()
        small_ref[ALL] = blocks[place] + from_pair[ALL]
        ring.settle(0, first_orders)
        for stage in range(1, ATT_STAGES):
            ring.settle(stage, orders)


def attn_bwd(qkv, do, h, w_qkv, o, da, x, gr, vec, gvin, gbup, gup):
    one = lambda shape: pl.BlockSpec(shape, lambda g: (0,) * len(shape), pipeline_mode=ONCE)
    third = lambda t: pl.BlockSpec((ROWS, GROUP), lambda g: (0, t * GROUPS + g))
    wthird = lambda t: pl.BlockSpec((WIDTH, GROUP), lambda g: (0, t * GROUPS + g))
    col = pl.BlockSpec((ROWS, GROUP), lambda g: (0, g))
    anywhere = ANYWHERE
    shape = jax.ShapeDtypeStruct
    rows = (SUBS, LANES)
    vmem, dma = VM, pltpu.SemaphoreType.DMA
    return pl.pallas_call(
        attn_bwd_kernel, grid=(GROUPS,),
        out_shape=[shape((2, 3 * SUBS) + rows, F32), shape((2, SUBS) + rows, F32), shape((SEQS, TOKENS, WIDTH), BF), shape(rows, F32), shape((PACK, HIDDEN), F32)],
        in_specs=[third(0), third(1), third(2), col, one((ROWS, WIDTH)), wthird(0), wthird(1), wthird(2),
                  one((ROWS, WIDTH)), one((ROWS, WIDTH)), one((SEQS, TOKENS, WIDTH)), one((ROWS, WIDTH)),
                  one((SUBS, WIDTH)), one((SUBS, WIDTH)), one((SUBS, TILE)), one(gup.shape)],
        out_specs=[anywhere, anywhere, one((SEQS, TOKENS, WIDTH)), one(rows), one((PACK, HIDDEN))],
        scratch_shapes=[vmem((ROWS, WIDTH), F32), vmem((THIRDS, ROWS, GROUP), BF), vmem((ROWS, 3 * GROUP), BF),
                        vmem((WIDTH, ROWS), BF), vmem((2, TILE, LANES), BF), vmem((2, TILE, LANES), BF),
                        vmem((PAD, WIDTH), F32), vmem((PAD, WIDTH), BF), vmem((SUBS, WIDTH), F32), vmem((1, 3 * WIDTH), F32),
                        vmem(CUBE + rows, F32), vmem((3, 4, 4) + rows, F32), vmem((3, 4) + rows, F32),
                        vmem((3,) + rows, F32), vmem(rows, F32), dma((10,)), dma((10,))]
        + ring_scratch(ATT_SLOTS, ATT_STAGES, ATT_PARTS),
        compiler_params=pltpu.CompilerParams(vmem_limit_bytes=VMEM_CAP, collective_id=2, has_side_effects=True),
        name="attn_bwd",
    )(qkv, qkv, qkv, do, h, w_qkv, w_qkv, w_qkv, o, da, x, gr, vec, gvin, gbup, gup)


def layer(x, dz, w_qkv, b_qkv, w_out, w_up, b_up, w_down, vec_params):
    h1, qkv, o, a, h2, dm, vec, b_up, w_qkv, w_out, w_up, w_down = first(
        x, dz, (w_qkv, w_out, w_up, w_down), (b_qkv[None], b_up[None], vec_params))
    w_qkv, w_out, w_up = (w.reshape(WIDTH, -1) for w in (w_qkv, w_out, w_up))
    gw_up, gw_down, gb_up, z, gr, da, do, gvec = mlp(h2, dm, w_up, b_up, w_down, x, dz, a, w_out, vec)
    gw_qkv, gw_out, dx, small, gw_up = attn_bwd(qkv, do, h1, w_qkv, o, da, x, gr, vec, gvec, gb_up, gw_up)
    plain = lambda g: g.swapaxes(1, 2).reshape(g.shape[0] * SUBS, -1)
    return (z, dx, plain(gw_qkv), small[0, 16:SHARDS], plain(gw_out), gw_up, small[:, 64:72].reshape(SHARDS),
            plain(gw_down), small[:, 0:PACK])


def solution(mesh):
    batch = P(("rep", "fsdp"), None, None)
    rows, flat = P("fsdp", None), P("fsdp")
    params = (rows, flat, rows, rows, flat, rows, P(None, "fsdp"))
    return jax.shard_map(layer, mesh=mesh, in_specs=(batch, batch) + params, out_specs=(batch, batch) + params, check_vma=False)
```

```python
import jax
import jax.numpy as jnp
from jax import lax
from jax.experimental import pallas as pl
from jax.experimental.pallas import tpu as pltpu
from jax.sharding import PartitionSpec as P

LN_EPS = 1e-5

ALL = ...
FIRST, ONE = 0, 1
PACK, SHARDS, FLAT, LANES, SPAN, TRIPLE, TILE = 16, 64, 192, 128, 256, 384, 512
SUBS, RING = 8, 4
CUBE, BLOCK = (RING,) * 3, (2, SUBS, LANES)
AXES, SIDES = range(3), range(2)
ONCE = pl.Buffered(ONE)
ANYWHERE = pl.BlockSpec(memory_space=pl.ANY)
VM = pltpu.VMEM
KEEP = True
MIN = float("-inf")


def row(ref, k):
    return ref[k:k + ONE, :]


def other(rep):
    return ONE - rep


def iota(dims, axis):
    return lax.broadcasted_iota(jnp.int32, dims, axis)


def loop(count, body, start, **options):
    return lax.fori_loop(FIRST, count, body, start, **options)


def sum_rows(t):
    return jnp.sum(t, axis=FIRST, keepdims=KEEP)


def max_rows(t):
    return jnp.max(t, axis=FIRST, keepdims=KEEP)


def sum_lanes(t):
    return jnp.sum(t, axis=-ONE, keepdims=KEEP)


def max_lanes(t):
    return jnp.max(t, axis=-ONE, keepdims=KEEP)


def mean_lanes(t):
    return jnp.mean(t, axis=-ONE, keepdims=KEEP)


SEQS, TOKENS, PAD, WIDTH, HIDDEN = 6, 197, 208, 1024, 4096
ROWS = SEQS * PAD
BF, F32 = jnp.bfloat16, jnp.float32
VMEM_CAP = 67043328


def nn(a, b):
    return lax.dot_general(a, b, (((1,), (0,)), ((), ())), preferred_element_type=F32)


def nt(a, b):
    return lax.dot_general(a, b, (((1,), (1,)), ((), ())), preferred_element_type=F32)


def tn(a, b):
    return lax.dot_general(a, b, (((0,), (0,)), ((), ())), preferred_element_type=F32)


def row_stats(t):
    mean = mean_lanes(t)
    centered = t - mean
    variance = mean_lanes(centered * centered)
    return centered, lax.rsqrt(variance + LN_EPS)


def norm_back(dt, xhat, rstd):
    return rstd * (dt - mean_lanes(dt) - xhat * mean_lanes(dt * xhat))


def head_halves(width=LANES):
    lane = iota((1, width), 1)
    return lane < SHARDS


def stack_heads(dst, rows, low):
    zero = jnp.zeros_like(rows)
    dst[:PAD] = jnp.where(low, rows, zero)
    dst[SPAN:SPAN + PAD] = jnp.where(low, zero, rows)


def padded(dst, base, rows_ref, s):
    dst[base + FLAT:base + PAD] = jnp.zeros((PACK, WIDTH), dst.dtype)
    dst[base:base + TOKENS] = rows_ref[s].astype(dst.dtype)


MESH_ID = pl.DeviceIdType.MESH
ORDERS = ((2, 1, 0), (1, 0, 2), (0, 2, 1))
HOPS = (1, 2, 3)
GREETED = 10
FAR, NEAR, DIRECT = "far", "near", "direct"
EVERY = slice(None)


def my_place():
    rep, flat = lax.axis_index("rep"), lax.axis_index("fsdp")
    return rep, (flat // PACK, (flat // RING) % RING, flat % RING)


def along(place, dim, shift):
    moved = list(place)
    moved[dim] = (place[dim] + shift) % RING
    return tuple(moved)


def flat_of(place):
    return place[0] * PACK + place[1] * 4 + place[2]


def greet(sem, rep, place):
    pl.semaphore_signal(sem, inc=1, device_id=(other(rep), flat_of(place)), device_id_type=MESH_ID)
    for dim in AXES:
        for shift in HOPS:
            pl.semaphore_signal(sem, inc=1, device_id=(rep, flat_of(along(place, dim, shift))), device_id_type=MESH_ID)


def entry_barrier(rep, place):
    barrier = pltpu.get_barrier_semaphore()
    greet(barrier, rep, place)
    pl.semaphore_wait(barrier, GREETED)


def ring_scratch(slots, stages, parts):
    dma = pltpu.SemaphoreType.DMA
    block = BLOCK
    cube, square, line = CUBE, CUBE[1:], CUBE[2:]
    sides = (parts, 3)
    buffers = [(slots, parts) + cube + block, (parts,) + cube + block, (parts,) + cube + block,
               (stages, parts) + square + block,
               (slots,) + sides + square + block, (stages,) + sides + line + block, (stages,) + sides + block]
    sems = [()] * 2 + [(slots, 2)] * 2 + [(stages, 2)] * 2 + [(stages,)] * 3
    regular = pltpu.SemaphoreType.REGULAR
    return [VM(b, F32) for b in buffers] + [dma(s) for s in sems] + [regular((slots,)), regular]


class Ring:
    def __init__(self, refs, slots, steps, window):
        (self.acc, self.inbox, self.outbox, self.rest, land0, land1, land2, self.pair_send, self.pair_recv,
         self.send, self.recv, self.rest_send, self.rest_recv, self.out_sem, self.out_send, self.out_recv,
         self.free, self.emptied) = refs
        self.landing = (land0, land1, land2)
        self.slots, self.steps, self.last = slots, steps, len(steps)
        self.window = window
        self.rep, self.place = my_place()
        self.partner = (other(self.rep), flat_of(self.place))

    def across(self, ref, send, recv, into=None):
        return pltpu.make_async_remote_copy(
            src_ref=ref, dst_ref=ref if into is None else into, send_sem=send, recv_sem=recv, device_id=self.partner,
            device_id_type=MESH_ID)

    def pair(self, parts):
        some = pl.ds(FIRST, parts)
        return self.across(self.outbox.at[some], self.pair_send, self.pair_recv, self.inbox.at[some])

    def sems(self, stage, step):
        phase, kind = step
        if phase:
            at = (stage, phase - 1)
            return self.rest_send.at[at], self.rest_recv.at[at]
        at = (stage % self.slots, 1 if kind == NEAR else 0)
        return self.send.at[at], self.recv.at[at]

    def landed(self, stage, parts, step):
        phase, kind = step
        at = self.home(stage, 0, phase)[1][:1] + (pl.ds(FIRST, parts),)
        sides = {FAR: 2, NEAR: pl.ds(FIRST, 2), DIRECT: EVERY}[kind]
        return self.across(self.landing[phase].at[at + (sides,)], *self.sems(stage, step))

    def axis(self, order, phase, index):
        at = {dim: EVERY for dim in order}
        for dim in order[:phase]:
            at[dim] = self.place[dim]
        at[order[phase]] = index
        if phase:
            del at[order[0]]
        return tuple(at[dim] for dim in sorted(at))

    def home(self, stage, part, phase):
        if phase:
            return self.rest, (stage, part)
        return self.acc, (stage % self.slots, part)

    def hops(self, stage, part, order, step):
        phase, kind = step
        dim = order[phase]
        memory, at = self.home(stage, part, phase)
        send, recv = self.sems(stage, step)
        found = []
        for side, shift in enumerate((1, 3) if kind != DIRECT else HOPS):
            source, target, place = shift, 0, at + (side,)
            if kind == FAR:
                source, target = 2, shift
            src = at + self.axis(order, phase, (self.place[dim] + source) % RING)
            into = at + self.axis(order, phase, (self.place[dim] + target) % RING)
            if kind == FAR:
                src, into, place = src + (side,), into + (side,), at + (2,) + (EVERY, EVERY, side)
            copy = pltpu.make_async_remote_copy(
                src_ref=memory.at[src], dst_ref=self.landing[phase].at[place], send_sem=send, recv_sem=recv,
                device_id=(self.rep, flat_of(along(self.place, dim, shift))), device_id_type=MESH_ID)
            found.append((copy, into, place))
        return found

    def results(self, stage, orders):
        for part, order in orders.items():
            src = self.rest.at[(stage, part) + tuple(self.place[dim] for dim in sorted(order[1:]))]
            dst = self.window(stage, part)
            pltpu.make_async_copy(src, dst, self.out_sem.at[stage]).start()
            self.across(src, self.out_send.at[stage], self.out_recv.at[stage], dst).start()

    def level(self, stage, level, orders, credit, refill):
        if level == 0:
            self.pair(len(orders)).wait()
            for part in orders:
                at = (stage % self.slots, part)
                for z in range(4):
                    self.acc[at + (z,)] = self.acc[at + (z,)] + self.inbox[part, z]

            @pl.when(stage >= self.slots)
            def _():
                pl.semaphore_wait(self.free.at[stage % self.slots], GREETED)

            @pl.when(refill)
            def _():
                pl.semaphore_signal(self.emptied, inc=1, device_id=self.partner, device_id_type=MESH_ID)
        else:
            step = self.steps[level - 1]
            phase, kind = step
            self.landed(stage, len(orders), step).wait_recv()
            for part, order in orders.items():
                memory = self.home(stage, part, phase)[0]
                hops = self.hops(stage, part, order, step)
                if kind == FAR:
                    for _, into, place in hops:
                        memory[into] = memory[into] + self.landing[phase][place]
                    continue
                into = hops[0][1]
                total = memory[into]
                for _, _, place in hops:
                    total = total + self.landing[phase][place]
                if phase:
                    memory[into] = total
                else:
                    self.rest[stage, part] = total
            if phase == 0 and kind != FAR:
                self.sent(stage, orders, (0,))

                @pl.when(credit)
                def _():
                    greet(self.free.at[stage % self.slots], self.rep, self.place)
        if level < self.last:
            for part, order in orders.items():
                for copy, _, _ in self.hops(stage, part, order, self.steps[level]):
                    copy.start()
        else:
            self.results(stage, orders)
            self.sent(stage, orders, (1, 2))

    def sent(self, stage, orders, phases):
        for step in self.steps:
            if step[0] in phases:
                self.landed(stage, len(orders), step).wait_send()

    def settle(self, stage, parts):
        ref = self.rest.at[stage, pl.ds(FIRST, parts), 0, 0]
        pltpu.make_async_copy(ref, ref, self.out_sem.at[stage]).wait()
        self.across(ref, self.out_send.at[stage], self.out_recv.at[stage]).wait()

    def reopen_box(self):
        pl.semaphore_wait(self.emptied, 1)


PIECE = TILE
QKV, OUT, UP, DOWN, SMALL = range(5)


def gather_items():
    rest = [(OUT, 0, 0, PIECE)]
    rest += [(UP, 0, PIECE * j, HIDDEN // 2) for j in range(4)]
    rest += [(DOWN, PACK * j, 0, PIECE) for j in range(4)]
    items = [(0, QKV, 0, PIECE * j, 3 * PIECE, ORDERS[j]) for j in AXES] + [(0, SMALL, 0, 0, 0, ORDERS[0])]
    return items + [(1 + k // 3,) + piece + (ORDERS[k % 3],) for k, piece in enumerate(rest)]


def small_rows(table, vec, b_qkv, b_up):
    lane = iota((SUBS, LANES), 1)

    def moved(f, half, shift):
        return pltpu.roll(table[f // PACK, f // RING % RING, f % RING, half], shift % LANES, 1)

    def fill(ref, tile, owners, half, width, first):
        total = jnp.zeros((SUBS, LANES), F32)
        for f in owners:
            start = width * f - LANES * tile
            here = jnp.logical_and(lane >= start, lane < start + width)
            total = jnp.where(here, moved(f, half, start - first), total)
        ref[:, tile * LANES:tile * LANES + LANES] = total[:ref.shape[0]]

    for tile in range(WIDTH // LANES):
        fill(vec, tile, range(SUBS * tile, SUBS * tile + SUBS), 0, PACK, 0)
    for tile in range(TILE // LANES):
        fill(b_up, tile, range(PACK * tile, PACK * tile + PACK), 1, SUBS, 0)
    for tile in range(3 * WIDTH // LANES):
        fill(b_qkv, tile, range(LANES * tile // 48, (LANES * tile + LANES - 1) // 48 + 1), 0, 48, PACK)


def placed(values, first, period=LANES):
    size = values.shape[ONE]
    lane = iota((size, LANES), 1)
    row = iota((size, LANES), 0)
    return nn(values.astype(BF), jnp.where(lane == row % period + first, 1.0, 0.0).astype(BF))


def unit_columns(j):
    column = iota((WIDTH, LANES), 1)
    row = iota((WIDTH, LANES), 0)
    taken = row == SHARDS * (column // SUBS) + SUBS * j + column % SUBS
    return jnp.where(taken, 1.0, 0.0).astype(BF)


def first_kernel(x_ref, dz_ref, sq_ref, so_ref, su_ref, sd_ref, bq_ref, bu_ref, sv_ref,
                 h1_ref, qkv_ref, o_ref, a_ref, h2_ref, dm_ref, vec_ref, bup_ref, wq_hbm, wo_hbm, wu_hbm, wd_hbm,
                 wq, wo, su, sd, packed, table, bias, xhat, kst, vst, xp,
                 own_sem, send_sem, recv_sem, pair_send, pair_recv, save_sem):
    t = pl.program_id(0)
    rep, place = my_place()
    partner = (other(rep), flat_of(place))
    items = gather_items()
    fulls = (wq, wo, wu_hbm, wd_hbm, table)

    def block(item, shards, half=None):
        _, array, row, first, step, _ = items[item]
        if array == SMALL:
            return table.at[shards + ((half,) if half is not None else ())]
        col, cols = rep * step + first, PIECE
        if half is not None:
            col, cols = col + half * (PIECE // 2), PIECE // 2
        return fulls[array].at[shards + (pl.ds(row, PACK), pl.ds(pl.multiple_of(col, LANES), cols))]

    def shard(item):
        _, array, row, first, step, _ = items[item]
        return (su, sd)[array - UP].at[pl.ds(row, PACK), pl.ds(pl.multiple_of(rep * step + first, LANES), PIECE)]

    def own(item):
        return pltpu.make_async_copy(shard(item), block(item, place), own_sem.at[item])

    def pair(item):
        everywhere = block(item, (EVERY,) * 3)
        return pltpu.make_async_remote_copy(
            src_ref=everywhere, dst_ref=everywhere, send_sem=pair_send.at[item], recv_sem=pair_recv.at[item],
            device_id=partner, device_id_type=MESH_ID)

    def hops(item, level):
        array, order = items[item][ONE], items[item][-1]
        phase, second = level // 2, level % 2
        dim = order[phase]
        found = []
        for side, shift in enumerate((1, 3)):
            at = [EVERY] * 3
            for later in order[phase:]:
                at[later] = place[later]
            if second:
                at[dim] = (place[dim] + 4 - shift) % RING
            dst = block(item, tuple(at), side if second else None)
            src = shard(item) if level == 0 and array in (UP, DOWN) else dst
            found.append(pltpu.make_async_remote_copy(
                src_ref=src, dst_ref=dst, send_sem=send_sem.at[item, level], recv_sem=recv_sem.at[item, level],
                device_id=(rep, flat_of(along(place, dim, shift))), device_id_type=MESH_ID))
        return found

    def both(item, level):
        order = items[item][-1]
        phase, second = level // 2, level % 2
        at = [EVERY] * 3
        for later in order[phase:]:
            at[later] = place[later]
        if not second:
            at[order[phase]] = pl.ds(FIRST, 2)
        ref = block(item, tuple(at))
        return pltpu.make_async_remote_copy(
            src_ref=ref, dst_ref=ref, send_sem=send_sem.at[item, level], recv_sem=recv_sem.at[item, level],
            device_id=partner, device_id_type=MESH_ID)

    def advance(*todo):
        for stage, level in todo:
            for item in range(len(items)):
                if items[item][FIRST] != stage:
                    continue
                if level:
                    both(item, level - 1).wait_recv()
                if level == 2 and items[item][ONE] in (UP, DOWN):
                    own(item).wait()
                if level == 6:
                    if items[item][ONE] != SMALL:
                        pair(item).start()
                else:
                    for copy in hops(item, level):
                        copy.start()

    def arrived(*arrays):
        for item in range(len(items)):
            if items[item][ONE] in arrays:
                pair(item).wait_recv()

    def saves():
        return (pltpu.make_async_copy(wq, wq_hbm, save_sem.at[FIRST]), pltpu.make_async_copy(wo, wo_hbm, save_sem.at[1]))

    @pl.when(t == FIRST)
    def _():
        for full, piece, half in ((wq, sq_ref, 3 * PIECE), (wo, so_ref, PIECE)):
            cols = pl.ds(pl.multiple_of(rep * half, LANES), half)
            full[place + (EVERY, cols)] = piece[:, cols].astype(BF)
        for b in range(4):
            packed[b * 16:b * PACK + PACK] = su_ref[:, b * WIDTH:b * WIDTH + WIDTH].astype(BF)
        sd[ALL] = sd_ref[ALL].astype(BF)
        first_row = iota((SUBS, 48), 0) == 0
        table[place + (0,)] = placed(sv_ref[ALL], 0) + placed(jnp.where(first_row, bq_ref[ALL], 0.0), PACK)
        unit = iota((SUBS, SHARDS), 1) // SUBS == iota((SUBS, SHARDS), 0)
        table[place + (1,)] = placed(jnp.where(unit, bu_ref[ALL], 0.0), 0, SUBS)
        entry_barrier(rep, place)
        advance((0, 0))
        for j in range(SUBS):
            turned = nn(packed[ALL], unit_columns(j)).astype(BF)
            for b in range(4):
                su[:, j * TILE + b * LANES:j * TILE + b * LANES + LANES] = turned[b * 16:b * PACK + PACK]
        for item in range(len(items)):
            if items[item][ONE] in (UP, DOWN):
                own(item).start()
        for s in range(SEQS):
            base = s * PAD
            xp[FLAT:PAD] = jnp.zeros((PACK, WIDTH), BF)
            xp[:TOKENS] = x_ref[s]
            centered, rstd = row_stats(xp[ALL].astype(F32))
            xhat[base:base + PAD] = centered * rstd
            level = s + 1
            if s < 5:
                advance(*((stage, level - stage) for stage in range(min(level, 3) + 1)))
        advance((0, 6))
        small_rows(table, vec_ref, bias, bup_ref)
        real = iota((PAD, 1), 0) < TOKENS

        def scaled(s, carry):
            here = pl.ds(pl.multiple_of(s * PAD, PACK), PAD)
            h1_ref[here, :] = jnp.where(real, xhat[here, :] * vec_ref[:1, :] + row(vec_ref, 1), 0.0).astype(BF)
            return carry

        loop(SEQS, scaled, 0)
        kst[ALL] = jnp.zeros_like(kst)
        vst[ALL] = jnp.zeros_like(vst)

    @pl.when(t > FIRST)
    def _():
        base = pl.multiple_of((t - 1) * (2 * PAD), PACK)

        def qkv_tile(n, carry):
            cols = pl.ds(pl.multiple_of((rep * 3 + n) % 6 * PIECE, PIECE), PIECE)
            weights = wq[:, :, :, :, cols].reshape(WIDTH, PIECE)
            qkv_ref[:, cols] = (nn(h1_ref[pl.ds(base, 2 * PAD), :], weights) + bias[:, cols]).astype(BF)
            return carry

        loop(3, qkv_tile, 0)

        @pl.when(t == 1)
        def _():
            arrived(QKV)
            saves()[0].start()

        lax.fori_loop(3, 6, qkv_tile, 0)

    @pl.when(t == 1)
    def _():
        advance((1, 5), (2, 4), (3, 3))

    low = head_halves()
    visible = iota((1, SPAN), 1) < TOKENS

    def head_pair(p, carry):
        def cols(third):
            return pl.ds(pl.multiple_of(third * WIDTH + p * LANES, LANES), LANES)

        for s in SIDES:
            rows = pl.ds(s * PAD, PAD)
            stack_heads(kst.at[s], qkv_ref[rows, cols(1)], low)
            stack_heads(vst.at[s], qkv_ref[rows, cols(2)], low)
        for s in SIDES:
            rows = pl.ds(s * PAD, PAD)
            scores = nt(qkv_ref[rows, cols(0)], kst[s])
            probs = []
            for half in SIDES:
                part = jnp.where(visible, scores[:, half * SPAN:half * SPAN + SPAN], -jnp.inf)
                top = max_lanes(part)
                e = jnp.exp((part - top) * 0.125)
                probs.append((e * (1.0 / sum_lanes(e))).astype(BF))
            o_ref[rows, pl.ds(pl.multiple_of(p * LANES, LANES), LANES)] = nn(jnp.concatenate(probs, axis=1), vst[s]).astype(BF)
        return carry

    def two_pairs(i, carry):
        head_pair(2 * i, carry)
        head_pair(2 * i + 1, carry)
        for step, turn, todo in ((1, 0, ((1, 6),)), (2, 1, ((3, 5),)), (1, 2, ((2, 5), (3, 4))), (2, 3, ((3, 6),))):
            @pl.when(jnp.logical_and(t == step, i == turn))
            def _(todo=todo):
                advance(*todo)

        return carry

    @pl.when(t > FIRST)
    def _():
        loop(4, two_pairs, 0)

    @pl.when(t == 1)
    def _():
        arrived(OUT)
        saves()[1].start()

    @pl.when(t > FIRST)
    def _():
        for s in SIDES:
            padded(xp, 0, x_ref, 2 * (t - 1) + s)
            xhat[s * PAD:s * PAD + PAD] = xp[ALL].astype(F32)
            dm_ref[s * PAD + FLAT:s * PAD + PAD] = jnp.zeros((PACK, WIDTH), BF)
            dm_ref[s * PAD:s * PAD + TOKENS] = (dz_ref[s].astype(F32) * row(vec_ref, 7)).astype(BF)
        a_ref[ALL] = nn(o_ref[ALL], wo[ALL].reshape(WIDTH, WIDTH)) + row(vec_ref, 2)

        def rows(i, carry):
            at = pl.ds(pl.multiple_of(i * 32, 32), 32)
            y = xhat[at, :] + row(vec_ref, 3) * a_ref[at, :]
            centered, rstd = row_stats(y)
            h2_ref[at, :] = (centered * rstd * row(vec_ref, 4) + row(vec_ref, 5)).astype(BF)
            return carry

        loop(2 * PAD // 32, rows, 0, unroll=13)

    @pl.when(t == 1)
    def _():
        advance((2, 6))

    @pl.when(t == 3)
    def _():
        arrived(UP, DOWN)
        for item in range(len(items)):
            if items[item][ONE] != SMALL:
                pair(item).wait_send()
            for level in range(6):
                both(item, level).wait_send()
        for copy in saves():
            copy.wait()


def first(x, dz, shards, small):
    whole = lambda dims: pl.BlockSpec(dims, lambda t: (0,) * len(dims), pipeline_mode=ONCE)
    pair = lambda t: jnp.maximum(t - 1, 0)
    rows = lambda width: pl.BlockSpec((2 * PAD, width), lambda t: (pair(t), 0))
    anywhere = ANYWHERE
    shape, vmem, dma = jax.ShapeDtypeStruct, VM, pltpu.SemaphoreType.DMA
    n = len(gather_items())
    cube = CUBE
    return pl.pallas_call(
        first_kernel, grid=(4,),
        out_shape=[shape((ROWS, WIDTH), BF), shape((ROWS, 3 * WIDTH), BF), shape((ROWS, WIDTH), BF), shape((ROWS, WIDTH), F32),
                   shape((ROWS, WIDTH), BF), shape((ROWS, WIDTH), BF), shape((SUBS, WIDTH), F32), shape((SUBS, TILE), F32)]
        + [shape(cube + s.shape, BF) for s in shards],
        in_specs=[whole((SEQS, TOKENS, WIDTH)), pl.BlockSpec((2, TOKENS, WIDTH), lambda t: (pair(t), 0, 0))]
        + [whole(s.shape) for s in shards + small],
        out_specs=[whole((ROWS, WIDTH)), rows(3 * WIDTH), rows(WIDTH), rows(WIDTH), rows(WIDTH), rows(WIDTH),
                   whole((SUBS, WIDTH)), whole((SUBS, TILE))] + [anywhere] * 4,
        scratch_shapes=[vmem(cube + shards[QKV].shape, BF), vmem(cube + shards[OUT].shape, BF), vmem(shards[UP].shape, BF),
                        vmem(shards[DOWN].shape, BF), vmem((SHARDS, WIDTH), BF), vmem(cube + (2, SUBS, LANES), F32), vmem((1, 3 * WIDTH), F32),
                        vmem((ROWS, WIDTH), F32), vmem((2, PIECE, LANES), BF), vmem((2, PIECE, LANES), BF),
                        vmem((PAD, WIDTH), BF),
                        dma((n,)), dma((n, 6)), dma((n, 6)), dma((n,)), dma((n,)), dma((2,))],
        compiler_params=pltpu.CompilerParams(vmem_limit_bytes=VMEM_CAP, collective_id=FIRST, has_side_effects=True),
        name="first",
    )(x, dz, *shards, *small)


CHUNK = 624
TILES = HIDDEN // TILE
MLP_SLOTS, MLP_PARTS = 3, 4
MLP_STEPS = ((0, FAR), (0, NEAR), (1, DIRECT), (2, DIRECT))


def gelu_and_slope(u):
    cdf = 0.5 * (1.0 + lax.erf(u * (2.0 ** -0.5)))
    pdf = jnp.exp(u * u * -0.5) * ((2.0 * jnp.pi) ** -0.5)
    return u * cdf, cdf + u * pdf


def mlp_kernel(h_ref, dm_ref, w1_ref, w2_ref, b1_ref, x_ref, dz_ref, a_ref, wo_ref, vec_ref,
               gw1_ref, gw2_ref, gb_ref, z_ref, gr_ref, da_ref, do_ref, gv_ref,
               m_acc, dh_acc, act, dpre, turned, xp, zp, zo, *ring_refs):
    j = pl.program_id(0)

    def window(stage, part):
        if part < 2:
            return gw2_ref.at[stage, pl.ds(rep * 4 + part * 2, 2)]
        return gw1_ref.at[:, stage * 4 + rep * 2 + part - 2]

    ring = Ring(ring_refs, MLP_SLOTS, MLP_STEPS, window)
    rep = ring.rep
    every_part = range(MLP_PARTS)

    def run(lag, level):
        stage = j - lag
        for turn in AXES:
            orders = {part: ORDERS[(turn + part) % 3] for part in every_part}

            @pl.when(jnp.logical_and(jnp.logical_and(stage >= 0, stage < TILES), stage % 3 == turn))
            def _(orders=orders):
                ring.level(stage, level, orders, stage < TILES - MLP_SLOTS, stage < TILES - 1)

    @pl.when(j == FIRST)
    def _():
        entry_barrier(rep, ring.place)
        m_acc[ALL] = jnp.zeros_like(m_acc)
        dh_acc[ALL] = jnp.zeros_like(dh_acc)
        turned[ALL] = jnp.transpose(h_ref[ALL])

    def chunk(i, total):
        at = pl.ds(pl.multiple_of(i * CHUNK, PACK), CHUNK)
        w1, w2 = w1_ref[ALL], w2_ref[ALL].reshape(TILE, WIDTH)
        u = nn(h_ref[at, :], w1) + b1_ref[pl.ds(j, 1), :]
        value, slope = gelu_and_slope(u)
        act[at, :] = value.astype(BF)
        d = nt(dm_ref[at, :], w2) * slope
        dpre[at, :] = d.astype(BF)
        m_acc[at, :] += nn(act[at, :], w2)
        dh_acc[at, :] += nt(dpre[at, :], w1)
        return sum_rows(d) + total

    def grads(core, target):
        cols = pl.ds(pl.multiple_of(core * TILE, TILE), TILE)
        g = tn(act[ALL], dm_ref[:, cols])
        for part in SIDES:
            for half in SIDES:
                first = (part * 2 + half) * LANES
                target(part, half, g[:, first:first + LANES].reshape(CUBE + BLOCK[1:]))

    def grads_up(core, target):
        g = nn(turned[ALL], dpre[:, pl.ds(pl.multiple_of(core * SPAN, SPAN), SPAN)])
        for part in SIDES:
            target(part + 2, EVERY, g[:, part * LANES:part * LANES + LANES].reshape(CUBE + BLOCK))

    @pl.when(j < TILES)
    def _():
        gb_ref[pl.ds(j, 1), :] = loop(ROWS // CHUNK, chunk, jnp.zeros((1, TILE), F32))

    @pl.when(j == TILES)
    def _():
        gv_ref[ALL] = jnp.zeros_like(gv_ref)

    @pl.when(j >= TILES)
    def _():
        padded(xp, 0, x_ref, 0)
        padded(zp, 0, dz_ref, 0)
        s1, g2, b2, s2 = (vec_ref[k:k + 1, :] for k in (3, 4, 6, 7))
        here = pl.ds(pl.multiple_of((j - TILES) * PAD, PACK), PAD)
        a = a_ref[ALL]
        y = xp[ALL].astype(F32) + s1 * a
        mlp_out = m_acc[here, :] + b2
        g_out = zp[ALL].astype(F32)
        zo[ALL] = (y + s2 * mlp_out).astype(BF)
        centered, rstd = row_stats(y)
        xhat = centered * rstd
        dh = dh_acc[here, :]
        g_resid = g_out + norm_back(dh * g2, xhat, rstd)
        d_att = g_resid * s1
        gr_ref[ALL] = g_resid
        da_ref[ALL] = d_att.astype(BF)
        for k, total in enumerate((d_att, g_resid * a, dh * xhat, dh, g_out * s2, g_out * mlp_out)):
            gv_ref[2 + k:3 + k, :] += sum_rows(total)
        z_ref[0] = zo[:TOKENS]
        do_ref[ALL] = nt(da_ref[ALL], wo_ref[ALL]).astype(BF)

    for lag in range(ring.last + 1, 0, -1):
        run(lag, lag - 1)

    @pl.when(j < TILES)
    def _():
        slot = j % MLP_SLOTS

        def out(part, half, value):
            ring.outbox[part, :, :, :, half] = value

        def own(part, half, value):
            ring.acc[slot, part, :, :, :, half] = value

        grads(other(rep), out)
        grads_up(other(rep), out)

        @pl.when(j >= 1)
        def _():
            ring.reopen_box()

        ring.pair(MLP_PARTS).start()
        grads(rep, own)
        grads_up(rep, own)

    @pl.when(j == TILES + SEQS - 1)
    def _():
        for stage in range(TILES):
            ring.settle(stage, MLP_PARTS)


def mlp(h, dm, w1, b1, w2, x, dz, a, w_out, vec):
    whole = lambda shape: pl.BlockSpec(shape, lambda j: (0, 0), pipeline_mode=ONCE)
    tile = lambda j: jnp.minimum(j, TILES - 1)
    seq = lambda j: jnp.maximum(j - TILES, 0)
    b1_spec = whole((SUBS, TILE))
    seqs = pl.BlockSpec((1, TOKENS, WIDTH), lambda j: (seq(j), 0, 0))
    rows = pl.BlockSpec((PAD, WIDTH), lambda j: (seq(j), 0))
    anywhere = ANYWHERE
    shape = jax.ShapeDtypeStruct
    return pl.pallas_call(
        mlp_kernel, grid=(TILES + SEQS,),
        out_shape=[shape((2, HIDDEN // LANES, SUBS, LANES), F32), shape((SUBS, SUBS, SUBS, LANES), F32), shape((SUBS, TILE), F32),
                   shape((SEQS, TOKENS, WIDTH), BF), shape((ROWS, WIDTH), F32), shape((ROWS, WIDTH), BF),
                   shape((ROWS, WIDTH), BF), shape((8, WIDTH), F32)],
        in_specs=[whole((ROWS, WIDTH)), whole((ROWS, WIDTH)), pl.BlockSpec((WIDTH, TILE), lambda j: (0, tile(j))),
                  pl.BlockSpec((SHARDS, SUBS, WIDTH), lambda j: (0, tile(j), 0)), b1_spec, seqs, seqs, rows,
                  whole((WIDTH, WIDTH)), whole((8, WIDTH))],
        out_specs=[anywhere, anywhere, whole((SUBS, TILE)), seqs, rows, rows, rows, whole((8, WIDTH))],
        scratch_shapes=[VM((ROWS, WIDTH), F32), VM((ROWS, WIDTH), F32), VM((ROWS, TILE), BF),
                        VM((ROWS, TILE), BF), VM((WIDTH, ROWS), BF), VM((PAD, WIDTH), BF),
                        VM((PAD, WIDTH), BF), VM((PAD, WIDTH), BF)] + ring_scratch(MLP_SLOTS, TILES, MLP_PARTS),
        compiler_params=pltpu.CompilerParams(vmem_limit_bytes=VMEM_CAP, collective_id=1, has_side_effects=True),
        name="mlp",
    )(h, dm, w1, w2.reshape(SHARDS, SHARDS, WIDTH), b1, x, dz, a, w_out, vec)


GROUP = SPAN
GROUPS = WIDTH // GROUP
THIRDS = 3
ATT_SLOTS, ATT_STAGES, ATT_PARTS = 2, GROUPS + 1, 4
ATT_STEPS = tuple((phase, DIRECT) for phase in AXES)


def small_blocks(target, vec, b_qkv, b_up):
    lane = iota((SUBS, LANES), 1)

    def turned(ref, tile, first, to):
        return pltpu.roll(ref[:, tile * LANES:tile * LANES + LANES], (to - first) % LANES, 1)

    for f in range(SHARDS):
        tile, first = divmod(48 * f, LANES)
        bias = turned(b_qkv, tile, first, PACK)
        if first + 48 > LANES:
            bias = jnp.where(lane[:1] < PACK + LANES - first, bias, turned(b_qkv, tile + 1, first, PACK))
        rows = turned(vec, f // SUBS, PACK * (f % SUBS), 0)
        up = turned(b_up, f // PACK, SUBS * (f % PACK), SHARDS)
        target[f // PACK, f // RING % RING, f % RING] = jnp.where(lane < PACK, rows, jnp.where(lane < SHARDS, bias, up))


def attn_bwd_kernel(q_ref, k_ref, v_ref, do_ref, h_ref, wq_ref, wk_ref, wv_ref, o_ref, da_ref, x_ref, gr_ref, vec_ref,
                    gvin_ref, gbup_ref, gup_ref, gw_ref, gwo_ref, dx_ref, small_ref, up_ref,
                    dh, grads, by_core, turned, qst, dst, xp, dxp, sums, biases, blocks, from_x, from_y, from_z, from_pair,
                    small_send, small_recv, *ring_refs):
    g = pl.program_id(0)

    def window(stage, part):
        if isinstance(stage, int) and stage == 0:
            return gwo_ref.at[:, rep * 4 + part]
        return gw_ref.at[:, part * SUBS + (stage - 1) * 2 + rep]

    ring = Ring(ring_refs, ATT_SLOTS, ATT_STEPS, window)
    rep, place = ring.rep, ring.place
    first_orders = {part: ORDERS[part % 3] for part in range(ATT_PARTS)}
    orders = {part: ORDERS[part] for part in range(THIRDS)}

    def level(stage, which, at):
        ring.level(stage, at, which, stage < ATT_STAGES - ATT_SLOTS, stage < ATT_STAGES - 1)

    def poll(todo):
        for lag, at in todo:
            @pl.when(g - lag >= 1)
            def _(lag=lag, at=at):
                level(g - lag, orders, at)

            @pl.when(g == lag)
            def _(at=at):
                level(0, first_orders, at)

    @pl.when(g == FIRST)
    def _():
        entry_barrier(rep, place)
        dh[ALL] = jnp.zeros_like(dh)
        qst[ALL] = jnp.zeros_like(qst)
        dst[ALL] = jnp.zeros_like(dst)
        turned[ALL] = jnp.transpose(h_ref[ALL])
        for core, box in ((other(rep), ring.outbox), (rep, ring.acc.at[FIRST])):
            w = tn(o_ref[ALL], da_ref[:, pl.ds(pl.multiple_of(core * TILE, TILE), TILE)])
            for part in range(ATT_PARTS):
                box[part] = w[:, part * LANES:part * LANES + LANES].reshape(CUBE + BLOCK)
            if box is ring.outbox:
                ring.pair(ATT_PARTS).start()

    poll(((2, 2),))
    low = head_halves()
    low_rows = iota((LANES, 1), 0) < SHARDS
    hidden = iota((PAD, 1), 0) >= TOKENS

    def seq(s, sums):
        rows = pl.ds(pl.multiple_of(s * PAD, PACK), PAD)
        out = []
        for p in SIDES:
            cols = slice(p * LANES, p * LANES + LANES)
            qs, ds = qst.at[p], dst.at[p]
            k_rows, v_rows = k_ref[rows, cols], v_ref[rows, cols]
            stack_heads(qs, q_ref[rows, cols], low)
            stack_heads(ds, do_ref[rows, cols], low)
            scores = jnp.where(hidden, -jnp.inf, nt(k_rows, qs[ALL]))
            top = max_rows(scores)
            e = jnp.exp((scores - top) * 0.125)
            probs = e * (1.0 / sum_rows(e))
            d_probs = nt(v_rows, ds[ALL])
            inner = sum_rows(d_probs * probs)
            d_scores = (probs * (d_probs - inner) * 0.125).astype(BF)
            grad_v = nn(probs.astype(BF), ds[ALL])
            grad_k = nn(d_scores, qs[ALL])
            folded = nn(jnp.transpose(k_rows), d_scores)
            grad_q = jnp.transpose(jnp.where(low_rows, folded[:, :SPAN], folded[:, SPAN:TILE]))[:PAD]
            for third, value in enumerate((grad_q, grad_k, grad_v)):
                rounded = value.astype(BF)
                grads[third, rows, cols] = rounded
                by_core[rows, p * TRIPLE + third * LANES:p * TRIPLE + third * LANES + LANES] = rounded
                out.append(sum_rows(value))
        return tuple(t + n for t, n in zip(sums, out))

    zero = jnp.zeros((ONE, LANES), F32)
    bias_sums = loop(SEQS, seq, (zero,) * 6, unroll=2)
    for p in SIDES:
        for third in range(THIRDS):
            at = pl.multiple_of(third * WIDTH + g * GROUP + p * LANES, LANES)
            biases[:, pl.ds(at, LANES)] = bias_sums[3 * p + third]
    poll(((2, 3), (1, 1), (0, 0)))
    stage = g + 1

    ring.reopen_box()

    w = nn(turned[ALL], by_core[ALL])
    for part in range(THIRDS):
        both = [w[:, at:at + LANES].reshape(CUBE + BLOCK) for at in (part * LANES, TRIPLE + part * LANES)]
        ring.outbox[part] = jnp.where(rep == 0, both[1], both[0])
        ring.acc[stage % ATT_SLOTS, part] = jnp.where(rep == 0, both[0], both[1])
    ring.pair(THIRDS).start()

    def chunk(i, carry):
        at = pl.ds(pl.multiple_of(i * CHUNK, PACK), CHUNK)
        dh[at, :] += nt(grads[0, at, :], wq_ref[ALL]) + nt(grads[1, at, :], wk_ref[ALL]) + nt(grads[2, at, :], wv_ref[ALL])
        return carry

    loop(ROWS // CHUNK, chunk, 0)

    def exchange(dim, landing, at, number):
        copies = []
        for hops in range(ONE, 4):
            index = list(at)
            index[dim] = (place[dim] + hops) % RING
            copies.append(pltpu.make_async_remote_copy(
                src_ref=blocks.at[tuple(index)], dst_ref=landing.at[hops - 1], send_sem=small_send.at[number + hops],
                recv_sem=small_recv.at[number + hops], device_id=(rep, flat_of(along(place, dim, hops))),
                device_id_type=MESH_ID))
        return copies

    def start(copies):
        for copy in copies:
            copy.start()
        return copies

    def collect(copies, dim, landing, at):
        for copy in copies:
            copy.wait()
        index = list(at)
        index[dim] = place[dim]
        index = tuple(index)
        blocks[index] = blocks[index] + landing[0] + landing[1] + landing[2]

    @pl.when(g == GROUPS - 1)
    def _():
        def tail(*todo):
            for stage, at in todo:
                level(stage, orders, at)

        gain = vec_ref[:1, :]
        tail((2, 2), (3, 1), (4, 0))
        sums[ALL] = gvin_ref[ALL]
        def norm_one(s, carry):
            padded(xp, 0, x_ref, s)
            here = pl.ds(pl.multiple_of(s * PAD, PACK), PAD)
            centered, rstd = row_stats(xp[ALL])
            xhat = centered * rstd
            d = dh[here, :]
            dxp[ALL] = (gr_ref[here, :] + norm_back(d * gain, xhat, rstd)).astype(BF)
            for k, value in enumerate((d * xhat, d)):
                sums[k:k + 1, :] += sum_rows(value)
            dx_ref[s] = dxp[:TOKENS]

            @pl.when(s == 3)
            def _():
                tail((2, 3), (3, 2))

            return carry

        loop(SEQS, norm_one, 0)
        small_blocks(blocks, sums, biases, gbup_ref)
        at = [EVERY] * 3
        number = 0
        def shard_order():
            for j in range(SUBS):
                turned[:, j * LANES:j * LANES + LANES] = unit_columns(j)
                for b in range(4):
                    for h in SIDES:
                        xp[b * PACK + h * SUBS:b * PACK + h * SUBS + SUBS, j * LANES:j * LANES + LANES] = gup_ref[h, j * 4 + b]
            left = xp[:SHARDS]
            total = jnp.zeros_like(left)
            for _ in AXES:
                piece = left.astype(BF)
                total = total + nt(piece, turned[:, :WIDTH])
                left = left - piece.astype(F32)
            for b in range(4):
                up_ref[:, b * WIDTH:b * WIDTH + WIDTH] = total[b * 16:b * PACK + PACK]

        for dim, landing, todo in ((2, from_x, ((4, 1),)), (1, from_y, ((3, 3),)), (0, from_z, ((4, 2),))):
            copies = start(exchange(dim, landing, at, number))
            if dim == 1:
                shard_order()
            tail(*todo)
            collect(copies, dim, landing, at)
            at[dim] = place[dim]
            number += 3
        last = pltpu.make_async_remote_copy(
            src_ref=blocks.at[place], dst_ref=from_pair, send_sem=small_send.at[FIRST], recv_sem=small_recv.at[FIRST],
            device_id=ring.partner, device_id_type=MESH_ID)
        last.start()
        tail((4, 3))
        last.wait()
        small_ref[ALL] = blocks[place] + from_pair[ALL]
        ring.settle(0, ATT_PARTS)
        for stage in range(ONE, ATT_STAGES):
            ring.settle(stage, THIRDS)


def attn_bwd(qkv, do, h, w_qkv, o, da, x, gr, vec, gvin, gbup, gup):
    one = lambda shape: pl.BlockSpec(shape, lambda g: (0,) * len(shape), pipeline_mode=ONCE)
    third = lambda t: pl.BlockSpec((ROWS, GROUP), lambda g: (0, t * GROUPS + g))
    wthird = lambda t: pl.BlockSpec((WIDTH, GROUP), lambda g: (0, t * GROUPS + g))
    col = pl.BlockSpec((ROWS, GROUP), lambda g: (0, g))
    anywhere = ANYWHERE
    shape = jax.ShapeDtypeStruct
    rows = (SUBS, LANES)
    vmem, dma = VM, pltpu.SemaphoreType.DMA
    return pl.pallas_call(
        attn_bwd_kernel, grid=(GROUPS,),
        out_shape=[shape((2, 3 * SUBS) + rows, F32), shape((2, SUBS) + rows, F32), shape((SEQS, TOKENS, WIDTH), BF), shape(rows, F32), shape((PACK, HIDDEN), F32)],
        in_specs=[third(0), third(1), third(2), col, one((ROWS, WIDTH)), wthird(0), wthird(1), wthird(2),
                  one((ROWS, WIDTH)), one((ROWS, WIDTH)), one((SEQS, TOKENS, WIDTH)), one((ROWS, WIDTH)),
                  one((SUBS, WIDTH)), one((SUBS, WIDTH)), one((SUBS, TILE)), one(gup.shape)],
        out_specs=[anywhere, anywhere, one((SEQS, TOKENS, WIDTH)), one(rows), one((PACK, HIDDEN))],
        scratch_shapes=[vmem((ROWS, WIDTH), F32), vmem((THIRDS, ROWS, GROUP), BF), vmem((ROWS, 3 * GROUP), BF),
                        vmem((WIDTH, ROWS), BF), vmem((2, TILE, LANES), BF), vmem((2, TILE, LANES), BF),
                        vmem((PAD, WIDTH), F32), vmem((PAD, WIDTH), BF), vmem((SUBS, WIDTH), F32), vmem((1, 3 * WIDTH), F32),
                        vmem(CUBE + rows, F32), vmem((3, 4, 4) + rows, F32), vmem((3, 4) + rows, F32),
                        vmem((3,) + rows, F32), vmem(rows, F32), dma((10,)), dma((10,))]
        + ring_scratch(ATT_SLOTS, ATT_STAGES, ATT_PARTS),
        compiler_params=pltpu.CompilerParams(vmem_limit_bytes=VMEM_CAP, collective_id=2, has_side_effects=True),
        name="attn_bwd",
    )(qkv, qkv, qkv, do, h, w_qkv, w_qkv, w_qkv, o, da, x, gr, vec, gvin, gbup, gup)


def layer(x, dz, w_qkv, b_qkv, w_out, w_up, b_up, w_down, vec_params):
    h1, qkv, o, a, h2, dm, vec, b_up, w_qkv, w_out, w_up, w_down = first(
        x, dz, (w_qkv, w_out, w_up, w_down), (b_qkv[None], b_up[None], vec_params))
    w_qkv, w_out, w_up = (w.reshape(WIDTH, -1) for w in (w_qkv, w_out, w_up))
    gw_up, gw_down, gb_up, z, gr, da, do, gvec = mlp(h2, dm, w_up, b_up, w_down, x, dz, a, w_out, vec)
    gw_qkv, gw_out, dx, small, gw_up = attn_bwd(qkv, do, h1, w_qkv, o, da, x, gr, vec, gvec, gb_up, gw_up)
    plain = lambda g: g.swapaxes(1, 2).reshape(g.shape[0] * SUBS, -1)
    return (z, dx, plain(gw_qkv), small[0, 16:SHARDS], plain(gw_out), gw_up, small[:, 64:72].reshape(SHARDS),
            plain(gw_down), small[:, :PACK])


def solution(mesh):
    batch = P(("rep", "fsdp"), None, None)
    rows, flat = P("fsdp", None), P("fsdp")
    params = (rows, flat, rows, rows, flat, rows, P(None, "fsdp"))
    return jax.shard_map(layer, mesh=mesh, in_specs=(batch, batch) + params, out_specs=(batch, batch) + params, check_vma=False)
```

```python
import jax
import jax.numpy as jnp
from jax import lax
from jax.experimental import pallas as pl
from jax.experimental.pallas import tpu as pltpu
from jax.sharding import PartitionSpec as P

LN_EPS = 1e-5

ALL = ...
FIRST, ONE = 0, 1
PACK, SHARDS, FLAT, LANES, SPAN, TRIPLE, TILE = 16, 64, 192, 128, 256, 384, 512
SUBS, RING = 8, 4
CUBE, BLOCK = (RING,) * 3, (2, SUBS, LANES)
AXES, SIDES = range(3), range(2)
ONCE = pl.Buffered(ONE)
ANYWHERE = pl.BlockSpec(memory_space=pl.ANY)
VM = pltpu.VMEM
KEEP = True
UNIT, NIL = 1.0, 0.0
TILE_SHAPE = BLOCK[ONE:]


def row(ref, k):
    return ref[k:k + ONE, :]


def other(rep):
    return ONE - rep


def iota(dims, axis):
    return lax.broadcasted_iota(jnp.int32, dims, axis)


def loop(count, body, start, **options):
    return lax.fori_loop(FIRST, count, body, start, **options)


def sum_rows(t):
    return jnp.sum(t, axis=FIRST, keepdims=KEEP)


def max_rows(t):
    return jnp.max(t, axis=FIRST, keepdims=KEEP)


def sum_lanes(t):
    return jnp.sum(t, axis=-ONE, keepdims=KEEP)


def max_lanes(t):
    return jnp.max(t, axis=-ONE, keepdims=KEEP)


def mean_lanes(t):
    return jnp.mean(t, axis=-ONE, keepdims=KEEP)


SEQS, TOKENS, PAD, WIDTH, HIDDEN = 6, 197, 208, 1024, 4096
ROWS = SEQS * PAD
BF, F32 = jnp.bfloat16, jnp.float32
VMEM_CAP = 67043328


def nn(a, b):
    return lax.dot_general(a, b, (((1,), (0,)), ((), ())), preferred_element_type=F32)


def nt(a, b):
    return lax.dot_general(a, b, (((1,), (1,)), ((), ())), preferred_element_type=F32)


def tn(a, b):
    return lax.dot_general(a, b, (((0,), (0,)), ((), ())), preferred_element_type=F32)


def row_stats(t):
    mean = mean_lanes(t)
    centered = t - mean
    variance = mean_lanes(centered * centered)
    return centered, lax.rsqrt(variance + LN_EPS)


def norm_back(dt, xhat, rstd):
    return rstd * (dt - mean_lanes(dt) - xhat * mean_lanes(dt * xhat))


def head_halves(width=LANES):
    lane = iota((1, width), 1)
    return lane < SHARDS


def stack_heads(dst, rows, low):
    zero = jnp.zeros_like(rows)
    dst[:PAD] = jnp.where(low, rows, zero)
    dst[SPAN:SPAN + PAD] = jnp.where(low, zero, rows)


def padded(dst, base, rows_ref, s):
    dst[base + FLAT:base + PAD] = jnp.zeros((PACK, WIDTH), dst.dtype)
    dst[base:base + TOKENS] = rows_ref[s].astype(dst.dtype)


MESH_ID = pl.DeviceIdType.MESH
ORDERS = ((2, 1, 0), (1, 0, 2), (0, 2, 1))
HOPS = (1, 2, 3)
GREETED = 10
FAR, NEAR, DIRECT = "far", "near", "direct"
EVERY = slice(None)


def my_place():
    rep, flat = lax.axis_index("rep"), lax.axis_index("fsdp")
    return rep, (flat // PACK, (flat // RING) % RING, flat % RING)


def along(place, dim, shift):
    moved = list(place)
    moved[dim] = (place[dim] + shift) % RING
    return tuple(moved)


def flat_of(place):
    return place[0] * PACK + place[1] * 4 + place[2]


def greet(sem, rep, place):
    pl.semaphore_signal(sem, inc=1, device_id=(other(rep), flat_of(place)), device_id_type=MESH_ID)
    for dim in AXES:
        for shift in HOPS:
            pl.semaphore_signal(sem, inc=1, device_id=(rep, flat_of(along(place, dim, shift))), device_id_type=MESH_ID)


def entry_barrier(rep, place):
    barrier = pltpu.get_barrier_semaphore()
    greet(barrier, rep, place)
    pl.semaphore_wait(barrier, GREETED)


def ring_scratch(slots, stages, parts):
    dma = pltpu.SemaphoreType.DMA
    block = BLOCK
    cube, square, line = CUBE, CUBE[1:], CUBE[2:]
    sides = (parts, 3)
    buffers = [(slots, parts) + cube + block, (parts,) + cube + block, (parts,) + cube + block,
               (stages, parts) + square + block,
               (slots,) + sides + square + block, (stages,) + sides + line + block, (stages,) + sides + block]
    sems = [()] * 2 + [(slots, 2)] * 2 + [(stages, 2)] * 2 + [(stages,)] * 3
    regular = pltpu.SemaphoreType.REGULAR
    return [VM(b, F32) for b in buffers] + [dma(s) for s in sems] + [regular((slots,)), regular]


class Ring:
    def __init__(self, refs, slots, steps, window):
        (self.acc, self.inbox, self.outbox, self.rest, land0, land1, land2, self.pair_send, self.pair_recv,
         self.send, self.recv, self.rest_send, self.rest_recv, self.out_sem, self.out_send, self.out_recv,
         self.free, self.emptied) = refs
        self.landing = (land0, land1, land2)
        self.slots, self.steps, self.last = slots, steps, len(steps)
        self.window = window
        self.rep, self.place = my_place()
        self.partner = (other(self.rep), flat_of(self.place))

    def across(self, ref, send, recv, into=None):
        return pltpu.make_async_remote_copy(
            src_ref=ref, dst_ref=ref if into is None else into, send_sem=send, recv_sem=recv, device_id=self.partner,
            device_id_type=MESH_ID)

    def pair(self, parts):
        some = pl.ds(FIRST, parts)
        return self.across(self.outbox.at[some], self.pair_send, self.pair_recv, self.inbox.at[some])

    def sems(self, stage, step):
        phase, kind = step
        if phase:
            at = (stage, phase - 1)
            return self.rest_send.at[at], self.rest_recv.at[at]
        at = (stage % self.slots, 1 if kind == NEAR else 0)
        return self.send.at[at], self.recv.at[at]

    def landed(self, stage, parts, step):
        phase, kind = step
        at = self.home(stage, 0, phase)[1][:1] + (pl.ds(FIRST, parts),)
        sides = {FAR: 2, NEAR: pl.ds(FIRST, 2), DIRECT: EVERY}[kind]
        return self.across(self.landing[phase].at[at + (sides,)], *self.sems(stage, step))

    def axis(self, order, phase, index):
        at = {dim: EVERY for dim in order}
        for dim in order[:phase]:
            at[dim] = self.place[dim]
        at[order[phase]] = index
        if phase:
            del at[order[0]]
        return tuple(at[dim] for dim in sorted(at))

    def home(self, stage, part, phase):
        if phase:
            return self.rest, (stage, part)
        return self.acc, (stage % self.slots, part)

    def hops(self, stage, part, order, step):
        phase, kind = step
        dim = order[phase]
        memory, at = self.home(stage, part, phase)
        send, recv = self.sems(stage, step)
        found = []
        for side, shift in enumerate((1, 3) if kind != DIRECT else HOPS):
            source, target, place = shift, 0, at + (side,)
            if kind == FAR:
                source, target = 2, shift
            src = at + self.axis(order, phase, (self.place[dim] + source) % RING)
            into = at + self.axis(order, phase, (self.place[dim] + target) % RING)
            if kind == FAR:
                src, into, place = src + (side,), into + (side,), at + (2,) + (EVERY, EVERY, side)
            copy = pltpu.make_async_remote_copy(
                src_ref=memory.at[src], dst_ref=self.landing[phase].at[place], send_sem=send, recv_sem=recv,
                device_id=(self.rep, flat_of(along(self.place, dim, shift))), device_id_type=MESH_ID)
            found.append((copy, into, place))
        return found

    def results(self, stage, orders):
        for part, order in orders.items():
            src = self.rest.at[(stage, part) + tuple(self.place[dim] for dim in sorted(order[1:]))]
            dst = self.window(stage, part)
            pltpu.make_async_copy(src, dst, self.out_sem.at[stage]).start()
            self.across(src, self.out_send.at[stage], self.out_recv.at[stage], dst).start()

    def level(self, stage, level, orders, credit, refill):
        if level == 0:
            self.pair(len(orders)).wait()
            for part in orders:
                at = (stage % self.slots, part)
                for z in range(4):
                    self.acc[at + (z,)] = self.acc[at + (z,)] + self.inbox[part, z]

            @pl.when(stage >= self.slots)
            def _():
                pl.semaphore_wait(self.free.at[stage % self.slots], GREETED)

            @pl.when(refill)
            def _():
                pl.semaphore_signal(self.emptied, inc=1, device_id=self.partner, device_id_type=MESH_ID)
        else:
            step = self.steps[level - 1]
            phase, kind = step
            self.landed(stage, len(orders), step).wait_recv()
            for part, order in orders.items():
                memory = self.home(stage, part, phase)[0]
                hops = self.hops(stage, part, order, step)
                if kind == FAR:
                    for _, into, place in hops:
                        memory[into] = memory[into] + self.landing[phase][place]
                    continue
                into = hops[0][1]
                total = memory[into]
                for _, _, place in hops:
                    total = total + self.landing[phase][place]
                if phase:
                    memory[into] = total
                else:
                    self.rest[stage, part] = total
            if phase == 0 and kind != FAR:
                self.sent(stage, orders, (0,))

                @pl.when(credit)
                def _():
                    greet(self.free.at[stage % self.slots], self.rep, self.place)
        if level < self.last:
            for part, order in orders.items():
                for copy, _, _ in self.hops(stage, part, order, self.steps[level]):
                    copy.start()
        else:
            self.results(stage, orders)
            self.sent(stage, orders, (1, 2))

    def sent(self, stage, orders, phases):
        for step in self.steps:
            if step[0] in phases:
                self.landed(stage, len(orders), step).wait_send()

    def settle(self, stage, parts):
        ref = self.rest.at[stage, pl.ds(FIRST, parts), 0, 0]
        pltpu.make_async_copy(ref, ref, self.out_sem.at[stage]).wait()
        self.across(ref, self.out_send.at[stage], self.out_recv.at[stage]).wait()

    def reopen_box(self):
        pl.semaphore_wait(self.emptied, 1)


THIRDS = 3
PIECE = TILE
QKV, OUT, UP, DOWN, SMALL = range(5)


def gather_items():
    items = [(half, QKV, 0, third * WIDTH + half * PIECE, PIECE // 2, PIECE // 2, ORDERS[third])
             for half in SIDES for third in range(THIRDS)]
    rest = [(OUT, 0, 0, PIECE)]
    rest += [(UP, 0, PIECE * j, HIDDEN // 2) for j in range(4)]
    rest += [(DOWN, PACK * j, 0, PIECE) for j in range(4)]
    items += [(2 + k // 3,) + piece + (PIECE, ORDERS[k % 3]) for k, piece in enumerate(rest)]
    return items + [(0, SMALL, 0, 0, 0, 0, ORDERS[0])]


def small_rows(table, vec, b_qkv, b_up):
    lane = iota((SUBS, LANES), ONE)

    def moved(f, half, shift):
        return pltpu.roll(table[f // PACK, f // RING % RING, f % RING, half], shift % LANES, ONE)

    def fill(ref, tile, owners, half, width, first):
        total = jnp.zeros((SUBS, LANES), F32)
        for f in owners:
            start = width * f - LANES * tile
            here = jnp.logical_and(lane >= start, lane < start + width)
            total = jnp.where(here, moved(f, half, start - first), total)
        ref[:, tile * LANES:tile * LANES + LANES] = total[:ref.shape[0]]

    for tile in range(WIDTH // LANES):
        fill(vec, tile, range(SUBS * tile, SUBS * tile + SUBS), 0, PACK, 0)
    for tile in range(TILE // LANES):
        fill(b_up, tile, range(PACK * tile, PACK * tile + PACK), 1, SUBS, 0)
    for tile in range(3 * WIDTH // LANES):
        fill(b_qkv, tile, range(LANES * tile // 48, (LANES * tile + LANES - 1) // 48 + 1), 0, 48, PACK)


def placed(values, first, period=LANES):
    size = values.shape[ONE]
    lane = iota((size, LANES), ONE)
    row = iota((size, LANES), FIRST)
    return nn(values.astype(BF), jnp.where(lane == row % period + first, UNIT, NIL).astype(BF))


def unit_columns(j):
    column = iota((WIDTH, LANES), ONE)
    row = iota((WIDTH, LANES), FIRST)
    taken = row == SHARDS * (column // SUBS) + SUBS * j + column % SUBS
    return jnp.where(taken, UNIT, NIL).astype(BF)


def first_kernel(x_ref, dz_ref, sq_ref, so_ref, su_ref, sd_ref, bq_ref, bu_ref, sv_ref,
                 h1_ref, qkv_ref, o_ref, a_ref, h2_ref, dm_ref, vec_ref, bup_ref, wq_hbm, wo_hbm, wu_hbm, wd_hbm,
                 wq, wo, su, sd, packed, table, bias, xhat, kst, vst, xp,
                 own_sem, send_sem, recv_sem, pair_send, pair_recv, save_sem):
    t = pl.program_id(0)
    rep, place = my_place()
    partner = (other(rep), flat_of(place))
    items = gather_items()
    fulls = (wq, wo, wu_hbm, wd_hbm, table)

    def block(item, shards, half=None):
        _, array, row, first, step, cols, _ = items[item]
        if array == SMALL:
            return table.at[shards + ((half,) if half is not None else ())]
        col = rep * step + first
        if half is not None:
            cols = cols // 2
            col = col + half * cols
        return fulls[array].at[shards + (pl.ds(row, PACK), pl.ds(pl.multiple_of(col, LANES), cols))]

    def shard(item):
        _, array, row, first, step, _, _ = items[item]
        return (su, sd)[array - UP].at[pl.ds(row, PACK), pl.ds(pl.multiple_of(rep * step + first, LANES), PIECE)]

    def own(item):
        return pltpu.make_async_copy(shard(item), block(item, place), own_sem.at[item])

    def pair(item):
        everywhere = block(item, (EVERY,) * 3)
        return pltpu.make_async_remote_copy(
            src_ref=everywhere, dst_ref=everywhere, send_sem=pair_send.at[item], recv_sem=pair_recv.at[item],
            device_id=partner, device_id_type=MESH_ID)

    def hops(item, level):
        array, order = items[item][ONE], items[item][-1]
        phase, second = level // 2, level % 2
        dim = order[phase]
        found = []
        for side, shift in enumerate((1, 3)):
            at = [EVERY] * 3
            for later in order[phase:]:
                at[later] = place[later]
            if second:
                at[dim] = (place[dim] + 4 - shift) % RING
            dst = block(item, tuple(at), side if second else None)
            src = shard(item) if level == 0 and array in (UP, DOWN) else dst
            found.append(pltpu.make_async_remote_copy(
                src_ref=src, dst_ref=dst, send_sem=send_sem.at[item, level], recv_sem=recv_sem.at[item, level],
                device_id=(rep, flat_of(along(place, dim, shift))), device_id_type=MESH_ID))
        return found

    def both(item, level):
        order = items[item][-1]
        phase, second = level // 2, level % 2
        at = [EVERY] * 3
        for later in order[phase:]:
            at[later] = place[later]
        if not second:
            at[order[phase]] = pl.ds(FIRST, 2)
        ref = block(item, tuple(at))
        return pltpu.make_async_remote_copy(
            src_ref=ref, dst_ref=ref, send_sem=send_sem.at[item, level], recv_sem=recv_sem.at[item, level],
            device_id=partner, device_id_type=MESH_ID)

    def advance(*todo):
        for stage, level in todo:
            for item in range(len(items)):
                if items[item][FIRST] != stage:
                    continue
                if level:
                    both(item, level - 1).wait_recv()
                if level == 2 and items[item][ONE] in (UP, DOWN):
                    own(item).wait()
                if level == 6:
                    if items[item][ONE] != SMALL:
                        pair(item).start()
                else:
                    for copy in hops(item, level):
                        copy.start()

    def arrived(*stages):
        for item in range(len(items)):
            if items[item][FIRST] in stages and items[item][ONE] != SMALL:
                pair(item).wait_recv()

    def saves():
        return (pltpu.make_async_copy(wq, wq_hbm, save_sem.at[FIRST]), pltpu.make_async_copy(wo, wo_hbm, save_sem.at[1]))

    @pl.when(t == FIRST)
    def _():
        for _, array, _, first, step, width, _ in items:
            if array in (QKV, OUT):
                cols = pl.ds(pl.multiple_of(rep * step + first, LANES), width)
                (wq, wo)[array][place + (EVERY, cols)] = (sq_ref, so_ref)[array][:, cols].astype(BF)
        for b in range(4):
            packed[b * 16:b * PACK + PACK] = su_ref[:, b * WIDTH:b * WIDTH + WIDTH].astype(BF)
        sd[ALL] = sd_ref[ALL].astype(BF)
        first_row = iota((SUBS, 48), 0) == 0
        table[place + (0,)] = placed(sv_ref[ALL], 0) + placed(jnp.where(first_row, bq_ref[ALL], NIL), PACK)
        unit = iota((SUBS, SHARDS), ONE) // SUBS == iota((SUBS, SHARDS), FIRST)
        table[place + (1,)] = placed(jnp.where(unit, bu_ref[ALL], NIL), 0, SUBS)
        entry_barrier(rep, place)
        advance((0, 0), (1, 0))
        for j in range(SUBS):
            turned = nn(packed[ALL], unit_columns(j)).astype(BF)
            for b in range(4):
                su[:, j * TILE + b * LANES:j * TILE + b * LANES + LANES] = turned[b * 16:b * PACK + PACK]
        for item in range(len(items)):
            if items[item][ONE] in (UP, DOWN):
                own(item).start()
        later = (2, 3, 4)
        advance(*((stage, 0) for stage in later))
        everything = (0, 1) + later
        for s, todo in enumerate((
                [(stage, 1) for stage in everything], [(stage, 2) for stage in everything], [(0, 3), (1, 3)],
                [(0, 4), (1, 4)] + [(stage, 3) for stage in later], [(0, 5), (2, 4)], [(0, 6), (1, 5)])):
            base = s * PAD
            xp[FLAT:PAD] = jnp.zeros((PACK, WIDTH), BF)
            xp[:TOKENS] = x_ref[s]
            centered, rstd = row_stats(xp[ALL].astype(F32))
            xhat[base:base + PAD] = centered * rstd
            advance(*todo)
        small_rows(table, vec_ref, bias, bup_ref)
        real = iota((PAD, 1), 0) < TOKENS

        def scaled(s, carry):
            here = pl.ds(pl.multiple_of(s * PAD, PACK), PAD)
            h1_ref[here, :] = jnp.where(real, xhat[here, :] * vec_ref[:1, :] + row(vec_ref, 1), NIL).astype(BF)
            return carry

        loop(SEQS, scaled, 0)
        kst[ALL] = jnp.zeros_like(kst)
        vst[ALL] = jnp.zeros_like(vst)

    half, seqs = jnp.maximum(t - ONE, FIRST) // 3, jnp.maximum(t - ONE, FIRST) % 3
    base = pl.multiple_of(seqs * (2 * PAD), PACK)

    @pl.when(t == 1)
    def _():
        arrived(0)

    @pl.when(t == 4)
    def _():
        arrived(1)
        saves()[0].start()

    @pl.when(t > FIRST)
    def _():
        for third in range(THIRDS):
            cols = pl.ds(pl.multiple_of(third * WIDTH + half * PIECE, PIECE), PIECE)
            weights = wq[:, :, :, :, cols].reshape(WIDTH, PIECE)
            qkv = nn(h1_ref[pl.ds(base, 2 * PAD), :], weights) + bias[:, cols]
            qkv_ref[:, third * PIECE:third * PIECE + PIECE] = qkv.astype(BF)

    @pl.when(t == 1)
    def _():
        advance((3, 4))

    low = head_halves()
    visible = iota((1, SPAN), 1) < TOKENS

    half_cols = half * PIECE

    def head_pair(p, carry):
        def cols(third):
            return pl.ds(pl.multiple_of(third * PIECE + p * LANES, LANES), LANES)

        for s in SIDES:
            rows = pl.ds(s * PAD, PAD)
            stack_heads(kst.at[s], qkv_ref[rows, cols(1)], low)
            stack_heads(vst.at[s], qkv_ref[rows, cols(2)], low)
        for s in SIDES:
            rows = pl.ds(s * PAD, PAD)
            scores = nt(qkv_ref[rows, cols(0)], kst[s])
            probs = []
            for head in SIDES:
                part = jnp.where(visible, scores[:, head * SPAN:head * SPAN + SPAN], -jnp.inf)
                top = max_lanes(part)
                e = jnp.exp((part - top) * 0.125)
                probs.append((e * (1.0 / sum_lanes(e))).astype(BF))
            here = pl.ds(pl.multiple_of(base + s * PAD, PACK), PAD)
            heads = pl.ds(pl.multiple_of(half_cols + p * LANES, LANES), LANES)
            o_ref[here, heads] = nn(jnp.concatenate(probs, axis=1), vst[s]).astype(BF)
        return carry

    def two_pairs(i, carry):
        head_pair(2 * i, carry)
        head_pair(2 * i + 1, carry)
        for step, turn, todo in ((1, 0, (1, 6)), (1, 1, (2, 5)), (2, 0, (4, 4)), (2, 1, (3, 5)), (3, 0, (2, 6)),
                                 (4, 1, (4, 5)), (5, 0, (3, 6)), (5, 1, (4, 6))):
            @pl.when(jnp.logical_and(t == step, i == turn))
            def _(todo=todo):
                advance(todo)

        return carry

    @pl.when(t > FIRST)
    def _():
        loop(2, two_pairs, 0)

    @pl.when(t == 4)
    def _():
        arrived(2)
        saves()[1].start()

    @pl.when(t > 3)
    def _():
        for s in SIDES:
            padded(xp, 0, x_ref, 2 * seqs + s)
            xhat[s * PAD:s * PAD + PAD] = xp[ALL].astype(F32)
            dm_ref[s * PAD + FLAT:s * PAD + PAD] = jnp.zeros((PACK, WIDTH), BF)
            dm_ref[s * PAD:s * PAD + TOKENS] = (dz_ref[s].astype(F32) * row(vec_ref, 7)).astype(BF)
        a_ref[ALL] = nn(o_ref[pl.ds(base, 2 * PAD), :], wo[ALL].reshape(WIDTH, WIDTH)) + row(vec_ref, 2)

        def rows(i, carry):
            at = pl.ds(pl.multiple_of(i * 32, 32), 32)
            y = xhat[at, :] + row(vec_ref, 3) * a_ref[at, :]
            centered, rstd = row_stats(y)
            h2_ref[at, :] = (centered * rstd * row(vec_ref, 4) + row(vec_ref, 5)).astype(BF)
            return carry

        loop(2 * PAD // 32, rows, 0, unroll=13)

    @pl.when(t == 6)
    def _():
        arrived(3, 4)
        for item in range(len(items)):
            if items[item][ONE] != SMALL:
                pair(item).wait_send()
            for level in range(6):
                both(item, level).wait_send()
        for copy in saves():
            copy.wait()


def first(x, dz, shards, small):
    whole = lambda dims: pl.BlockSpec(dims, lambda t: (0,) * len(dims), pipeline_mode=ONCE)
    pair = lambda t: jnp.maximum(t - RING, FIRST)
    past = lambda t: jnp.maximum(t - ONE, FIRST)
    rows = pl.BlockSpec((2 * PAD, WIDTH), lambda t: (pair(t), 0))
    halves = pl.BlockSpec((2 * PAD, 3 * PIECE), lambda t: (past(t) % 3, past(t) // 3))
    anywhere = ANYWHERE
    shape, vmem, dma = jax.ShapeDtypeStruct, VM, pltpu.SemaphoreType.DMA
    n = len(gather_items())
    cube = CUBE
    return pl.pallas_call(
        first_kernel, grid=(7,),
        out_shape=[shape((ROWS, WIDTH), BF), shape((ROWS, 3 * WIDTH), BF), shape((ROWS, WIDTH), BF), shape((ROWS, WIDTH), F32),
                   shape((ROWS, WIDTH), BF), shape((ROWS, WIDTH), BF), shape((SUBS, WIDTH), F32), shape((SUBS, TILE), F32)]
        + [shape(cube + s.shape, BF) for s in shards],
        in_specs=[whole((SEQS, TOKENS, WIDTH)), pl.BlockSpec((2, TOKENS, WIDTH), lambda t: (pair(t), 0, 0))]
        + [whole(s.shape) for s in shards + small],
        out_specs=[whole((ROWS, WIDTH)), halves, whole((ROWS, WIDTH)), rows, rows, rows,
                   whole((SUBS, WIDTH)), whole((SUBS, TILE))] + [anywhere] * 4,
        scratch_shapes=[vmem(cube + shards[QKV].shape, BF), vmem(cube + shards[OUT].shape, BF), vmem(shards[UP].shape, BF),
                        vmem(shards[DOWN].shape, BF), vmem((SHARDS, WIDTH), BF), vmem(cube + (2, SUBS, LANES), F32), vmem((1, 3 * WIDTH), F32),
                        vmem((ROWS, WIDTH), F32), vmem((2, PIECE, LANES), BF), vmem((2, PIECE, LANES), BF),
                        vmem((PAD, WIDTH), BF),
                        dma((n,)), dma((n, 6)), dma((n, 6)), dma((n,)), dma((n,)), dma((2,))],
        compiler_params=pltpu.CompilerParams(vmem_limit_bytes=VMEM_CAP, collective_id=FIRST, has_side_effects=True),
        name="first",
    )(x, dz, *shards, *small)


CHUNK = 624
TILES = HIDDEN // TILE
MLP_SLOTS, MLP_PARTS = 3, 4
MLP_STEPS = ((0, FAR), (0, NEAR), (1, DIRECT), (2, DIRECT))


def gelu_and_slope(u):
    cdf = 0.5 * (1.0 + lax.erf(u * (2.0 ** -0.5)))
    pdf = jnp.exp(u * u * -0.5) * ((2.0 * jnp.pi) ** -0.5)
    return u * cdf, cdf + u * pdf


def mlp_kernel(h_ref, dm_ref, w1_ref, w2_ref, b1_ref, x_ref, dz_ref, a_ref, wo_ref, vec_ref,
               gw1_ref, gw2_ref, gb_ref, z_ref, gr_ref, da_ref, do_ref, gv_ref,
               m_acc, dh_acc, act, dpre, turned, xp, zp, zo, *ring_refs):
    j = pl.program_id(0)

    def window(stage, part):
        if part < 2:
            return gw2_ref.at[stage, pl.ds(rep * 4 + part * 2, 2)]
        return gw1_ref.at[:, stage * 4 + rep * 2 + part - 2]

    ring = Ring(ring_refs, MLP_SLOTS, MLP_STEPS, window)
    rep = ring.rep
    every_part = range(MLP_PARTS)

    def run(lag, level):
        stage = j - lag
        for turn in AXES:
            orders = {part: ORDERS[(turn + part) % 3] for part in every_part}

            @pl.when(jnp.logical_and(jnp.logical_and(stage >= 0, stage < TILES), stage % 3 == turn))
            def _(orders=orders):
                ring.level(stage, level, orders, stage < TILES - MLP_SLOTS, stage < TILES - 1)

    @pl.when(j == FIRST)
    def _():
        entry_barrier(rep, ring.place)
        m_acc[ALL] = jnp.zeros_like(m_acc)
        dh_acc[ALL] = jnp.zeros_like(dh_acc)
        turned[ALL] = jnp.transpose(h_ref[ALL])

    def chunk(i, total):
        at = pl.ds(pl.multiple_of(i * CHUNK, PACK), CHUNK)
        w1, w2 = w1_ref[ALL], w2_ref[ALL].reshape(TILE, WIDTH)
        u = nn(h_ref[at, :], w1) + b1_ref[pl.ds(j, 1), :]
        value, slope = gelu_and_slope(u)
        act[at, :] = value.astype(BF)
        d = nt(dm_ref[at, :], w2) * slope
        dpre[at, :] = d.astype(BF)
        m_acc[at, :] += nn(act[at, :], w2)
        dh_acc[at, :] += nt(dpre[at, :], w1)
        return sum_rows(d) + total

    def grads(core, target):
        cols = pl.ds(pl.multiple_of(core * TILE, TILE), TILE)
        g = tn(act[ALL], dm_ref[:, cols])
        for part in SIDES:
            for half in SIDES:
                first = (part * 2 + half) * LANES
                target(part, half, g[:, first:first + LANES].reshape(CUBE + TILE_SHAPE))

    def grads_up(core, target):
        g = nn(turned[ALL], dpre[:, pl.ds(pl.multiple_of(core * SPAN, SPAN), SPAN)])
        for part in SIDES:
            target(part + 2, EVERY, g[:, part * LANES:part * LANES + LANES].reshape(CUBE + BLOCK))

    @pl.when(j < TILES)
    def _():
        gb_ref[pl.ds(j, 1), :] = loop(ROWS // CHUNK, chunk, jnp.zeros((1, TILE), F32))

    @pl.when(j == TILES)
    def _():
        gv_ref[ALL] = jnp.zeros_like(gv_ref)

    @pl.when(j >= TILES)
    def _():
        padded(xp, 0, x_ref, 0)
        padded(zp, 0, dz_ref, 0)
        s1, g2, b2, s2 = (vec_ref[k:k + 1, :] for k in (3, 4, 6, 7))
        here = pl.ds(pl.multiple_of((j - TILES) * PAD, PACK), PAD)
        a = a_ref[ALL]
        y = xp[ALL].astype(F32) + s1 * a
        mlp_out = m_acc[here, :] + b2
        g_out = zp[ALL].astype(F32)
        zo[ALL] = (y + s2 * mlp_out).astype(BF)
        centered, rstd = row_stats(y)
        xhat = centered * rstd
        dh = dh_acc[here, :]
        g_resid = g_out + norm_back(dh * g2, xhat, rstd)
        d_att = g_resid * s1
        gr_ref[ALL] = g_resid
        da_ref[ALL] = d_att.astype(BF)
        for k, total in enumerate((d_att, g_resid * a, dh * xhat, dh, g_out * s2, g_out * mlp_out)):
            gv_ref[2 + k:3 + k, :] += sum_rows(total)
        z_ref[0] = zo[:TOKENS]
        do_ref[ALL] = nt(da_ref[ALL], wo_ref[ALL]).astype(BF)

    for lag in range(ring.last + 1, 0, -1):
        run(lag, lag - 1)

    @pl.when(j < TILES)
    def _():
        slot = j % MLP_SLOTS

        def out(part, half, value):
            ring.outbox[part, :, :, :, half] = value

        def own(part, half, value):
            ring.acc[slot, part, :, :, :, half] = value

        grads(other(rep), out)
        grads_up(other(rep), out)

        @pl.when(j >= 1)
        def _():
            ring.reopen_box()

        ring.pair(MLP_PARTS).start()
        grads(rep, own)
        grads_up(rep, own)

    @pl.when(j == TILES + SEQS - 1)
    def _():
        for stage in range(TILES):
            ring.settle(stage, MLP_PARTS)


def mlp(h, dm, w1, b1, w2, x, dz, a, w_out, vec):
    whole = lambda shape: pl.BlockSpec(shape, lambda j: (0, 0), pipeline_mode=ONCE)
    tile = lambda j: jnp.minimum(j, TILES - 1)
    seq = lambda j: jnp.maximum(j - TILES, FIRST)
    b1_spec = whole((SUBS, TILE))
    seqs = pl.BlockSpec((1, TOKENS, WIDTH), lambda j: (seq(j), 0, 0))
    rows = pl.BlockSpec((PAD, WIDTH), lambda j: (seq(j), 0))
    anywhere = ANYWHERE
    shape = jax.ShapeDtypeStruct
    return pl.pallas_call(
        mlp_kernel, grid=(TILES + SEQS,),
        out_shape=[shape((2, HIDDEN // LANES, SUBS, LANES), F32), shape((SUBS, SUBS, SUBS, LANES), F32), shape((SUBS, TILE), F32),
                   shape((SEQS, TOKENS, WIDTH), BF), shape((ROWS, WIDTH), F32), shape((ROWS, WIDTH), BF),
                   shape((ROWS, WIDTH), BF), shape((8, WIDTH), F32)],
        in_specs=[whole((ROWS, WIDTH)), whole((ROWS, WIDTH)), pl.BlockSpec((WIDTH, TILE), lambda j: (0, tile(j))),
                  pl.BlockSpec((SHARDS, SUBS, WIDTH), lambda j: (0, tile(j), 0)), b1_spec, seqs, seqs, rows,
                  whole((WIDTH, WIDTH)), whole((8, WIDTH))],
        out_specs=[anywhere, anywhere, whole((SUBS, TILE)), seqs, rows, rows, rows, whole((8, WIDTH))],
        scratch_shapes=[VM((ROWS, WIDTH), F32), VM((ROWS, WIDTH), F32), VM((ROWS, TILE), BF),
                        VM((ROWS, TILE), BF), VM((WIDTH, ROWS), BF), VM((PAD, WIDTH), BF),
                        VM((PAD, WIDTH), BF), VM((PAD, WIDTH), BF)] + ring_scratch(MLP_SLOTS, TILES, MLP_PARTS),
        compiler_params=pltpu.CompilerParams(vmem_limit_bytes=VMEM_CAP, collective_id=1, has_side_effects=True),
        name="mlp",
    )(h, dm, w1, w2.reshape(SHARDS, SHARDS, WIDTH), b1, x, dz, a, w_out, vec)


GROUP = SPAN
GROUPS = WIDTH // GROUP
ATT_SLOTS, ATT_STAGES, ATT_PARTS = 2, GROUPS + 1, 4
ATT_STEPS = tuple((phase, DIRECT) for phase in AXES)


def small_blocks(target, vec, b_qkv, b_up):
    lane = iota((SUBS, LANES), ONE)

    def turned(ref, tile, first, to):
        return pltpu.roll(ref[:, tile * LANES:tile * LANES + LANES], (to - first) % LANES, ONE)

    for f in range(SHARDS):
        tile, first = divmod(48 * f, LANES)
        bias = turned(b_qkv, tile, first, PACK)
        if first + 48 > LANES:
            bias = jnp.where(lane[:1] < PACK + LANES - first, bias, turned(b_qkv, tile + 1, first, PACK))
        rows = turned(vec, f // SUBS, PACK * (f % SUBS), 0)
        up = turned(b_up, f // PACK, SUBS * (f % PACK), SHARDS)
        target[f // PACK, f // RING % RING, f % RING] = jnp.where(lane < PACK, rows, jnp.where(lane < SHARDS, bias, up))


def attn_bwd_kernel(q_ref, k_ref, v_ref, do_ref, h_ref, wq_ref, wk_ref, wv_ref, o_ref, da_ref, x_ref, gr_ref, vec_ref,
                    gvin_ref, gbup_ref, gup_ref, gw_ref, gwo_ref, dx_ref, small_ref, up_ref,
                    dh, grads, by_core, turned, qst, dst, xp, dxp, sums, biases, blocks, from_x, from_y, from_z, from_pair,
                    small_send, small_recv, *ring_refs):
    g = pl.program_id(0)

    def window(stage, part):
        if isinstance(stage, int) and stage == 0:
            return gwo_ref.at[:, rep * 4 + part]
        return gw_ref.at[:, part * SUBS + (stage - 1) * 2 + rep]

    ring = Ring(ring_refs, ATT_SLOTS, ATT_STEPS, window)
    rep, place = ring.rep, ring.place
    first_orders = {part: ORDERS[part % 3] for part in range(ATT_PARTS)}
    orders = {part: ORDERS[part] for part in range(THIRDS)}

    def level(stage, which, at):
        ring.level(stage, at, which, stage < ATT_STAGES - ATT_SLOTS, stage < ATT_STAGES - 1)

    def poll(todo):
        for lag, at in todo:
            @pl.when(g - lag >= 1)
            def _(lag=lag, at=at):
                level(g - lag, orders, at)

            @pl.when(g == lag)
            def _(at=at):
                level(0, first_orders, at)

    @pl.when(g == FIRST)
    def _():
        entry_barrier(rep, place)
        dh[ALL] = jnp.zeros_like(dh)
        qst[ALL] = jnp.zeros_like(qst)
        dst[ALL] = jnp.zeros_like(dst)
        turned[ALL] = jnp.transpose(h_ref[ALL])
        for core, box in ((other(rep), ring.outbox), (rep, ring.acc.at[FIRST])):
            w = tn(o_ref[ALL], da_ref[:, pl.ds(pl.multiple_of(core * TILE, TILE), TILE)])
            for part in range(ATT_PARTS):
                box[part] = w[:, part * LANES:part * LANES + LANES].reshape(CUBE + BLOCK)
            if box is ring.outbox:
                ring.pair(ATT_PARTS).start()

    poll(((2, 2),))
    low = head_halves()
    low_rows = iota((LANES, ONE), 0) < SHARDS
    hidden = iota((PAD, 1), 0) >= TOKENS

    def seq(s, sums):
        rows = pl.ds(pl.multiple_of(s * PAD, PACK), PAD)
        out = []
        for p in SIDES:
            cols = slice(p * LANES, p * LANES + LANES)
            qs, ds = qst.at[p], dst.at[p]
            k_rows, v_rows = k_ref[rows, cols], v_ref[rows, cols]
            stack_heads(qs, q_ref[rows, cols], low)
            stack_heads(ds, do_ref[rows, cols], low)
            scores = jnp.where(hidden, -jnp.inf, nt(k_rows, qs[ALL]))
            top = max_rows(scores)
            e = jnp.exp((scores - top) * 0.125)
            probs = e * (1.0 / sum_rows(e))
            d_probs = nt(v_rows, ds[ALL])
            inner = sum_rows(d_probs * probs)
            d_scores = (probs * (d_probs - inner) * 0.125).astype(BF)
            grad_v = nn(probs.astype(BF), ds[ALL])
            grad_k = nn(d_scores, qs[ALL])
            folded = nn(jnp.transpose(k_rows), d_scores)
            grad_q = jnp.transpose(jnp.where(low_rows, folded[:, :SPAN], folded[:, SPAN:TILE]))[:PAD]
            for third, value in enumerate((grad_q, grad_k, grad_v)):
                rounded = value.astype(BF)
                grads[third, rows, cols] = rounded
                by_core[rows, p * TRIPLE + third * LANES:p * TRIPLE + third * LANES + LANES] = rounded
                out.append(sum_rows(value))
        return tuple(t + n for t, n in zip(sums, out))

    zero = jnp.zeros((ONE, LANES), F32)
    bias_sums = loop(SEQS, seq, (zero,) * 6, unroll=2)
    for p in SIDES:
        for third in range(THIRDS):
            at = pl.multiple_of(third * WIDTH + g * GROUP + p * LANES, LANES)
            biases[:, pl.ds(at, LANES)] = bias_sums[3 * p + third]
    poll(((2, 3), (1, 1), (0, 0)))
    stage = g + 1

    ring.reopen_box()

    w = nn(turned[ALL], by_core[ALL])
    for part in range(THIRDS):
        both = [w[:, at:at + LANES].reshape(CUBE + BLOCK) for at in (part * LANES, TRIPLE + part * LANES)]
        ring.outbox[part] = jnp.where(rep == 0, both[1], both[0])
        ring.acc[stage % ATT_SLOTS, part] = jnp.where(rep == 0, both[0], both[1])
    ring.pair(THIRDS).start()

    def chunk(i, carry):
        at = pl.ds(pl.multiple_of(i * CHUNK, PACK), CHUNK)
        dh[at, :] += nt(grads[0, at, :], wq_ref[ALL]) + nt(grads[1, at, :], wk_ref[ALL]) + nt(grads[2, at, :], wv_ref[ALL])
        return carry

    loop(ROWS // CHUNK, chunk, 0)

    def exchange(dim, landing, at, number):
        copies = []
        for hops in range(ONE, 4):
            index = list(at)
            index[dim] = (place[dim] + hops) % RING
            copies.append(pltpu.make_async_remote_copy(
                src_ref=blocks.at[tuple(index)], dst_ref=landing.at[hops - 1], send_sem=small_send.at[number + hops],
                recv_sem=small_recv.at[number + hops], device_id=(rep, flat_of(along(place, dim, hops))),
                device_id_type=MESH_ID))
        return copies

    def start(copies):
        for copy in copies:
            copy.start()
        return copies

    def collect(copies, dim, landing, at):
        for copy in copies:
            copy.wait()
        index = list(at)
        index[dim] = place[dim]
        index = tuple(index)
        blocks[index] = blocks[index] + landing[0] + landing[1] + landing[2]

    @pl.when(g == GROUPS - 1)
    def _():
        def tail(*todo):
            for stage, at in todo:
                level(stage, orders, at)

        gain = vec_ref[:1, :]
        tail((2, 2), (3, 1), (4, 0))
        sums[ALL] = gvin_ref[ALL]
        def norm_one(s, carry):
            padded(xp, 0, x_ref, s)
            here = pl.ds(pl.multiple_of(s * PAD, PACK), PAD)
            centered, rstd = row_stats(xp[ALL])
            xhat = centered * rstd
            d = dh[here, :]
            dxp[ALL] = (gr_ref[here, :] + norm_back(d * gain, xhat, rstd)).astype(BF)
            for k, value in enumerate((d * xhat, d)):
                sums[k:k + 1, :] += sum_rows(value)
            dx_ref[s] = dxp[:TOKENS]

            @pl.when(s == 3)
            def _():
                tail((2, 3), (3, 2))

            return carry

        loop(SEQS, norm_one, 0)
        small_blocks(blocks, sums, biases, gbup_ref)
        at = [EVERY] * 3
        number = 0
        def shard_order():
            for j in range(SUBS):
                turned[:, j * LANES:j * LANES + LANES] = unit_columns(j)
                for b in range(4):
                    for h in SIDES:
                        xp[b * PACK + h * SUBS:b * PACK + h * SUBS + SUBS, j * LANES:j * LANES + LANES] = gup_ref[h, j * 4 + b]
            left = xp[:SHARDS]
            total = jnp.zeros_like(left)
            for _ in AXES:
                piece = left.astype(BF)
                total = total + nt(piece, turned[:, :WIDTH])
                left = left - piece.astype(F32)
            for b in range(4):
                up_ref[:, b * WIDTH:b * WIDTH + WIDTH] = total[b * 16:b * PACK + PACK]

        for dim, landing, todo in ((2, from_x, ((4, 1),)), (1, from_y, ((3, 3),)), (0, from_z, ((4, 2),))):
            copies = start(exchange(dim, landing, at, number))
            if dim == 1:
                shard_order()
            tail(*todo)
            collect(copies, dim, landing, at)
            at[dim] = place[dim]
            number += 3
        last = pltpu.make_async_remote_copy(
            src_ref=blocks.at[place], dst_ref=from_pair, send_sem=small_send.at[FIRST], recv_sem=small_recv.at[FIRST],
            device_id=ring.partner, device_id_type=MESH_ID)
        last.start()
        tail((4, 3))
        last.wait()
        small_ref[ALL] = blocks[place] + from_pair[ALL]
        ring.settle(0, ATT_PARTS)
        for stage in range(ONE, ATT_STAGES):
            ring.settle(stage, THIRDS)


def attn_bwd(qkv, do, h, w_qkv, o, da, x, gr, vec, gvin, gbup, gup):
    one = lambda shape: pl.BlockSpec(shape, lambda g: (0,) * len(shape), pipeline_mode=ONCE)
    third = lambda t: pl.BlockSpec((ROWS, GROUP), lambda g: (0, g // 2 * 6 + t * 2 + g % 2))
    wthird = lambda t: pl.BlockSpec((WIDTH, GROUP), lambda g: (0, t * GROUPS + g))
    col = pl.BlockSpec((ROWS, GROUP), lambda g: (0, g))
    anywhere = ANYWHERE
    shape = jax.ShapeDtypeStruct
    rows = (SUBS, LANES)
    vmem, dma = VM, pltpu.SemaphoreType.DMA
    return pl.pallas_call(
        attn_bwd_kernel, grid=(GROUPS,),
        out_shape=[shape((2, 3 * SUBS) + rows, F32), shape((2, SUBS) + rows, F32), shape((SEQS, TOKENS, WIDTH), BF), shape(rows, F32), shape((PACK, HIDDEN), F32)],
        in_specs=[third(0), third(1), third(2), col, one((ROWS, WIDTH)), wthird(0), wthird(1), wthird(2),
                  one((ROWS, WIDTH)), one((ROWS, WIDTH)), one((SEQS, TOKENS, WIDTH)), one((ROWS, WIDTH)),
                  one((SUBS, WIDTH)), one((SUBS, WIDTH)), one((SUBS, TILE)), one(gup.shape)],
        out_specs=[anywhere, anywhere, one((SEQS, TOKENS, WIDTH)), one(rows), one((PACK, HIDDEN))],
        scratch_shapes=[vmem((ROWS, WIDTH), F32), vmem((THIRDS, ROWS, GROUP), BF), vmem((ROWS, 3 * GROUP), BF),
                        vmem((WIDTH, ROWS), BF), vmem((2, TILE, LANES), BF), vmem((2, TILE, LANES), BF),
                        vmem((PAD, WIDTH), F32), vmem((PAD, WIDTH), BF), vmem((SUBS, WIDTH), F32), vmem((1, 3 * WIDTH), F32),
                        vmem(CUBE + rows, F32), vmem((3, 4, 4) + rows, F32), vmem((3, 4) + rows, F32),
                        vmem((3,) + rows, F32), vmem(rows, F32), dma((10,)), dma((10,))]
        + ring_scratch(ATT_SLOTS, ATT_STAGES, ATT_PARTS),
        compiler_params=pltpu.CompilerParams(vmem_limit_bytes=VMEM_CAP, collective_id=2, has_side_effects=True),
        name="attn_bwd",
    )(qkv, qkv, qkv, do, h, w_qkv, w_qkv, w_qkv, o, da, x, gr, vec, gvin, gbup, gup)


def layer(x, dz, w_qkv, b_qkv, w_out, w_up, b_up, w_down, vec_params):
    h1, qkv, o, a, h2, dm, vec, b_up, w_qkv, w_out, w_up, w_down = first(
        x, dz, (w_qkv, w_out, w_up, w_down), (b_qkv[None], b_up[None], vec_params))
    w_qkv, w_out, w_up = (w.reshape(WIDTH, -1) for w in (w_qkv, w_out, w_up))
    gw_up, gw_down, gb_up, z, gr, da, do, gvec = mlp(h2, dm, w_up, b_up, w_down, x, dz, a, w_out, vec)
    gw_qkv, gw_out, dx, small, gw_up = attn_bwd(qkv, do, h1, w_qkv, o, da, x, gr, vec, gvec, gb_up, gw_up)
    plain = lambda g: g.swapaxes(1, 2).reshape(g.shape[0] * SUBS, -1)
    return (z, dx, plain(gw_qkv), small[0, 16:SHARDS], plain(gw_out), gw_up, small[:, 64:72].reshape(SHARDS),
            plain(gw_down), small[:, :PACK])


def solution(mesh):
    batch = P(("rep", "fsdp"), None, None)
    rows, flat = P("fsdp", None), P("fsdp")
    params = (rows, flat, rows, rows, flat, rows, P(None, "fsdp"))
    return jax.shard_map(layer, mesh=mesh, in_specs=(batch, batch) + params, out_specs=(batch, batch) + params, check_vma=False)
```

```python
import jax
import jax.numpy as jnp
from jax import lax
from jax.experimental import pallas as pl
from jax.experimental.pallas import tpu as pltpu
from jax.sharding import PartitionSpec as P

LN_EPS = 1e-5

ALL = ...
FIRST, ONE, PAIR, THREE = range(4)
PACK, SHARDS, FLAT, LANES, SPAN, TRIPLE, TILE = 16, 64, 192, 128, 256, 384, 512
SUBS, RING = 8, 4
CUBE, BLOCK = (RING,) * 3, (2, SUBS, LANES)
AXES, SIDES = range(3), range(2)
ONCE = pl.Buffered(ONE)
ANYWHERE = pl.BlockSpec(memory_space=pl.ANY)
VM = pltpu.VMEM
KEEP = True
UNIT, NIL = 1.0, 0.0
TILE_SHAPE = BLOCK[ONE:]


def row(ref, k):
    return ref[k:k + ONE, :]


def other(rep):
    return ONE - rep


def iota(dims, axis):
    return lax.broadcasted_iota(jnp.int32, dims, axis)


def loop(count, body, start, **options):
    return lax.fori_loop(FIRST, count, body, start, **options)


def sum_rows(t):
    return jnp.sum(t, axis=FIRST, keepdims=KEEP)


def max_rows(t):
    return jnp.max(t, axis=FIRST, keepdims=KEEP)


def sum_lanes(t):
    return jnp.sum(t, axis=-ONE, keepdims=KEEP)


def max_lanes(t):
    return jnp.max(t, axis=-ONE, keepdims=KEEP)


def mean_lanes(t):
    return jnp.mean(t, axis=-ONE, keepdims=KEEP)


SEQS, TOKENS, PAD, WIDTH, HIDDEN = 6, 197, 208, 1024, 4096
ROWS = SEQS * PAD
BF, F32 = jnp.bfloat16, jnp.float32
VMEM_CAP = 67043328


def nn(a, b):
    return lax.dot_general(a, b, (((1,), (0,)), ((), ())), preferred_element_type=F32)


def nt(a, b):
    return lax.dot_general(a, b, (((1,), (1,)), ((), ())), preferred_element_type=F32)


def tn(a, b):
    return lax.dot_general(a, b, (((0,), (0,)), ((), ())), preferred_element_type=F32)


def row_stats(t):
    mean = mean_lanes(t)
    centered = t - mean
    variance = mean_lanes(centered * centered)
    return centered, lax.rsqrt(variance + LN_EPS)


def norm_back(dt, xhat, rstd):
    return rstd * (dt - mean_lanes(dt) - xhat * mean_lanes(dt * xhat))


def head_halves(width=LANES):
    lane = iota((1, width), 1)
    return lane < SHARDS


def stack_heads(dst, rows, low):
    zero = jnp.zeros_like(rows)
    dst[:PAD] = jnp.where(low, rows, zero)
    dst[SPAN:SPAN + PAD] = jnp.where(low, zero, rows)


def padded(dst, base, rows_ref, s):
    dst[base + FLAT:base + PAD] = jnp.zeros((PACK, WIDTH), dst.dtype)
    dst[base:base + TOKENS] = rows_ref[s].astype(dst.dtype)


MESH_ID = pl.DeviceIdType.MESH
ORDERS = ((2, 1, 0), (1, 0, 2), (0, 2, 1))
HOPS = (1, 2, 3)
GREETED = 10
FAR, NEAR, DIRECT = "far", "near", "direct"
EVERY = slice(None)


def my_place():
    rep, flat = lax.axis_index("rep"), lax.axis_index("fsdp")
    return rep, (flat // PACK, (flat // RING) % RING, flat % RING)


def along(place, dim, shift):
    moved = list(place)
    moved[dim] = (place[dim] + shift) % RING
    return tuple(moved)


def flat_of(place):
    return place[0] * PACK + place[1] * RING + place[2]


def greet(sem, rep, place):
    pl.semaphore_signal(sem, inc=1, device_id=(other(rep), flat_of(place)), device_id_type=MESH_ID)
    for dim in AXES:
        for shift in HOPS:
            pl.semaphore_signal(sem, inc=1, device_id=(rep, flat_of(along(place, dim, shift))), device_id_type=MESH_ID)


def entry_barrier(rep, place):
    barrier = pltpu.get_barrier_semaphore()
    greet(barrier, rep, place)
    pl.semaphore_wait(barrier, GREETED)


def ring_scratch(slots, stages, parts):
    dma = pltpu.SemaphoreType.DMA
    block = BLOCK
    cube, square, line = CUBE, CUBE[1:], CUBE[2:]
    sides = (parts, 3)
    buffers = [(slots, parts) + cube + block, (parts,) + cube + block, (parts,) + cube + block,
               (stages, parts) + square + block,
               (slots,) + sides + square + block, (stages,) + sides + line + block, (stages,) + sides + block]
    sems = [()] * PAIR + [(slots, 2)] * PAIR + [(stages, 2)] * PAIR + [(stages,)] * THREE
    regular = pltpu.SemaphoreType.REGULAR
    return [VM(b, F32) for b in buffers] + [dma(s) for s in sems] + [regular((slots,)), regular]


class Ring:
    def __init__(self, refs, slots, steps, window):
        (self.acc, self.inbox, self.outbox, self.rest, land0, land1, land2, self.pair_send, self.pair_recv,
         self.send, self.recv, self.rest_send, self.rest_recv, self.out_sem, self.out_send, self.out_recv,
         self.free, self.emptied) = refs
        self.landing = (land0, land1, land2)
        self.slots, self.steps, self.last = slots, steps, len(steps)
        self.window = window
        self.rep, self.place = my_place()
        self.partner = (other(self.rep), flat_of(self.place))

    def across(self, ref, send, recv, into=None):
        return pltpu.make_async_remote_copy(
            src_ref=ref, dst_ref=ref if into is None else into, send_sem=send, recv_sem=recv, device_id=self.partner,
            device_id_type=MESH_ID)

    def pair(self, parts):
        some = pl.ds(FIRST, parts)
        return self.across(self.outbox.at[some], self.pair_send, self.pair_recv, self.inbox.at[some])

    def sems(self, stage, step):
        phase, kind = step
        if phase:
            at = (stage, phase - 1)
            return self.rest_send.at[at], self.rest_recv.at[at]
        at = (stage % self.slots, 1 if kind == NEAR else 0)
        return self.send.at[at], self.recv.at[at]

    def landed(self, stage, parts, step):
        phase, kind = step
        at = self.home(stage, 0, phase)[1][:1] + (pl.ds(FIRST, parts),)
        sides = {FAR: 2, NEAR: pl.ds(FIRST, 2), DIRECT: EVERY}[kind]
        return self.across(self.landing[phase].at[at + (sides,)], *self.sems(stage, step))

    def axis(self, order, phase, index):
        at = {dim: EVERY for dim in order}
        for dim in order[:phase]:
            at[dim] = self.place[dim]
        at[order[phase]] = index
        if phase:
            del at[order[0]]
        return tuple(at[dim] for dim in sorted(at))

    def home(self, stage, part, phase):
        if phase:
            return self.rest, (stage, part)
        return self.acc, (stage % self.slots, part)

    def hops(self, stage, part, order, step):
        phase, kind = step
        dim = order[phase]
        memory, at = self.home(stage, part, phase)
        send, recv = self.sems(stage, step)
        found = []
        for side, shift in enumerate((1, 3) if kind != DIRECT else HOPS):
            source, target, place = shift, 0, at + (side,)
            if kind == FAR:
                source, target = 2, shift
            src = at + self.axis(order, phase, (self.place[dim] + source) % RING)
            into = at + self.axis(order, phase, (self.place[dim] + target) % RING)
            if kind == FAR:
                src, into, place = src + (side,), into + (side,), at + (2,) + (EVERY, EVERY, side)
            copy = pltpu.make_async_remote_copy(
                src_ref=memory.at[src], dst_ref=self.landing[phase].at[place], send_sem=send, recv_sem=recv,
                device_id=(self.rep, flat_of(along(self.place, dim, shift))), device_id_type=MESH_ID)
            found.append((copy, into, place))
        return found

    def results(self, stage, orders):
        for part, order in orders.items():
            src = self.rest.at[(stage, part) + tuple(self.place[dim] for dim in sorted(order[1:]))]
            dst = self.window(stage, part)
            pltpu.make_async_copy(src, dst, self.out_sem.at[stage]).start()
            self.across(src, self.out_send.at[stage], self.out_recv.at[stage], dst).start()

    def level(self, stage, level, orders, credit, refill):
        if level == 0:
            self.pair(len(orders)).wait()
            for part in orders:
                at = (stage % self.slots, part)
                for z in range(4):
                    self.acc[at + (z,)] = self.acc[at + (z,)] + self.inbox[part, z]

            @pl.when(stage >= self.slots)
            def _():
                pl.semaphore_wait(self.free.at[stage % self.slots], GREETED)

            @pl.when(refill)
            def _():
                pl.semaphore_signal(self.emptied, inc=1, device_id=self.partner, device_id_type=MESH_ID)
        else:
            step = self.steps[level - 1]
            phase, kind = step
            self.landed(stage, len(orders), step).wait_recv()
            for part, order in orders.items():
                memory = self.home(stage, part, phase)[0]
                hops = self.hops(stage, part, order, step)
                if kind == FAR:
                    for _, into, place in hops:
                        memory[into] = memory[into] + self.landing[phase][place]
                    continue
                into = hops[0][1]
                total = memory[into]
                for _, _, place in hops:
                    total = total + self.landing[phase][place]
                if phase:
                    memory[into] = total
                else:
                    self.rest[stage, part] = total
            if phase == 0 and kind != FAR:
                self.sent(stage, orders, (0,))

                @pl.when(credit)
                def _():
                    greet(self.free.at[stage % self.slots], self.rep, self.place)
        if level < self.last:
            for part, order in orders.items():
                for copy, _, _ in self.hops(stage, part, order, self.steps[level]):
                    copy.start()
        else:
            self.results(stage, orders)
            self.sent(stage, orders, (1, 2))

    def sent(self, stage, orders, phases):
        for step in self.steps:
            if step[0] in phases:
                self.landed(stage, len(orders), step).wait_send()

    def settle(self, stage, parts):
        ref = self.rest.at[stage, pl.ds(FIRST, parts), 0, 0]
        pltpu.make_async_copy(ref, ref, self.out_sem.at[stage]).wait()
        self.across(ref, self.out_send.at[stage], self.out_recv.at[stage]).wait()

    def reopen_box(self):
        pl.semaphore_wait(self.emptied, 1)


THIRDS = 3
PIECE = TILE
QKV, OUT, UP, DOWN, SMALL = range(5)


def gather_items():
    items = [(half, QKV, 0, third * WIDTH + half * PIECE, PIECE // PAIR, PIECE // PAIR, ORDERS[third])
             for half in SIDES for third in range(THIRDS)]
    rest = [(OUT, 0, 0, PIECE)]
    rest += [(UP, 0, PIECE * j, HIDDEN // PAIR) for j in range(4)]
    rest += [(DOWN, PACK * j, 0, PIECE) for j in range(4)]
    items += [(2 + k // THREE,) + piece + (PIECE, ORDERS[k % THREE]) for k, piece in enumerate(rest)]
    return items + [(0, SMALL, 0, 0, 0, 0, ORDERS[0])]


def small_rows(table, vec, b_qkv, b_up):
    lane = iota((SUBS, LANES), ONE)

    def moved(f, half, shift):
        return pltpu.roll(table[f // PACK, f // RING % RING, f % RING, half], shift % LANES, ONE)

    def fill(ref, tile, owners, half, width, first):
        total = jnp.zeros((SUBS, LANES), F32)
        for f in owners:
            start = width * f - LANES * tile
            here = jnp.logical_and(lane >= start, lane < start + width)
            total = jnp.where(here, moved(f, half, start - first), total)
        ref[:, tile * LANES:tile * LANES + LANES] = total[:ref.shape[0]]

    for tile in range(WIDTH // LANES):
        fill(vec, tile, range(SUBS * tile, SUBS * tile + SUBS), 0, PACK, 0)
    for tile in range(TILE // LANES):
        fill(b_up, tile, range(PACK * tile, PACK * tile + PACK), 1, SUBS, 0)
    for tile in range(THREE * WIDTH // LANES):
        fill(b_qkv, tile, range(LANES * tile // 48, (LANES * tile + LANES - 1) // 48 + 1), 0, 48, PACK)


def placed(values, first, period=LANES):
    size = values.shape[ONE]
    lane = iota((size, LANES), ONE)
    row = iota((size, LANES), FIRST)
    return nn(values.astype(BF), jnp.where(lane == row % period + first, UNIT, NIL).astype(BF))


def unit_columns(j):
    column = iota((WIDTH, LANES), ONE)
    row = iota((WIDTH, LANES), FIRST)
    taken = row == SHARDS * (column // SUBS) + SUBS * j + column % SUBS
    return jnp.where(taken, UNIT, NIL).astype(BF)


def first_kernel(x_ref, dz_ref, sq_ref, so_ref, su_ref, sd_ref, bq_ref, bu_ref, sv_ref,
                 h1_hbm, qkv_ref, o_hbm, a_ref, h2_ref, dm_ref, vec_ref, bup_ref, wq_hbm, wo_hbm, wu_hbm, wd_hbm,
                 wq, wo, su, sd, packed, table, bias, xhat, kst, vst, xp,
                 own_sem, send_sem, recv_sem, pair_send, pair_recv, save_sem, h1_ref, o_ref, o_sem):
    t = pl.program_id(0)
    rep, place = my_place()
    partner = (other(rep), flat_of(place))
    items = gather_items()
    fulls = (wq, wo, wu_hbm, wd_hbm, table)

    def block(item, shards, half=None):
        _, array, row, first, step, cols, _ = items[item]
        if array == SMALL:
            return table.at[shards + ((half,) if half is not None else ())]
        col = rep * step + first
        if half is not None:
            cols = cols // PAIR
            col = col + half * cols
        return fulls[array].at[shards + (pl.ds(row, PACK), pl.ds(pl.multiple_of(col, LANES), cols))]

    def shard(item):
        _, array, row, first, step, _, _ = items[item]
        return (su, sd)[array - UP].at[pl.ds(row, PACK), pl.ds(pl.multiple_of(rep * step + first, LANES), PIECE)]

    def own(item):
        return pltpu.make_async_copy(shard(item), block(item, place), own_sem.at[item])

    def pair(item):
        everywhere = block(item, (EVERY,) * THREE)
        return pltpu.make_async_remote_copy(
            src_ref=everywhere, dst_ref=everywhere, send_sem=pair_send.at[item], recv_sem=pair_recv.at[item],
            device_id=partner, device_id_type=MESH_ID)

    def hops(item, level):
        array, order = items[item][ONE], items[item][-1]
        phase, second = level // PAIR, level % PAIR
        dim = order[phase]
        found = []
        for side, shift in enumerate((1, 3)):
            at = [EVERY] * THREE
            for later in order[phase:]:
                at[later] = place[later]
            if second:
                at[dim] = (place[dim] + 4 - shift) % RING
            dst = block(item, tuple(at), side if second else None)
            src = shard(item) if level == 0 and array in (UP, DOWN) else dst
            found.append(pltpu.make_async_remote_copy(
                src_ref=src, dst_ref=dst, send_sem=send_sem.at[item, level], recv_sem=recv_sem.at[item, level],
                device_id=(rep, flat_of(along(place, dim, shift))), device_id_type=MESH_ID))
        return found

    def both(item, level):
        order = items[item][-1]
        phase, second = level // PAIR, level % PAIR
        at = [EVERY] * THREE
        for later in order[phase:]:
            at[later] = place[later]
        if not second:
            at[order[phase]] = pl.ds(FIRST, 2)
        ref = block(item, tuple(at))
        return pltpu.make_async_remote_copy(
            src_ref=ref, dst_ref=ref, send_sem=send_sem.at[item, level], recv_sem=recv_sem.at[item, level],
            device_id=partner, device_id_type=MESH_ID)

    def advance(*todo):
        for stage, level in todo:
            for item in range(len(items)):
                if items[item][FIRST] != stage:
                    continue
                if level:
                    both(item, level - 1).wait_recv()
                if level == 2 and items[item][ONE] in (UP, DOWN):
                    own(item).wait()
                if level == 6:
                    if items[item][ONE] != SMALL:
                        pair(item).start()
                else:
                    for copy in hops(item, level):
                        copy.start()

    def arrived(*stages):
        for item in range(len(items)):
            if items[item][FIRST] in stages and items[item][ONE] != SMALL:
                pair(item).wait_recv()

    def saves():
        return (pltpu.make_async_copy(wq, wq_hbm, save_sem.at[FIRST]), pltpu.make_async_copy(wo, wo_hbm, save_sem.at[1]),
                pltpu.make_async_copy(h1_ref, h1_hbm, save_sem.at[2]))

    def heads_out(number):
        rows = pl.ds(number * (PAIR * PAD), PAIR * PAD)
        return pltpu.make_async_copy(o_ref.at[rows], o_hbm.at[rows], o_sem.at[number])

    @pl.when(t == FIRST)
    def _():
        for _, array, _, first, step, width, _ in items:
            if array in (QKV, OUT):
                cols = pl.ds(pl.multiple_of(rep * step + first, LANES), width)
                (wq, wo)[array][place + (EVERY, cols)] = (sq_ref, so_ref)[array][:, cols].astype(BF)
        for b in range(4):
            packed[b * 16:b * PACK + PACK] = su_ref[:, b * WIDTH:b * WIDTH + WIDTH].astype(BF)
        sd[ALL] = sd_ref[ALL].astype(BF)
        first_row = iota((SUBS, 48), 0) == 0
        table[place + (0,)] = placed(sv_ref[ALL], 0) + placed(jnp.where(first_row, bq_ref[ALL], NIL), PACK)
        unit = iota((SUBS, SHARDS), ONE) // SUBS == iota((SUBS, SHARDS), FIRST)
        table[place + (1,)] = placed(jnp.where(unit, bu_ref[ALL], NIL), 0, SUBS)
        entry_barrier(rep, place)
        advance((0, 0), (1, 0))
        for j in range(SUBS):
            turned = nn(packed[ALL], unit_columns(j)).astype(BF)
            for b in range(4):
                su[:, j * TILE + b * LANES:j * TILE + b * LANES + LANES] = turned[b * 16:b * PACK + PACK]
        for item in range(len(items)):
            if items[item][ONE] in (UP, DOWN):
                own(item).start()
        later = (2, 3, 4)
        advance(*((stage, 0) for stage in later))
        everything = (0, 1) + later
        for s, todo in enumerate((
                [(stage, 1) for stage in everything], [(stage, 2) for stage in everything], [(0, 3), (1, 3)],
                [(0, 4), (1, 4)] + [(stage, 3) for stage in later], [(0, 5), (2, 4)], [(0, 6), (1, 5)])):
            base = s * PAD
            xp[FLAT:PAD] = jnp.zeros((PACK, WIDTH), BF)
            xp[:TOKENS] = x_ref[s]
            centered, rstd = row_stats(xp[ALL].astype(F32))
            xhat[base:base + PAD] = centered * rstd
            advance(*todo)
        small_rows(table, vec_ref, bias, bup_ref)
        real = iota((PAD, 1), 0) < TOKENS

        def scaled(s, carry):
            here = pl.ds(pl.multiple_of(s * PAD, PACK), PAD)
            h1_ref[here, :] = jnp.where(real, xhat[here, :] * vec_ref[:1, :] + row(vec_ref, 1), NIL).astype(BF)
            return carry

        loop(SEQS, scaled, 0)
        kst[ALL] = jnp.zeros_like(kst)
        vst[ALL] = jnp.zeros_like(vst)

    half, seqs = jnp.maximum(t - ONE, FIRST) // THREE, jnp.maximum(t - ONE, FIRST) % THREE
    base = pl.multiple_of(seqs * (PAIR * PAD), PACK)

    @pl.when(t == 1)
    def _():
        arrived(0)
        saves()[2].start()

    @pl.when(t == 4)
    def _():
        arrived(1)
        saves()[0].start()

    @pl.when(t > FIRST)
    def _():
        for third in range(THIRDS):
            cols = pl.ds(pl.multiple_of(third * WIDTH + half * PIECE, PIECE), PIECE)
            weights = wq[:, :, :, :, cols].reshape(WIDTH, PIECE)
            qkv = nn(h1_ref[pl.ds(base, PAIR * PAD), :], weights) + bias[:, cols]
            qkv_ref[:, third * PIECE:third * PIECE + PIECE] = qkv.astype(BF)

    @pl.when(t == 1)
    def _():
        advance((3, 4))

    low = head_halves()
    visible = iota((1, SPAN), 1) < TOKENS

    half_cols = half * PIECE

    def head_pair(p, carry):
        def cols(third):
            return pl.ds(pl.multiple_of(third * PIECE + p * LANES, LANES), LANES)

        for s in SIDES:
            rows = pl.ds(s * PAD, PAD)
            stack_heads(kst.at[s], qkv_ref[rows, cols(1)], low)
            stack_heads(vst.at[s], qkv_ref[rows, cols(2)], low)
        for s in SIDES:
            rows = pl.ds(s * PAD, PAD)
            scores = nt(qkv_ref[rows, cols(0)], kst[s])
            probs = []
            for head in SIDES:
                part = jnp.where(visible, scores[:, head * SPAN:head * SPAN + SPAN], -jnp.inf)
                top = max_lanes(part)
                e = jnp.exp((part - top) * 0.125)
                probs.append((e * (1.0 / sum_lanes(e))).astype(BF))
            here = pl.ds(pl.multiple_of(base + s * PAD, PACK), PAD)
            heads = pl.ds(pl.multiple_of(half_cols + p * LANES, LANES), LANES)
            o_ref[here, heads] = nn(jnp.concatenate(probs, axis=1), vst[s]).astype(BF)
        return carry

    def two_pairs(i, carry):
        head_pair(PAIR * i, carry)
        head_pair(PAIR * i + 1, carry)
        for step, turn, todo in ((1, 0, (1, 6)), (1, 1, (2, 5)), (2, 0, (4, 4)), (2, 1, (3, 5)), (3, 0, (2, 6)),
                                 (4, 1, (4, 5)), (5, 0, (3, 6)), (5, 1, (4, 6))):
            @pl.when(jnp.logical_and(t == step, i == turn))
            def _(todo=todo):
                advance(todo)

        return carry

    @pl.when(t > FIRST)
    def _():
        loop(2, two_pairs, 0)

    for number in AXES:
        @pl.when(t == 4 + number)
        def _(number=number):
            heads_out(number).start()

    @pl.when(t == 4)
    def _():
        arrived(2)
        saves()[1].start()

    @pl.when(t > 3)
    def _():
        for s in SIDES:
            padded(xp, 0, x_ref, PAIR * seqs + s)
            xhat[s * PAD:s * PAD + PAD] = xp[ALL].astype(F32)
            dm_ref[s * PAD + FLAT:s * PAD + PAD] = jnp.zeros((PACK, WIDTH), BF)
            dm_ref[s * PAD:s * PAD + TOKENS] = (dz_ref[s].astype(F32) * row(vec_ref, 7)).astype(BF)
        a_ref[ALL] = nn(o_ref[pl.ds(base, PAIR * PAD), :], wo[ALL].reshape(WIDTH, WIDTH)) + row(vec_ref, 2)

        def rows(i, carry):
            at = pl.ds(pl.multiple_of(i * 32, 32), 32)
            y = xhat[at, :] + row(vec_ref, 3) * a_ref[at, :]
            centered, rstd = row_stats(y)
            h2_ref[at, :] = (centered * rstd * row(vec_ref, 4) + row(vec_ref, 5)).astype(BF)
            return carry

        loop(PAIR * PAD // 32, rows, 0, unroll=13)

    @pl.when(t == 6)
    def _():
        arrived(3, 4)
        for item in range(len(items)):
            if items[item][ONE] != SMALL:
                pair(item).wait_send()
            for level in range(6):
                both(item, level).wait_send()
        for copy in saves():
            copy.wait()
        for number in AXES:
            heads_out(number).wait()


def first(x, dz, shards, small):
    whole = lambda dims: pl.BlockSpec(dims, lambda t: (0,) * len(dims), pipeline_mode=ONCE)
    pair = lambda t: jnp.maximum(t - RING, FIRST)
    past = lambda t: jnp.maximum(t - ONE, FIRST)
    rows = pl.BlockSpec((PAIR * PAD, WIDTH), lambda t: (pair(t), 0))
    halves = pl.BlockSpec((PAIR * PAD, THREE * PIECE), lambda t: (past(t) % THREE, past(t) // THREE))
    anywhere = ANYWHERE
    shape, vmem, dma = jax.ShapeDtypeStruct, VM, pltpu.SemaphoreType.DMA
    n = len(gather_items())
    cube = CUBE
    return pl.pallas_call(
        first_kernel, grid=(7,),
        out_shape=[shape((ROWS, WIDTH), BF), shape((ROWS, THREE * WIDTH), BF), shape((ROWS, WIDTH), BF), shape((ROWS, WIDTH), F32),
                   shape((ROWS, WIDTH), BF), shape((ROWS, WIDTH), BF), shape((SUBS, WIDTH), F32), shape((SUBS, TILE), F32)]
        + [shape(cube + s.shape, BF) for s in shards],
        in_specs=[whole((SEQS, TOKENS, WIDTH)), pl.BlockSpec((2, TOKENS, WIDTH), lambda t: (pair(t), 0, 0))]
        + [whole(s.shape) for s in shards + small],
        out_specs=[anywhere, halves, anywhere, rows, rows, rows,
                   whole((SUBS, WIDTH)), whole((SUBS, TILE))] + [anywhere] * RING,
        scratch_shapes=[vmem(cube + shards[QKV].shape, BF), vmem(cube + shards[OUT].shape, BF), vmem(shards[UP].shape, BF),
                        vmem(shards[DOWN].shape, BF), vmem((SHARDS, WIDTH), BF), vmem(cube + (2, SUBS, LANES), F32), vmem((1, THREE * WIDTH), F32),
                        vmem((ROWS, WIDTH), F32), vmem((2, PIECE, LANES), BF), vmem((2, PIECE, LANES), BF),
                        vmem((PAD, WIDTH), BF),
                        dma((n,)), dma((n, 6)), dma((n, 6)), dma((n,)), dma((n,)), dma((3,)), vmem((ROWS, WIDTH), BF), vmem((ROWS, WIDTH), BF), dma((3,))],
        compiler_params=pltpu.CompilerParams(vmem_limit_bytes=VMEM_CAP, collective_id=FIRST, has_side_effects=True),
        name="first",
    )(x, dz, *shards, *small)


CHUNK = 624
TILES = HIDDEN // TILE
MLP_SLOTS, MLP_PARTS = 3, 4
MLP_STEPS = ((0, FAR), (0, NEAR), (1, DIRECT), (2, DIRECT))


def gelu_and_slope(u):
    cdf = 0.5 * (1.0 + lax.erf(u * (2.0 ** -0.5)))
    pdf = jnp.exp(u * u * -0.5) * ((2.0 * jnp.pi) ** -0.5)
    return u * cdf, cdf + u * pdf


def mlp_kernel(h_ref, dm_ref, w1_ref, w2_ref, b1_ref, x_ref, dz_ref, a_ref, wo_ref, vec_ref,
               gw1_ref, gw2_ref, gb_ref, z_ref, gr_ref, da_ref, do_ref, gv_ref,
               m_acc, dh_acc, act, dpre, turned, xp, zp, zo, *ring_refs):
    j = pl.program_id(0)

    def window(stage, part):
        if part < 2:
            return gw2_ref.at[stage, pl.ds(rep * RING + part * PAIR, 2)]
        return gw1_ref.at[:, stage * RING + rep * PAIR + part - 2]

    ring = Ring(ring_refs, MLP_SLOTS, MLP_STEPS, window)
    rep = ring.rep
    every_part = range(MLP_PARTS)

    def run(lag, level):
        stage = j - lag
        for turn in AXES:
            orders = {part: ORDERS[(turn + part) % THREE] for part in every_part}

            @pl.when(jnp.logical_and(jnp.logical_and(stage >= 0, stage < TILES), stage % THREE == turn))
            def _(orders=orders):
                ring.level(stage, level, orders, stage < TILES - MLP_SLOTS, stage < TILES - 1)

    @pl.when(j == FIRST)
    def _():
        entry_barrier(rep, ring.place)
        m_acc[ALL] = jnp.zeros_like(m_acc)
        dh_acc[ALL] = jnp.zeros_like(dh_acc)
        turned[ALL] = jnp.transpose(h_ref[ALL])

    def chunk(i, total):
        at = pl.ds(pl.multiple_of(i * CHUNK, PACK), CHUNK)
        w1, w2 = w1_ref[ALL], w2_ref[ALL].reshape(TILE, WIDTH)
        u = nn(h_ref[at, :], w1) + b1_ref[pl.ds(j, 1), :]
        value, slope = gelu_and_slope(u)
        act[at, :] = value.astype(BF)
        d = nt(dm_ref[at, :], w2) * slope
        dpre[at, :] = d.astype(BF)
        return sum_rows(d) + total

    def onward(i, carry):
        at = pl.ds(pl.multiple_of(i * CHUNK, PACK), CHUNK)
        m_acc[at, :] += nn(act[at, :], w2_ref[ALL].reshape(TILE, WIDTH))
        dh_acc[at, :] += nt(dpre[at, :], w1_ref[ALL])
        return carry

    def grads(core, target):
        cols = pl.ds(pl.multiple_of(core * TILE, TILE), TILE)
        g = tn(act[ALL], dm_ref[:, cols])
        for part in SIDES:
            for half in SIDES:
                first = (part * PAIR + half) * LANES
                target(part, half, g[:, first:first + LANES].reshape(CUBE + TILE_SHAPE))

    def grads_up(core, target):
        g = nn(turned[ALL], dpre[:, pl.ds(pl.multiple_of(core * SPAN, SPAN), SPAN)])
        for part in SIDES:
            target(part + 2, EVERY, g[:, part * LANES:part * LANES + LANES].reshape(CUBE + BLOCK))

    for lag in range(ring.last + 1, 0, -1):
        run(lag, lag - 1)

    @pl.when(j < TILES)
    def _():
        gb_ref[pl.ds(j, 1), :] = loop(ROWS // CHUNK, chunk, jnp.zeros((1, TILE), F32))

    @pl.when(j == TILES)
    def _():
        gv_ref[ALL] = jnp.zeros_like(gv_ref)

    @pl.when(j >= TILES)
    def _():
        padded(xp, 0, x_ref, 0)
        padded(zp, 0, dz_ref, 0)
        s1, g2, b2, s2 = (vec_ref[k:k + 1, :] for k in (3, 4, 6, 7))
        here = pl.ds(pl.multiple_of((j - TILES) * PAD, PACK), PAD)
        a = a_ref[ALL]
        y = xp[ALL].astype(F32) + s1 * a
        mlp_out = m_acc[here, :] + b2
        g_out = zp[ALL].astype(F32)
        zo[ALL] = (y + s2 * mlp_out).astype(BF)
        centered, rstd = row_stats(y)
        xhat = centered * rstd
        dh = dh_acc[here, :]
        g_resid = g_out + norm_back(dh * g2, xhat, rstd)
        d_att = g_resid * s1
        gr_ref[ALL] = g_resid
        da_ref[ALL] = d_att.astype(BF)
        for k, total in enumerate((d_att, g_resid * a, dh * xhat, dh, g_out * s2, g_out * mlp_out)):
            gv_ref[2 + k:3 + k, :] += sum_rows(total)
        z_ref[0] = zo[:TOKENS]
        do_ref[ALL] = nt(da_ref[ALL], wo_ref[ALL]).astype(BF)

    @pl.when(j < TILES)
    def _():
        slot = j % MLP_SLOTS

        def out(part, half, value):
            ring.outbox[part, :, :, :, half] = value

        def own(part, half, value):
            ring.acc[slot, part, :, :, :, half] = value

        grads(other(rep), out)
        grads_up(other(rep), out)

        @pl.when(j >= 1)
        def _():
            ring.reopen_box()

        ring.pair(MLP_PARTS).start()
        grads(rep, own)
        grads_up(rep, own)
        loop(ROWS // CHUNK, onward, 0)

    @pl.when(j == TILES + SEQS - 1)
    def _():
        for stage in range(TILES):
            ring.settle(stage, MLP_PARTS)


def mlp(h, dm, w1, b1, w2, x, dz, a, w_out, vec):
    whole = lambda shape: pl.BlockSpec(shape, lambda j: (0, 0), pipeline_mode=ONCE)
    tile = lambda j: jnp.minimum(j, TILES - 1)
    seq = lambda j: jnp.maximum(j - TILES, FIRST)
    b1_spec = whole((SUBS, TILE))
    seqs = pl.BlockSpec((1, TOKENS, WIDTH), lambda j: (seq(j), 0, 0))
    rows = pl.BlockSpec((PAD, WIDTH), lambda j: (seq(j), 0))
    anywhere = ANYWHERE
    shape = jax.ShapeDtypeStruct
    return pl.pallas_call(
        mlp_kernel, grid=(TILES + SEQS,),
        out_shape=[shape((2, HIDDEN // LANES, SUBS, LANES), F32), shape((SUBS, SUBS, SUBS, LANES), F32), shape((SUBS, TILE), F32),
                   shape((SEQS, TOKENS, WIDTH), BF), shape((ROWS, WIDTH), F32), shape((ROWS, WIDTH), BF),
                   shape((ROWS, WIDTH), BF), shape((8, WIDTH), F32)],
        in_specs=[whole((ROWS, WIDTH)), whole((ROWS, WIDTH)), pl.BlockSpec((WIDTH, TILE), lambda j: (0, tile(j))),
                  pl.BlockSpec((SHARDS, SUBS, WIDTH), lambda j: (0, tile(j), 0)), b1_spec, seqs, seqs, rows,
                  whole((WIDTH, WIDTH)), whole((8, WIDTH))],
        out_specs=[anywhere, anywhere, whole((SUBS, TILE)), seqs, rows, rows, rows, whole((8, WIDTH))],
        scratch_shapes=[VM((ROWS, WIDTH), F32), VM((ROWS, WIDTH), F32), VM((ROWS, TILE), BF),
                        VM((ROWS, TILE), BF), VM((WIDTH, ROWS), BF), VM((PAD, WIDTH), BF),
                        VM((PAD, WIDTH), BF), VM((PAD, WIDTH), BF)] + ring_scratch(MLP_SLOTS, TILES, MLP_PARTS),
        compiler_params=pltpu.CompilerParams(vmem_limit_bytes=VMEM_CAP, collective_id=1, has_side_effects=True),
        name="mlp",
    )(h, dm, w1, w2.reshape(SHARDS, SHARDS, WIDTH), b1, x, dz, a, w_out, vec)


GROUP = SPAN
GROUPS = WIDTH // GROUP
ATT_SLOTS, ATT_STAGES, ATT_PARTS = 2, GROUPS + 1, 4
ATT_STEPS = tuple((phase, DIRECT) for phase in AXES)


def small_blocks(target, vec, b_qkv, b_up):
    lane = iota((SUBS, LANES), ONE)

    def turned(ref, tile, first, to):
        return pltpu.roll(ref[:, tile * LANES:tile * LANES + LANES], (to - first) % LANES, ONE)

    for f in range(SHARDS):
        tile, first = divmod(48 * f, LANES)
        bias = turned(b_qkv, tile, first, PACK)
        if first + 48 > LANES:
            bias = jnp.where(lane[:1] < PACK + LANES - first, bias, turned(b_qkv, tile + 1, first, PACK))
        rows = turned(vec, f // SUBS, PACK * (f % SUBS), 0)
        up = turned(b_up, f // PACK, SUBS * (f % PACK), SHARDS)
        target[f // PACK, f // RING % RING, f % RING] = jnp.where(lane < PACK, rows, jnp.where(lane < SHARDS, bias, up))


def attn_bwd_kernel(q_ref, k_ref, v_ref, do_ref, h_ref, wq_ref, wk_ref, wv_ref, o_ref, da_ref, x_ref, gr_ref, vec_ref,
                    gvin_ref, gbup_ref, gup_ref, gw_ref, gwo_ref, dx_ref, small_ref, up_ref,
                    dh, grads, by_core, turned, qst, dst, xp, gr, xs, dxs, seq_sem, dxp, sums, biases, blocks, from_x, from_y, from_z, from_pair,
                    small_send, small_recv, *ring_refs):
    g = pl.program_id(0)

    def window(stage, part):
        if isinstance(stage, int) and stage == 0:
            return gwo_ref.at[:, rep * RING + part]
        return gw_ref.at[:, part * SUBS + (stage - 1) * PAIR + rep]

    ring = Ring(ring_refs, ATT_SLOTS, ATT_STEPS, window)
    rep, place = ring.rep, ring.place
    first_orders = {part: ORDERS[part % THREE] for part in range(ATT_PARTS)}
    orders = {part: ORDERS[part] for part in range(THIRDS)}

    def level(stage, which, at):
        ring.level(stage, at, which, stage < ATT_STAGES - ATT_SLOTS, stage < ATT_STAGES - 1)

    def poll(todo):
        for lag, at in todo:
            @pl.when(g - lag >= 1)
            def _(lag=lag, at=at):
                level(g - lag, orders, at)

            @pl.when(g == lag)
            def _(at=at):
                level(0, first_orders, at)

    @pl.when(g == FIRST)
    def _():
        entry_barrier(rep, place)
        dh[ALL] = jnp.zeros_like(dh)
        qst[ALL] = jnp.zeros_like(qst)
        dst[ALL] = jnp.zeros_like(dst)
        turned[ALL] = jnp.transpose(h_ref[ALL])
        for core, box in ((other(rep), ring.outbox), (rep, ring.acc.at[FIRST])):
            w = tn(o_ref[ALL], da_ref[:, pl.ds(pl.multiple_of(core * TILE, TILE), TILE)])
            for part in range(ATT_PARTS):
                box[part] = w[:, part * LANES:part * LANES + LANES].reshape(CUBE + BLOCK)
            if box is ring.outbox:
                ring.pair(ATT_PARTS).start()

    poll(((2, 2),))
    low = head_halves()
    low_rows = iota((LANES, ONE), 0) < SHARDS
    hidden = iota((PAD, 1), 0) >= TOKENS

    def seq(s, sums):
        rows = pl.ds(pl.multiple_of(s * PAD, PACK), PAD)
        out = []
        for p in SIDES:
            cols = slice(p * LANES, p * LANES + LANES)
            qs, ds = qst.at[p], dst.at[p]
            k_rows, v_rows = k_ref[rows, cols], v_ref[rows, cols]
            stack_heads(qs, q_ref[rows, cols], low)
            stack_heads(ds, do_ref[rows, cols], low)
            scores = jnp.where(hidden, -jnp.inf, nt(k_rows, qs[ALL]))
            top = max_rows(scores)
            e = jnp.exp((scores - top) * 0.125)
            probs = e * (1.0 / sum_rows(e))
            d_probs = nt(v_rows, ds[ALL])
            inner = sum_rows(d_probs * probs)
            d_scores = (probs * (d_probs - inner) * 0.125).astype(BF)
            grad_v = nn(probs.astype(BF), ds[ALL])
            grad_k = nn(d_scores, qs[ALL])
            folded = nn(jnp.transpose(k_rows), d_scores)
            grad_q = jnp.transpose(jnp.where(low_rows, folded[:, :SPAN], folded[:, SPAN:TILE]))[:PAD]
            for third, value in enumerate((grad_q, grad_k, grad_v)):
                rounded = value.astype(BF)
                grads[third, rows, cols] = rounded
                by_core[rows, p * TRIPLE + third * LANES:p * TRIPLE + third * LANES + LANES] = rounded
                out.append(sum_rows(value))
        return tuple(t + n for t, n in zip(sums, out))

    zero = jnp.zeros((ONE, LANES), F32)
    bias_sums = loop(SEQS, seq, (zero,) * 6, unroll=3)
    for p in SIDES:
        for third in range(THIRDS):
            at = pl.multiple_of(third * WIDTH + g * GROUP + p * LANES, LANES)
            biases[:, pl.ds(at, LANES)] = bias_sums[THREE * p + third]
    poll(((2, 3), (1, 1), (0, 0)))
    stage = g + 1

    ring.reopen_box()

    w = nn(turned[ALL], by_core[ALL])
    for part in range(THIRDS):
        both = [w[:, at:at + LANES].reshape(CUBE + BLOCK) for at in (part * LANES, TRIPLE + part * LANES)]
        ring.outbox[part] = jnp.where(rep == 0, both[1], both[0])
        ring.acc[stage % ATT_SLOTS, part] = jnp.where(rep == 0, both[0], both[1])
    ring.pair(THIRDS).start()

    def chunk(i, carry):
        at = pl.ds(pl.multiple_of(i * CHUNK, PACK), CHUNK)
        dh[at, :] += nt(grads[0, at, :], wq_ref[ALL]) + nt(grads[1, at, :], wk_ref[ALL]) + nt(grads[2, at, :], wv_ref[ALL])
        return carry

    loop(ROWS // CHUNK, chunk, 0)

    def exchange(dim, landing, at, number):
        copies = []
        for hops in range(ONE, 4):
            index = list(at)
            index[dim] = (place[dim] + hops) % RING
            copies.append(pltpu.make_async_remote_copy(
                src_ref=blocks.at[tuple(index)], dst_ref=landing.at[hops - 1], send_sem=small_send.at[number + hops],
                recv_sem=small_recv.at[number + hops], device_id=(rep, flat_of(along(place, dim, hops))),
                device_id_type=MESH_ID))
        return copies

    def start(copies):
        for copy in copies:
            copy.start()
        return copies

    def collect(copies, dim, landing, at):
        for copy in copies:
            copy.wait()
        index = list(at)
        index[dim] = place[dim]
        index = tuple(index)
        blocks[index] = blocks[index] + landing[0] + landing[1] + landing[2]

    @pl.when(g == GROUPS - 1)
    def _():
        def tail(*todo):
            for stage, at in todo:
                level(stage, orders, at)

        def fetch(s):
            rows, box = pl.ds(pl.multiple_of(s * PAD, PACK), PAD), s % PAIR
            return (pltpu.make_async_copy(gr_ref.at[rows], gr.at[box], seq_sem.at[0, box]),
                    pltpu.make_async_copy(x_ref.at[s], xs.at[box], seq_sem.at[1, box]))

        def dx_out(s):
            return pltpu.make_async_copy(dxs.at[s % PAIR], dx_ref.at[s], seq_sem.at[2, s % PAIR])

        for copy in fetch(0):
            copy.start()
        gain = vec_ref[:1, :]
        tail((2, 2), (3, 1), (4, 0))
        sums[ALL] = gvin_ref[ALL]
        def norm_one(s, carry):
            @pl.when(s + 1 < SEQS)
            def _():
                for copy in fetch(s + 1):
                    copy.start()

            for copy in fetch(s):
                copy.wait()
            padded(xp, 0, xs, s % PAIR)
            here = pl.ds(pl.multiple_of(s * PAD, PACK), PAD)
            centered, rstd = row_stats(xp[ALL])
            xhat = centered * rstd
            d = dh[here, :]
            dxp[ALL] = (gr[s % PAIR] + norm_back(d * gain, xhat, rstd)).astype(BF)
            for k, value in enumerate((d * xhat, d)):
                sums[k:k + 1, :] += sum_rows(value)

            @pl.when(s >= 2)
            def _():
                dx_out(s - 2).wait()

            dxs[s % PAIR] = dxp[:TOKENS]
            dx_out(s).start()

            @pl.when(s == 3)
            def _():
                tail((2, 3), (3, 2))

            return carry

        loop(SEQS, norm_one, 0)
        for s in (SEQS - 2, SEQS - 1):
            dx_out(s).wait()
        small_blocks(blocks, sums, biases, gbup_ref)
        at = [EVERY] * THREE
        number = 0
        def shard_order():
            for j in range(SUBS):
                turned[:, j * LANES:j * LANES + LANES] = unit_columns(j)
                for b in range(4):
                    for h in SIDES:
                        xp[b * PACK + h * SUBS:b * PACK + h * SUBS + SUBS, j * LANES:j * LANES + LANES] = gup_ref[h, j * RING + b]
            left = xp[:SHARDS]
            total = jnp.zeros_like(left)
            for _ in AXES:
                piece = left.astype(BF)
                total = total + nt(piece, turned[:, :WIDTH])
                left = left - piece.astype(F32)
            for b in range(4):
                up_ref[:, b * WIDTH:b * WIDTH + WIDTH] = total[b * 16:b * PACK + PACK]

        for dim, landing, todo in ((2, from_x, ((4, 1),)), (1, from_y, ((3, 3),)), (0, from_z, ((4, 2),))):
            copies = start(exchange(dim, landing, at, number))
            if dim == 1:
                shard_order()
            tail(*todo)
            collect(copies, dim, landing, at)
            at[dim] = place[dim]
            number += 3
        last = pltpu.make_async_remote_copy(
            src_ref=blocks.at[place], dst_ref=from_pair, send_sem=small_send.at[FIRST], recv_sem=small_recv.at[FIRST],
            device_id=ring.partner, device_id_type=MESH_ID)
        last.start()
        tail((4, 3))
        last.wait()
        small_ref[ALL] = blocks[place] + from_pair[ALL]
        ring.settle(0, ATT_PARTS)
        for stage in range(ONE, ATT_STAGES):
            ring.settle(stage, THIRDS)


def attn_bwd(qkv, do, h, w_qkv, o, da, x, gr, vec, gvin, gbup, gup):
    one = lambda shape: pl.BlockSpec(shape, lambda g: (0,) * len(shape), pipeline_mode=ONCE)
    third = lambda t: pl.BlockSpec((ROWS, GROUP), lambda g: (0, g // PAIR * 6 + t * PAIR + g % PAIR))
    wthird = lambda t: pl.BlockSpec((WIDTH, GROUP), lambda g: (0, t * GROUPS + g))
    col = pl.BlockSpec((ROWS, GROUP), lambda g: (0, g))
    anywhere = ANYWHERE
    shape = jax.ShapeDtypeStruct
    rows = (SUBS, LANES)
    vmem, dma = VM, pltpu.SemaphoreType.DMA
    return pl.pallas_call(
        attn_bwd_kernel, grid=(GROUPS,),
        out_shape=[shape((2, THREE * SUBS) + rows, F32), shape((2, SUBS) + rows, F32), shape((SEQS, TOKENS, WIDTH), BF), shape(rows, F32), shape((PACK, HIDDEN), F32)],
        in_specs=[third(0), third(1), third(2), col, one((ROWS, WIDTH)), wthird(0), wthird(1), wthird(2),
                  one((ROWS, WIDTH)), one((ROWS, WIDTH)), anywhere, anywhere,
                  one((SUBS, WIDTH)), one((SUBS, WIDTH)), one((SUBS, TILE)), one(gup.shape)],
        out_specs=[anywhere, anywhere, anywhere, one(rows), one((PACK, HIDDEN))],
        scratch_shapes=[vmem((ROWS, WIDTH), F32), vmem((THIRDS, ROWS, GROUP), BF), vmem((ROWS, THREE * GROUP), BF),
                        vmem((WIDTH, ROWS), BF), vmem((2, TILE, LANES), BF), vmem((2, TILE, LANES), BF),
                        vmem((PAD, WIDTH), F32), vmem((2, PAD, WIDTH), F32), vmem((2, TOKENS, WIDTH), BF), vmem((2, TOKENS, WIDTH), BF), dma((3, 2)),
                        vmem((PAD, WIDTH), BF), vmem((SUBS, WIDTH), F32), vmem((1, THREE * WIDTH), F32),
                        vmem(CUBE + rows, F32), vmem((3, 4, 4) + rows, F32), vmem((3, 4) + rows, F32),
                        vmem((3,) + rows, F32), vmem(rows, F32), dma((10,)), dma((10,))]
        + ring_scratch(ATT_SLOTS, ATT_STAGES, ATT_PARTS),
        compiler_params=pltpu.CompilerParams(vmem_limit_bytes=VMEM_CAP, collective_id=2, has_side_effects=True),
        name="attn_bwd",
    )(qkv, qkv, qkv, do, h, w_qkv, w_qkv, w_qkv, o, da, x, gr, vec, gvin, gbup, gup)


def layer(x, dz, w_qkv, b_qkv, w_out, w_up, b_up, w_down, vec_params):
    h1, qkv, o, a, h2, dm, vec, b_up, w_qkv, w_out, w_up, w_down = first(
        x, dz, (w_qkv, w_out, w_up, w_down), (b_qkv[None], b_up[None], vec_params))
    w_qkv, w_out, w_up = (w.reshape(WIDTH, -1) for w in (w_qkv, w_out, w_up))
    gw_up, gw_down, gb_up, z, gr, da, do, gvec = mlp(h2, dm, w_up, b_up, w_down, x, dz, a, w_out, vec)
    gw_qkv, gw_out, dx, small, gw_up = attn_bwd(qkv, do, h1, w_qkv, o, da, x, gr, vec, gvec, gb_up, gw_up)
    plain = lambda g: g.swapaxes(1, 2).reshape(g.shape[0] * SUBS, -1)
    return (z, dx, plain(gw_qkv), small[0, 16:SHARDS], plain(gw_out), gw_up, small[:, 64:72].reshape(SHARDS),
            plain(gw_down), small[:, :PACK])


def solution(mesh):
    batch = P(("rep", "fsdp"), None, None)
    rows, flat = P("fsdp", None), P("fsdp")
    params = (rows, flat, rows, rows, flat, rows, P(None, "fsdp"))
    return jax.shard_map(layer, mesh=mesh, in_specs=(batch, batch) + params, out_specs=(batch, batch) + params, check_vma=False)
```

```python
import jax
import jax.numpy as jnp
from jax import lax
from jax.experimental import pallas as pl
from jax.experimental.pallas import tpu as pltpu
from jax.sharding import PartitionSpec as P

LN_EPS = 1e-5

ALL = ...
FIRST, ONE, PAIR, THREE = range(4)
PACK, SHARDS, FLAT, LANES, SPAN, TRIPLE, TILE = 16, 64, 192, 128, 256, 384, 512
SUBS, RING = 8, 4
CUBE, BLOCK = (RING,) * 3, (2, SUBS, LANES)
AXES, SIDES = range(3), range(2)
ONCE = pl.Buffered(ONE)
ANYWHERE = pl.BlockSpec(memory_space=pl.ANY)
VM = pltpu.VMEM
KEEP = True
UNIT, NIL = 1.0, 0.0
TILE_SHAPE = BLOCK[ONE:]


def row(ref, k):
    return ref[k:k + ONE, :]


def other(rep):
    return ONE - rep


def iota(dims, axis):
    return lax.broadcasted_iota(jnp.int32, dims, axis)


def loop(count, body, start, **options):
    return lax.fori_loop(FIRST, count, body, start, **options)


def sum_rows(t):
    return jnp.sum(t, axis=FIRST, keepdims=KEEP)


def max_rows(t):
    return jnp.max(t, axis=FIRST, keepdims=KEEP)


def sum_lanes(t):
    return jnp.sum(t, axis=-ONE, keepdims=KEEP)


def max_lanes(t):
    return jnp.max(t, axis=-ONE, keepdims=KEEP)


def mean_lanes(t):
    return jnp.mean(t, axis=-ONE, keepdims=KEEP)


SEQS, TOKENS, PAD, WIDTH, HIDDEN = 6, 197, 208, 1024, 4096
ROWS = SEQS * PAD
BF, F32 = jnp.bfloat16, jnp.float32
VMEM_CAP = 67043328


def nn(a, b):
    return lax.dot_general(a, b, (((1,), (0,)), ((), ())), preferred_element_type=F32)


def nt(a, b):
    return lax.dot_general(a, b, (((1,), (1,)), ((), ())), preferred_element_type=F32)


def tn(a, b):
    return lax.dot_general(a, b, (((0,), (0,)), ((), ())), preferred_element_type=F32)


def row_stats(t):
    mean = mean_lanes(t)
    centered = t - mean
    variance = mean_lanes(centered * centered)
    return centered, lax.rsqrt(variance + LN_EPS)


def norm_back(dt, xhat, rstd):
    return rstd * (dt - mean_lanes(dt) - xhat * mean_lanes(dt * xhat))


def head_halves(width=LANES):
    lane = iota((1, width), 1)
    return lane < SHARDS


def stack_heads(dst, rows, low):
    zero = jnp.zeros_like(rows)
    dst[:PAD] = jnp.where(low, rows, zero)
    dst[SPAN:SPAN + PAD] = jnp.where(low, zero, rows)


def padded(dst, base, rows_ref, s):
    dst[base + FLAT:base + PAD] = jnp.zeros((PACK, WIDTH), dst.dtype)
    dst[base:base + TOKENS] = rows_ref[s].astype(dst.dtype)


MESH_ID = pl.DeviceIdType.MESH
ORDERS = ((2, 1, 0), (1, 0, 2), (0, 2, 1))
HOPS = (1, 2, 3)
GREETED = 10
FAR, NEAR, DIRECT = "far", "near", "direct"
EVERY = slice(None)


def my_place():
    rep, flat = lax.axis_index("rep"), lax.axis_index("fsdp")
    return rep, (flat // PACK, (flat // RING) % RING, flat % RING)


def along(place, dim, shift):
    moved = list(place)
    moved[dim] = (place[dim] + shift) % RING
    return tuple(moved)


def flat_of(place):
    return place[0] * PACK + place[1] * RING + place[2]


def greet(sem, rep, place):
    pl.semaphore_signal(sem, inc=1, device_id=(other(rep), flat_of(place)), device_id_type=MESH_ID)
    for dim in AXES:
        for shift in HOPS:
            pl.semaphore_signal(sem, inc=1, device_id=(rep, flat_of(along(place, dim, shift))), device_id_type=MESH_ID)


def entry_barrier(rep, place):
    barrier = pltpu.get_barrier_semaphore()
    greet(barrier, rep, place)
    pl.semaphore_wait(barrier, GREETED)


def ring_scratch(slots, stages, parts):
    dma = pltpu.SemaphoreType.DMA
    block = BLOCK
    cube, square, line = CUBE, CUBE[1:], CUBE[2:]
    sides = (parts, 3)
    buffers = [(slots, parts) + cube + block, (parts,) + cube + block, (parts,) + cube + block,
               (stages, parts) + square + block,
               (slots,) + sides + square + block, (stages,) + sides + line + block, (stages,) + sides + block]
    sems = [()] * PAIR + [(slots, 2)] * PAIR + [(stages, 2)] * PAIR + [(stages,)] * THREE
    regular = pltpu.SemaphoreType.REGULAR
    return [VM(b, F32) for b in buffers] + [dma(s) for s in sems] + [regular((slots,)), regular]


class Ring:
    def __init__(self, refs, slots, steps, window):
        (self.acc, self.inbox, self.outbox, self.rest, land0, land1, land2, self.pair_send, self.pair_recv,
         self.send, self.recv, self.rest_send, self.rest_recv, self.out_sem, self.out_send, self.out_recv,
         self.free, self.emptied) = refs
        self.landing = (land0, land1, land2)
        self.slots, self.steps, self.last = slots, steps, len(steps)
        self.window = window
        self.rep, self.place = my_place()
        self.partner = (other(self.rep), flat_of(self.place))

    def across(self, ref, send, recv, into=None):
        return pltpu.make_async_remote_copy(
            src_ref=ref, dst_ref=ref if into is None else into, send_sem=send, recv_sem=recv, device_id=self.partner,
            device_id_type=MESH_ID)

    def pair(self, parts):
        some = pl.ds(FIRST, parts)
        return self.across(self.outbox.at[some], self.pair_send, self.pair_recv, self.inbox.at[some])

    def sems(self, stage, step):
        phase, kind = step
        if phase:
            at = (stage, phase - 1)
            return self.rest_send.at[at], self.rest_recv.at[at]
        at = (stage % self.slots, 1 if kind == NEAR else 0)
        return self.send.at[at], self.recv.at[at]

    def landed(self, stage, parts, step):
        phase, kind = step
        at = self.home(stage, 0, phase)[1][:1] + (pl.ds(FIRST, parts),)
        sides = {FAR: 2, NEAR: pl.ds(FIRST, 2), DIRECT: EVERY}[kind]
        return self.across(self.landing[phase].at[at + (sides,)], *self.sems(stage, step))

    def axis(self, order, phase, index):
        at = {dim: EVERY for dim in order}
        for dim in order[:phase]:
            at[dim] = self.place[dim]
        at[order[phase]] = index
        if phase:
            del at[order[0]]
        return tuple(at[dim] for dim in sorted(at))

    def home(self, stage, part, phase):
        if phase:
            return self.rest, (stage, part)
        return self.acc, (stage % self.slots, part)

    def hops(self, stage, part, order, step):
        phase, kind = step
        dim = order[phase]
        memory, at = self.home(stage, part, phase)
        send, recv = self.sems(stage, step)
        found = []
        for side, shift in enumerate((1, 3) if kind != DIRECT else HOPS):
            source, target, place = shift, 0, at + (side,)
            if kind == FAR:
                source, target = 2, shift
            src = at + self.axis(order, phase, (self.place[dim] + source) % RING)
            into = at + self.axis(order, phase, (self.place[dim] + target) % RING)
            if kind == FAR:
                src, into, place = src + (side,), into + (side,), at + (2,) + (EVERY, EVERY, side)
            copy = pltpu.make_async_remote_copy(
                src_ref=memory.at[src], dst_ref=self.landing[phase].at[place], send_sem=send, recv_sem=recv,
                device_id=(self.rep, flat_of(along(self.place, dim, shift))), device_id_type=MESH_ID)
            found.append((copy, into, place))
        return found

    def results(self, stage, orders):
        for part, order in orders.items():
            src = self.rest.at[(stage, part) + tuple(self.place[dim] for dim in sorted(order[1:]))]
            dst = self.window(stage, part)
            pltpu.make_async_copy(src, dst, self.out_sem.at[stage]).start()
            self.across(src, self.out_send.at[stage], self.out_recv.at[stage], dst).start()

    def level(self, stage, level, orders, credit, refill):
        if level == 0:
            self.pair(len(orders)).wait()
            for part in orders:
                at = (stage % self.slots, part)
                for z in range(4):
                    self.acc[at + (z,)] = self.acc[at + (z,)] + self.inbox[part, z]

            @pl.when(stage >= self.slots)
            def _():
                pl.semaphore_wait(self.free.at[stage % self.slots], GREETED)

            @pl.when(refill)
            def _():
                pl.semaphore_signal(self.emptied, inc=1, device_id=self.partner, device_id_type=MESH_ID)
        else:
            step = self.steps[level - 1]
            phase, kind = step
            self.landed(stage, len(orders), step).wait_recv()
            for part, order in orders.items():
                memory = self.home(stage, part, phase)[0]
                hops = self.hops(stage, part, order, step)
                if kind == FAR:
                    for _, into, place in hops:
                        memory[into] = memory[into] + self.landing[phase][place]
                    continue
                into = hops[0][1]
                total = memory[into]
                for _, _, place in hops:
                    total = total + self.landing[phase][place]
                if phase:
                    memory[into] = total
                else:
                    self.rest[stage, part] = total
            if phase == 0 and kind != FAR:
                self.sent(stage, orders, (0,))

                @pl.when(credit)
                def _():
                    greet(self.free.at[stage % self.slots], self.rep, self.place)
        if level < self.last:
            for part, order in orders.items():
                for copy, _, _ in self.hops(stage, part, order, self.steps[level]):
                    copy.start()
        else:
            self.results(stage, orders)
            self.sent(stage, orders, (1, 2))

    def sent(self, stage, orders, phases):
        for step in self.steps:
            if step[0] in phases:
                self.landed(stage, len(orders), step).wait_send()

    def settle(self, stage, parts):
        ref = self.rest.at[stage, pl.ds(FIRST, parts), 0, 0]
        pltpu.make_async_copy(ref, ref, self.out_sem.at[stage]).wait()
        self.across(ref, self.out_send.at[stage], self.out_recv.at[stage]).wait()

    def reopen_box(self):
        pl.semaphore_wait(self.emptied, 1)


THIRDS = 3
PIECE = TILE
QKV, OUT, UP, DOWN, SMALL = range(5)


def gather_items():
    items = [(half, QKV, 0, third * WIDTH + half * PIECE, PIECE // PAIR, PIECE // PAIR, ORDERS[third])
             for half in SIDES for third in range(THIRDS)]
    rest = [(OUT, 0, 0, PIECE)]
    rest += [(UP, 0, PIECE * j, HIDDEN // PAIR) for j in range(4)]
    rest += [(DOWN, PACK * j, 0, PIECE) for j in range(4)]
    items += [(2 + k // THREE,) + piece + (PIECE, ORDERS[k % THREE]) for k, piece in enumerate(rest)]
    return items + [(0, SMALL, 0, 0, 0, 0, ORDERS[0])]


def small_rows(table, vec, b_qkv, b_up):
    lane = iota((SUBS, LANES), ONE)

    def moved(f, half, shift):
        return pltpu.roll(table[f // PACK, f // RING % RING, f % RING, half], shift % LANES, ONE)

    def fill(ref, tile, owners, half, width, first):
        total = jnp.zeros((SUBS, LANES), F32)
        for f in owners:
            start = width * f - LANES * tile
            here = jnp.logical_and(lane >= start, lane < start + width)
            total = jnp.where(here, moved(f, half, start - first), total)
        ref[:, tile * LANES:tile * LANES + LANES] = total[:ref.shape[0]]

    for tile in range(WIDTH // LANES):
        fill(vec, tile, range(SUBS * tile, SUBS * tile + SUBS), 0, PACK, 0)
    for tile in range(TILE // LANES):
        fill(b_up, tile, range(PACK * tile, PACK * tile + PACK), 1, SUBS, 0)
    for tile in range(THREE * WIDTH // LANES):
        fill(b_qkv, tile, range(LANES * tile // 48, (LANES * tile + LANES - 1) // 48 + 1), 0, 48, PACK)


def placed(values, first, period=LANES):
    size = values.shape[ONE]
    lane = iota((size, LANES), ONE)
    row = iota((size, LANES), FIRST)
    return nn(values.astype(BF), jnp.where(lane == row % period + first, UNIT, NIL).astype(BF))


def unit_columns(j):
    column = iota((WIDTH, LANES), ONE)
    row = iota((WIDTH, LANES), FIRST)
    taken = row == SHARDS * (column // SUBS) + SUBS * j + column % SUBS
    return jnp.where(taken, UNIT, NIL).astype(BF)


def first_kernel(x_ref, dz_ref, sq_ref, so_ref, su_ref, sd_ref, bq_ref, bu_ref, sv_ref,
                 h1_hbm, qkv_ref, o_hbm, a_ref, h2_ref, dm_ref, vec_ref, bup_ref, wq_hbm, wo_hbm, wu_hbm, wd_hbm,
                 wq, wo, su, sd, packed, table, bias, xhat, kst, vst, xp,
                 own_sem, send_sem, recv_sem, pair_send, pair_recv, save_sem, h1_ref, o_ref, o_sem):
    t = pl.program_id(0)
    rep, place = my_place()
    partner = (other(rep), flat_of(place))
    items = gather_items()
    fulls = (wq, wo, wu_hbm, wd_hbm, table)

    def block(item, shards, half=None):
        _, array, row, first, step, cols, _ = items[item]
        if array == SMALL:
            return table.at[shards + ((half,) if half is not None else ())]
        col = rep * step + first
        if half is not None:
            cols = cols // PAIR
            col = col + half * cols
        return fulls[array].at[shards + (pl.ds(row, PACK), pl.ds(pl.multiple_of(col, LANES), cols))]

    def shard(item):
        _, array, row, first, step, _, _ = items[item]
        return (su, sd)[array - UP].at[pl.ds(row, PACK), pl.ds(pl.multiple_of(rep * step + first, LANES), PIECE)]

    def own(item):
        return pltpu.make_async_copy(shard(item), block(item, place), own_sem.at[item])

    def pair(item):
        everywhere = block(item, (EVERY,) * THREE)
        return pltpu.make_async_remote_copy(
            src_ref=everywhere, dst_ref=everywhere, send_sem=pair_send.at[item], recv_sem=pair_recv.at[item],
            device_id=partner, device_id_type=MESH_ID)

    def hops(item, level):
        array, order = items[item][ONE], items[item][-1]
        phase, second = level // PAIR, level % PAIR
        dim = order[phase]
        found = []
        for side, shift in enumerate((1, 3)):
            at = [EVERY] * THREE
            for later in order[phase:]:
                at[later] = place[later]
            if second:
                at[dim] = (place[dim] + 4 - shift) % RING
            dst = block(item, tuple(at), side if second else None)
            src = shard(item) if level == 0 and array in (UP, DOWN) else dst
            found.append(pltpu.make_async_remote_copy(
                src_ref=src, dst_ref=dst, send_sem=send_sem.at[item, level], recv_sem=recv_sem.at[item, level],
                device_id=(rep, flat_of(along(place, dim, shift))), device_id_type=MESH_ID))
        return found

    def both(item, level):
        order = items[item][-1]
        phase, second = level // PAIR, level % PAIR
        at = [EVERY] * THREE
        for later in order[phase:]:
            at[later] = place[later]
        if not second:
            at[order[phase]] = pl.ds(FIRST, 2)
        ref = block(item, tuple(at))
        return pltpu.make_async_remote_copy(
            src_ref=ref, dst_ref=ref, send_sem=send_sem.at[item, level], recv_sem=recv_sem.at[item, level],
            device_id=partner, device_id_type=MESH_ID)

    def advance(*todo):
        for stage, level in todo:
            for item in range(len(items)):
                if items[item][FIRST] != stage:
                    continue
                if level:
                    both(item, level - 1).wait_recv()
                if level == 2 and items[item][ONE] in (UP, DOWN):
                    own(item).wait()
                if level == 6:
                    if items[item][ONE] != SMALL:
                        pair(item).start()
                else:
                    for copy in hops(item, level):
                        copy.start()

    def arrived(*stages):
        for item in range(len(items)):
            if items[item][FIRST] in stages and items[item][ONE] != SMALL:
                pair(item).wait_recv()

    def saves():
        return (pltpu.make_async_copy(wq, wq_hbm, save_sem.at[FIRST]), pltpu.make_async_copy(wo, wo_hbm, save_sem.at[1]),
                pltpu.make_async_copy(h1_ref, h1_hbm, save_sem.at[2]))

    def heads_out(number):
        rows = pl.ds(number * (PAIR * PAD), PAIR * PAD)
        return pltpu.make_async_copy(o_ref.at[rows], o_hbm.at[rows], o_sem.at[number])

    @pl.when(t == FIRST)
    def _():
        for _, array, _, first, step, width, _ in items:
            if array in (QKV, OUT):
                cols = pl.ds(pl.multiple_of(rep * step + first, LANES), width)
                (wq, wo)[array][place + (EVERY, cols)] = (sq_ref, so_ref)[array][:, cols].astype(BF)
        for b in range(4):
            packed[b * 16:b * PACK + PACK] = su_ref[:, b * WIDTH:b * WIDTH + WIDTH].astype(BF)
        sd[ALL] = sd_ref[ALL].astype(BF)
        first_row = iota((SUBS, 48), 0) == 0
        table[place + (0,)] = placed(sv_ref[ALL], 0) + placed(jnp.where(first_row, bq_ref[ALL], NIL), PACK)
        unit = iota((SUBS, SHARDS), ONE) // SUBS == iota((SUBS, SHARDS), FIRST)
        table[place + (1,)] = placed(jnp.where(unit, bu_ref[ALL], NIL), 0, SUBS)
        entry_barrier(rep, place)
        advance((0, 0), (1, 0))
        for j in range(SUBS):
            turned = nn(packed[ALL], unit_columns(j)).astype(BF)
            for b in range(4):
                su[:, j * TILE + b * LANES:j * TILE + b * LANES + LANES] = turned[b * 16:b * PACK + PACK]
        for item in range(len(items)):
            if items[item][ONE] in (UP, DOWN):
                own(item).start()
        later = (2, 3, 4)
        advance(*((stage, 0) for stage in later))
        everything = (0, 1) + later
        for s, todo in enumerate((
                [(stage, 1) for stage in everything], [(stage, 2) for stage in everything], [(0, 3), (1, 3)],
                [(0, 4), (1, 4)] + [(stage, 3) for stage in later], [(0, 5), (2, 4)], [(0, 6), (1, 5)])):
            base = s * PAD
            xp[FLAT:PAD] = jnp.zeros((PACK, WIDTH), BF)
            xp[:TOKENS] = x_ref[s]
            centered, rstd = row_stats(xp[ALL].astype(F32))
            xhat[base:base + PAD] = centered * rstd
            advance(*todo)
        small_rows(table, vec_ref, bias, bup_ref)
        real = iota((PAD, 1), 0) < TOKENS

        def scaled(s, carry):
            here = pl.ds(pl.multiple_of(s * PAD, PACK), PAD)
            h1_ref[here, :] = jnp.where(real, xhat[here, :] * vec_ref[:1, :] + row(vec_ref, 1), NIL).astype(BF)
            return carry

        loop(SEQS, scaled, 0)
        kst[ALL] = jnp.zeros_like(kst)
        vst[ALL] = jnp.zeros_like(vst)

    half, seqs = jnp.maximum(t - ONE, FIRST) // THREE, jnp.maximum(t - ONE, FIRST) % THREE
    base = pl.multiple_of(seqs * (PAIR * PAD), PACK)

    @pl.when(t == 1)
    def _():
        arrived(0)
        saves()[2].start()

    @pl.when(t == 4)
    def _():
        arrived(1)
        saves()[0].start()

    @pl.when(t > FIRST)
    def _():
        for third in range(THIRDS):
            cols = pl.ds(pl.multiple_of(third * WIDTH + half * PIECE, PIECE), PIECE)
            weights = wq[:, :, :, :, cols].reshape(WIDTH, PIECE)
            qkv = nn(h1_ref[pl.ds(base, PAIR * PAD), :], weights) + bias[:, cols]
            qkv_ref[:, third * PIECE:third * PIECE + PIECE] = qkv.astype(BF)

    @pl.when(t == 1)
    def _():
        advance((3, 4))

    low = head_halves()
    visible = iota((1, SPAN), 1) < TOKENS

    half_cols = half * PIECE

    def head_pair(p, carry):
        def cols(third):
            return pl.ds(pl.multiple_of(third * PIECE + p * LANES, LANES), LANES)

        for s in SIDES:
            rows = pl.ds(s * PAD, PAD)
            stack_heads(kst.at[s], qkv_ref[rows, cols(1)], low)
            stack_heads(vst.at[s], qkv_ref[rows, cols(2)], low)
        for s in SIDES:
            rows = pl.ds(s * PAD, PAD)
            scores = nt(qkv_ref[rows, cols(0)], kst[s])
            probs = []
            for head in SIDES:
                part = jnp.where(visible, scores[:, head * SPAN:head * SPAN + SPAN], -jnp.inf)
                top = max_lanes(part)
                e = jnp.exp((part - top) * 0.125)
                probs.append((e * (1.0 / sum_lanes(e))).astype(BF))
            here = pl.ds(pl.multiple_of(base + s * PAD, PACK), PAD)
            heads = pl.ds(pl.multiple_of(half_cols + p * LANES, LANES), LANES)
            o_ref[here, heads] = nn(jnp.concatenate(probs, axis=1), vst[s]).astype(BF)
        return carry

    def two_pairs(i, carry):
        head_pair(PAIR * i, carry)
        head_pair(PAIR * i + 1, carry)
        for step, turn, todo in ((1, 0, (1, 6)), (1, 1, (2, 5)), (2, 0, (4, 4)), (2, 1, (3, 5)), (3, 0, (2, 6)),
                                 (4, 1, (4, 5)), (5, 0, (3, 6)), (5, 1, (4, 6))):
            @pl.when(jnp.logical_and(t == step, i == turn))
            def _(todo=todo):
                advance(todo)

        return carry

    @pl.when(t > FIRST)
    def _():
        loop(2, two_pairs, 0)

    for number in AXES:
        @pl.when(t == 4 + number)
        def _(number=number):
            heads_out(number).start()

    @pl.when(t == 4)
    def _():
        arrived(2)
        saves()[1].start()

    @pl.when(t > 3)
    def _():
        for s in SIDES:
            padded(xp, 0, x_ref, PAIR * seqs + s)
            xhat[s * PAD:s * PAD + PAD] = xp[ALL].astype(F32)
            dm_ref[s * PAD + FLAT:s * PAD + PAD] = jnp.zeros((PACK, WIDTH), BF)
            dm_ref[s * PAD:s * PAD + TOKENS] = (dz_ref[s].astype(F32) * row(vec_ref, 7)).astype(BF)
        a_ref[ALL] = nn(o_ref[pl.ds(base, PAIR * PAD), :], wo[ALL].reshape(WIDTH, WIDTH)) + row(vec_ref, 2)

        def rows(i, carry):
            at = pl.ds(pl.multiple_of(i * 32, 32), 32)
            y = xhat[at, :] + row(vec_ref, 3) * a_ref[at, :]
            centered, rstd = row_stats(y)
            h2_ref[at, :] = (centered * rstd * row(vec_ref, 4) + row(vec_ref, 5)).astype(BF)
            return carry

        loop(PAIR * PAD // 32, rows, 0, unroll=13)

    @pl.when(t == 6)
    def _():
        arrived(3, 4)
        for item in range(len(items)):
            if items[item][ONE] != SMALL:
                pair(item).wait_send()
            for level in range(6):
                both(item, level).wait_send()
        for copy in saves():
            copy.wait()
        for number in AXES:
            heads_out(number).wait()


def first(x, dz, shards, small):
    whole = lambda dims: pl.BlockSpec(dims, lambda t: (0,) * len(dims), pipeline_mode=ONCE)
    pair = lambda t: jnp.maximum(t - RING, FIRST)
    past = lambda t: jnp.maximum(t - ONE, FIRST)
    rows = pl.BlockSpec((PAIR * PAD, WIDTH), lambda t: (pair(t), 0))
    halves = pl.BlockSpec((PAIR * PAD, THREE * PIECE), lambda t: (past(t) % THREE, past(t) // THREE))
    anywhere = ANYWHERE
    shape, vmem, dma = jax.ShapeDtypeStruct, VM, pltpu.SemaphoreType.DMA
    n = len(gather_items())
    cube = CUBE
    return pl.pallas_call(
        first_kernel, grid=(7,),
        out_shape=[shape((ROWS, WIDTH), BF), shape((ROWS, THREE * WIDTH), BF), shape((ROWS, WIDTH), BF), shape((ROWS, WIDTH), F32),
                   shape((ROWS, WIDTH), BF), shape((ROWS, WIDTH), BF), shape((SUBS, WIDTH), F32), shape((SUBS, TILE), F32)]
        + [shape(cube + s.shape, BF) for s in shards],
        in_specs=[whole((SEQS, TOKENS, WIDTH)), pl.BlockSpec((2, TOKENS, WIDTH), lambda t: (pair(t), 0, 0))]
        + [whole(s.shape) for s in shards + small],
        out_specs=[anywhere, halves, anywhere, rows, rows, rows,
                   whole((SUBS, WIDTH)), whole((SUBS, TILE))] + [anywhere] * RING,
        scratch_shapes=[vmem(cube + shards[QKV].shape, BF), vmem(cube + shards[OUT].shape, BF), vmem(shards[UP].shape, BF),
                        vmem(shards[DOWN].shape, BF), vmem((SHARDS, WIDTH), BF), vmem(cube + (2, SUBS, LANES), F32), vmem((1, THREE * WIDTH), F32),
                        vmem((ROWS, WIDTH), F32), vmem((2, PIECE, LANES), BF), vmem((2, PIECE, LANES), BF),
                        vmem((PAD, WIDTH), BF),
                        dma((n,)), dma((n, 6)), dma((n, 6)), dma((n,)), dma((n,)), dma((3,)), vmem((ROWS, WIDTH), BF), vmem((ROWS, WIDTH), BF), dma((3,))],
        compiler_params=pltpu.CompilerParams(vmem_limit_bytes=VMEM_CAP, collective_id=FIRST, has_side_effects=True),
        name="first",
    )(x, dz, *shards, *small)


CHUNK = 624
TILES = HIDDEN // TILE
MLP_SLOTS, MLP_PARTS = 3, 4
MLP_STEPS = ((0, FAR), (0, NEAR), (1, DIRECT), (2, DIRECT))


def gelu_and_slope(u):
    cdf = 0.5 * (1.0 + lax.erf(u * (2.0 ** -0.5)))
    pdf = jnp.exp(u * u * -0.5) * ((2.0 * jnp.pi) ** -0.5)
    return u * cdf, cdf + u * pdf


def mlp_kernel(h_ref, dm_ref, w1_ref, w2_ref, b1_ref, x_ref, dz_ref, a_ref, wo_ref, vec_ref,
               gw1_ref, gw2_ref, gb_ref, z_ref, gr_ref, da_ref, do_ref, gv_ref,
               m_acc, dh_acc, act, dpre, turned, xp, zp, zo, *ring_refs):
    j = pl.program_id(0)

    def window(stage, part):
        if part < 2:
            return gw2_ref.at[stage, pl.ds(rep * RING + part * PAIR, 2)]
        return gw1_ref.at[:, stage * RING + rep * PAIR + part - 2]

    ring = Ring(ring_refs, MLP_SLOTS, MLP_STEPS, window)
    rep = ring.rep
    every_part = range(MLP_PARTS)

    def run(lag, level):
        stage = j - lag
        for turn in AXES:
            orders = {part: ORDERS[(turn + part) % THREE] for part in every_part}

            @pl.when(jnp.logical_and(jnp.logical_and(stage >= 0, stage < TILES), stage % THREE == turn))
            def _(orders=orders):
                ring.level(stage, level, orders, stage < TILES - MLP_SLOTS, stage < TILES - 1)

    @pl.when(j == FIRST)
    def _():
        entry_barrier(rep, ring.place)
        m_acc[ALL] = jnp.zeros_like(m_acc)
        dh_acc[ALL] = jnp.zeros_like(dh_acc)
        turned[ALL] = jnp.transpose(h_ref[ALL])

    def chunk(i, total):
        at = pl.ds(pl.multiple_of(i * CHUNK, PACK), CHUNK)
        w1, w2 = w1_ref[ALL], w2_ref[ALL].reshape(TILE, WIDTH)
        u = nn(h_ref[at, :], w1) + b1_ref[pl.ds(j, 1), :]
        value, slope = gelu_and_slope(u)
        act[at, :] = value.astype(BF)
        d = nt(dm_ref[at, :], w2) * slope
        dpre[at, :] = d.astype(BF)
        return sum_rows(d) + total

    def onward(i, carry):
        at = pl.ds(pl.multiple_of(i * CHUNK, PACK), CHUNK)
        m_acc[at, :] += nn(act[at, :], w2_ref[ALL].reshape(TILE, WIDTH))
        dh_acc[at, :] += nt(dpre[at, :], w1_ref[ALL])
        return carry

    def grads(core, target):
        cols = pl.ds(pl.multiple_of(core * TILE, TILE), TILE)
        g = tn(act[ALL], dm_ref[:, cols])
        for part in SIDES:
            for half in SIDES:
                first = (part * PAIR + half) * LANES
                target(part, half, g[:, first:first + LANES].reshape(CUBE + TILE_SHAPE))

    def grads_up(core, target):
        g = nn(turned[ALL], dpre[:, pl.ds(pl.multiple_of(core * SPAN, SPAN), SPAN)])
        for part in SIDES:
            target(part + 2, EVERY, g[:, part * LANES:part * LANES + LANES].reshape(CUBE + BLOCK))

    for lag in range(ring.last + 1, 0, -1):
        run(lag, lag - 1)

    @pl.when(j < TILES)
    def _():
        gb_ref[pl.ds(j, 1), :] = loop(ROWS // CHUNK, chunk, jnp.zeros((1, TILE), F32))

    @pl.when(j == TILES)
    def _():
        gv_ref[ALL] = jnp.zeros_like(gv_ref)

    @pl.when(j >= TILES)
    def _():
        padded(xp, 0, x_ref, 0)
        padded(zp, 0, dz_ref, 0)
        s1, g2, b2, s2 = (vec_ref[k:k + 1, :] for k in (3, 4, 6, 7))
        here = pl.ds(pl.multiple_of((j - TILES) * PAD, PACK), PAD)
        a = a_ref[ALL]
        y = xp[ALL].astype(F32) + s1 * a
        mlp_out = m_acc[here, :] + b2
        g_out = zp[ALL].astype(F32)
        zo[ALL] = (y + s2 * mlp_out).astype(BF)
        centered, rstd = row_stats(y)
        xhat = centered * rstd
        dh = dh_acc[here, :]
        g_resid = g_out + norm_back(dh * g2, xhat, rstd)
        d_att = g_resid * s1
        gr_ref[ALL] = g_resid
        da_ref[ALL] = d_att.astype(BF)
        for k, total in enumerate((d_att, g_resid * a, dh * xhat, dh, g_out * s2, g_out * mlp_out)):
            gv_ref[2 + k:3 + k, :] += sum_rows(total)
        z_ref[0] = zo[:TOKENS]
        do_ref[ALL] = nt(da_ref[ALL], wo_ref[ALL]).astype(BF)

    @pl.when(j < TILES)
    def _():
        slot = j % MLP_SLOTS

        def out(part, half, value):
            ring.outbox[part, :, :, :, half] = value

        def own(part, half, value):
            ring.acc[slot, part, :, :, :, half] = value

        grads(other(rep), out)
        grads_up(other(rep), out)

        @pl.when(j >= 1)
        def _():
            ring.reopen_box()

        ring.pair(MLP_PARTS).start()
        grads(rep, own)
        grads_up(rep, own)
        loop(ROWS // CHUNK, onward, 0)

    @pl.when(j == TILES + SEQS - 1)
    def _():
        for stage in range(TILES):
            ring.settle(stage, MLP_PARTS)


def mlp(h, dm, w1, b1, w2, x, dz, a, w_out, vec):
    whole = lambda shape: pl.BlockSpec(shape, lambda j: (0, 0), pipeline_mode=ONCE)
    tile = lambda j: jnp.minimum(j, TILES - 1)
    seq = lambda j: jnp.maximum(j - TILES, FIRST)
    b1_spec = whole((SUBS, TILE))
    seqs = pl.BlockSpec((1, TOKENS, WIDTH), lambda j: (seq(j), 0, 0))
    rows = pl.BlockSpec((PAD, WIDTH), lambda j: (seq(j), 0))
    anywhere = ANYWHERE
    shape = jax.ShapeDtypeStruct
    return pl.pallas_call(
        mlp_kernel, grid=(TILES + SEQS,),
        out_shape=[shape((2, HIDDEN // LANES, SUBS, LANES), F32), shape((SUBS, SUBS, SUBS, LANES), F32), shape((SUBS, TILE), F32),
                   shape((SEQS, TOKENS, WIDTH), BF), shape((ROWS, WIDTH), F32), shape((ROWS, WIDTH), BF),
                   shape((ROWS, WIDTH), BF), shape((8, WIDTH), F32)],
        in_specs=[whole((ROWS, WIDTH)), whole((ROWS, WIDTH)), pl.BlockSpec((WIDTH, TILE), lambda j: (0, tile(j))),
                  pl.BlockSpec((SHARDS, SUBS, WIDTH), lambda j: (0, tile(j), 0)), b1_spec, seqs, seqs, rows,
                  whole((WIDTH, WIDTH)), whole((8, WIDTH))],
        out_specs=[anywhere, anywhere, whole((SUBS, TILE)), seqs, rows, rows, rows, whole((8, WIDTH))],
        scratch_shapes=[VM((ROWS, WIDTH), F32), VM((ROWS, WIDTH), F32), VM((ROWS, TILE), BF),
                        VM((ROWS, TILE), BF), VM((WIDTH, ROWS), BF), VM((PAD, WIDTH), BF),
                        VM((PAD, WIDTH), BF), VM((PAD, WIDTH), BF)] + ring_scratch(MLP_SLOTS, TILES, MLP_PARTS),
        compiler_params=pltpu.CompilerParams(vmem_limit_bytes=VMEM_CAP, collective_id=1, has_side_effects=True),
        name="mlp",
    )(h, dm, w1, w2.reshape(SHARDS, SHARDS, WIDTH), b1, x, dz, a, w_out, vec)


GROUP = SPAN
GROUPS = WIDTH // GROUP
ATT_SLOTS, ATT_STAGES, ATT_PARTS = 2, GROUPS + 1, 4
ATT_STEPS = tuple((phase, DIRECT) for phase in AXES)


def small_blocks(target, vec, b_qkv, b_up):
    lane = iota((SUBS, LANES), ONE)

    def turned(ref, tile, first, to):
        return pltpu.roll(ref[:, tile * LANES:tile * LANES + LANES], (to - first) % LANES, ONE)

    for f in range(SHARDS):
        tile, first = divmod(48 * f, LANES)
        bias = turned(b_qkv, tile, first, PACK)
        if first + 48 > LANES:
            bias = jnp.where(lane[:1] < PACK + LANES - first, bias, turned(b_qkv, tile + 1, first, PACK))
        rows = turned(vec, f // SUBS, PACK * (f % SUBS), 0)
        up = turned(b_up, f // PACK, SUBS * (f % PACK), SHARDS)
        target[f // PACK, f // RING % RING, f % RING] = jnp.where(lane < PACK, rows, jnp.where(lane < SHARDS, bias, up))


def attn_bwd_kernel(q_ref, k_ref, v_ref, do_ref, h_ref, wq_ref, wk_ref, wv_ref, o_ref, da_ref, x_ref, gr_ref, vec_ref,
                    gvin_ref, gbup_ref, gup_ref, gw_ref, gwo_ref, dx_ref, small_ref, up_ref,
                    dh, grads, by_core, turned, qst, dst, xp, gr, xs, dxs, seq_sem, dxp, sums, biases, blocks, from_x, from_y, from_z, from_pair,
                    small_send, small_recv, *ring_refs):
    g = pl.program_id(0)

    def window(stage, part):
        if isinstance(stage, int) and stage == 0:
            return gwo_ref.at[:, rep * RING + part]
        return gw_ref.at[:, part * SUBS + (stage - 1) * PAIR + rep]

    ring = Ring(ring_refs, ATT_SLOTS, ATT_STEPS, window)
    rep, place = ring.rep, ring.place
    first_orders = {part: ORDERS[part % THREE] for part in range(ATT_PARTS)}
    orders = {part: ORDERS[part] for part in range(THIRDS)}

    def level(stage, which, at):
        ring.level(stage, at, which, stage < ATT_STAGES - ATT_SLOTS, stage < ATT_STAGES - 1)

    def poll(todo):
        for lag, at in todo:
            @pl.when(g - lag >= 1)
            def _(lag=lag, at=at):
                level(g - lag, orders, at)

            @pl.when(g == lag)
            def _(at=at):
                level(0, first_orders, at)

    @pl.when(g == FIRST)
    def _():
        entry_barrier(rep, place)
        dh[ALL] = jnp.zeros_like(dh)
        qst[ALL] = jnp.zeros_like(qst)
        dst[ALL] = jnp.zeros_like(dst)
        turned[ALL] = jnp.transpose(h_ref[ALL])
        for core, box in ((other(rep), ring.outbox), (rep, ring.acc.at[FIRST])):
            w = tn(o_ref[ALL], da_ref[:, pl.ds(pl.multiple_of(core * TILE, TILE), TILE)])
            for part in range(ATT_PARTS):
                box[part] = w[:, part * LANES:part * LANES + LANES].reshape(CUBE + BLOCK)
            if box is ring.outbox:
                ring.pair(ATT_PARTS).start()

    poll(((2, 2),))
    low = head_halves()
    low_rows = iota((LANES, ONE), 0) < SHARDS
    hidden = iota((PAD, 1), 0) >= TOKENS

    def seq(s, sums):
        rows = pl.ds(pl.multiple_of(s * PAD, PACK), PAD)
        out = []
        for p in SIDES:
            cols = slice(p * LANES, p * LANES + LANES)
            qs, ds = qst.at[p], dst.at[p]
            k_rows, v_rows = k_ref[rows, cols], v_ref[rows, cols]
            stack_heads(qs, q_ref[rows, cols], low)
            stack_heads(ds, do_ref[rows, cols], low)
            scores = jnp.where(hidden, -jnp.inf, nt(k_rows, qs[ALL]))
            top = max_rows(scores)
            e = jnp.exp((scores - top) * 0.125)
            probs = e * (1.0 / sum_rows(e))
            d_probs = nt(v_rows, ds[ALL])
            inner = sum_rows(d_probs * probs)
            d_scores = (probs * (d_probs - inner) * 0.125).astype(BF)
            grad_v = nn(probs.astype(BF), ds[ALL])
            grad_k = nn(d_scores, qs[ALL])
            folded = nn(jnp.transpose(k_rows), d_scores)
            grad_q = jnp.transpose(jnp.where(low_rows, folded[:, :SPAN], folded[:, SPAN:TILE]))[:PAD]
            for third, value in enumerate((grad_q, grad_k, grad_v)):
                rounded = value.astype(BF)
                grads[third, rows, cols] = rounded
                by_core[rows, p * TRIPLE + third * LANES:p * TRIPLE + third * LANES + LANES] = rounded
                out.append(sum_rows(value))
        return tuple(t + n for t, n in zip(sums, out))

    zero = jnp.zeros((ONE, LANES), F32)
    bias_sums = loop(SEQS, seq, (zero,) * 6, unroll=3)
    for p in SIDES:
        for third in range(THIRDS):
            at = pl.multiple_of(third * WIDTH + g * GROUP + p * LANES, LANES)
            biases[:, pl.ds(at, LANES)] = bias_sums[THREE * p + third]
    poll(((2, 3), (1, 1), (0, 0)))
    stage = g + 1

    ring.reopen_box()

    w = nn(turned[ALL], by_core[ALL])
    for part in range(THIRDS):
        both = [w[:, at:at + LANES].reshape(CUBE + BLOCK) for at in (part * LANES, TRIPLE + part * LANES)]
        ring.outbox[part] = jnp.where(rep == 0, both[1], both[0])
        ring.acc[stage % ATT_SLOTS, part] = jnp.where(rep == 0, both[0], both[1])
    ring.pair(THIRDS).start()

    def chunk(i, carry):
        at = pl.ds(pl.multiple_of(i * CHUNK, PACK), CHUNK)
        dh[at, :] += nt(grads[0, at, :], wq_ref[ALL]) + nt(grads[1, at, :], wk_ref[ALL]) + nt(grads[2, at, :], wv_ref[ALL])
        return carry

    loop(ROWS // CHUNK, chunk, 0)

    def exchange(dim, landing, at, number):
        copies = []
        for hops in range(ONE, 4):
            index = list(at)
            index[dim] = (place[dim] + hops) % RING
            copies.append(pltpu.make_async_remote_copy(
                src_ref=blocks.at[tuple(index)], dst_ref=landing.at[hops - 1], send_sem=small_send.at[number + hops],
                recv_sem=small_recv.at[number + hops], device_id=(rep, flat_of(along(place, dim, hops))),
                device_id_type=MESH_ID))
        return copies

    def start(copies):
        for copy in copies:
            copy.start()
        return copies

    def collect(copies, dim, landing, at):
        for copy in copies:
            copy.wait()
        index = list(at)
        index[dim] = place[dim]
        index = tuple(index)
        blocks[index] = blocks[index] + landing[0] + landing[1] + landing[2]

    @pl.when(g == GROUPS - 1)
    def _():
        def tail(*todo):
            for stage, at in todo:
                level(stage, orders, at)

        def fetch(s):
            rows, box = pl.ds(pl.multiple_of(s * PAD, PACK), PAD), s % PAIR
            return (pltpu.make_async_copy(gr_ref.at[rows], gr.at[box], seq_sem.at[0, box]),
                    pltpu.make_async_copy(x_ref.at[s], xs.at[box], seq_sem.at[1, box]))

        def dx_out(s):
            return pltpu.make_async_copy(dxs.at[s % PAIR], dx_ref.at[s], seq_sem.at[2, s % PAIR])

        for copy in fetch(0):
            copy.start()
        gain = vec_ref[:1, :]
        tail((2, 2), (3, 1), (4, 0))
        sums[ALL] = gvin_ref[ALL]
        def norm_one(s, carry):
            @pl.when(s + 1 < SEQS)
            def _():
                for copy in fetch(s + 1):
                    copy.start()

            for copy in fetch(s):
                copy.wait()
            padded(xp, 0, xs, s % PAIR)
            here = pl.ds(pl.multiple_of(s * PAD, PACK), PAD)
            centered, rstd = row_stats(xp[ALL])
            xhat = centered * rstd
            d = dh[here, :]
            dxp[ALL] = (gr[s % PAIR] + norm_back(d * gain, xhat, rstd)).astype(BF)
            for k, value in enumerate((d * xhat, d)):
                sums[k:k + 1, :] += sum_rows(value)

            @pl.when(s >= 2)
            def _():
                dx_out(s - 2).wait()

            dxs[s % PAIR] = dxp[:TOKENS]
            dx_out(s).start()

            @pl.when(s == 3)
            def _():
                tail((2, 3), (3, 2))

            return carry

        loop(SEQS, norm_one, 0)
        for s in (SEQS - 2, SEQS - 1):
            dx_out(s).wait()
        small_blocks(blocks, sums, biases, gbup_ref)
        at = [EVERY] * THREE
        number = 0
        def shard_order():
            for j in range(SUBS):
                turned[:, j * LANES:j * LANES + LANES] = unit_columns(j)
                for b in range(4):
                    for h in SIDES:
                        xp[b * PACK + h * SUBS:b * PACK + h * SUBS + SUBS, j * LANES:j * LANES + LANES] = gup_ref[h, j * RING + b]
            left = xp[:SHARDS]
            total = jnp.zeros_like(left)
            for _ in AXES:
                piece = left.astype(BF)
                total = total + nt(piece, turned[:, :WIDTH])
                left = left - piece.astype(F32)
            for b in range(4):
                up_ref[:, b * WIDTH:b * WIDTH + WIDTH] = total[b * 16:b * PACK + PACK]

        for dim, landing, todo in ((2, from_x, ((4, 1),)), (1, from_y, ((3, 3),)), (0, from_z, ((4, 2),))):
            copies = start(exchange(dim, landing, at, number))
            if dim == 1:
                shard_order()
            tail(*todo)
            collect(copies, dim, landing, at)
            at[dim] = place[dim]
            number += 3
        last = pltpu.make_async_remote_copy(
            src_ref=blocks.at[place], dst_ref=from_pair, send_sem=small_send.at[FIRST], recv_sem=small_recv.at[FIRST],
            device_id=ring.partner, device_id_type=MESH_ID)
        last.start()
        tail((4, 3))
        last.wait()
        small_ref[ALL] = blocks[place] + from_pair[ALL]
        ring.settle(0, ATT_PARTS)
        for stage in range(ONE, ATT_STAGES):
            ring.settle(stage, THIRDS)


def attn_bwd(qkv, do, h, w_qkv, o, da, x, gr, vec, gvin, gbup, gup):
    one = lambda shape: pl.BlockSpec(shape, lambda g: (0,) * len(shape), pipeline_mode=ONCE)
    third = lambda t: pl.BlockSpec((ROWS, GROUP), lambda g: (0, g // PAIR * 6 + t * PAIR + g % PAIR))
    wthird = lambda t: pl.BlockSpec((WIDTH, GROUP), lambda g: (0, t * GROUPS + g))
    col = pl.BlockSpec((ROWS, GROUP), lambda g: (0, g))
    anywhere = ANYWHERE
    shape = jax.ShapeDtypeStruct
    rows = (SUBS, LANES)
    vmem, dma = VM, pltpu.SemaphoreType.DMA
    return pl.pallas_call(
        attn_bwd_kernel, grid=(GROUPS,),
        out_shape=[shape((2, THREE * SUBS) + rows, F32), shape((2, SUBS) + rows, F32), shape((SEQS, TOKENS, WIDTH), BF), shape(rows, F32), shape((PACK, HIDDEN), F32)],
        in_specs=[third(0), third(1), third(2), col, one((ROWS, WIDTH)), wthird(0), wthird(1), wthird(2),
                  one((ROWS, WIDTH)), one((ROWS, WIDTH)), anywhere, anywhere,
                  one((SUBS, WIDTH)), one((SUBS, WIDTH)), one((SUBS, TILE)), one(gup.shape)],
        out_specs=[anywhere, anywhere, anywhere, one(rows), one((PACK, HIDDEN))],
        scratch_shapes=[vmem((ROWS, WIDTH), F32), vmem((THIRDS, ROWS, GROUP), BF), vmem((ROWS, THREE * GROUP), BF),
                        vmem((WIDTH, ROWS), BF), vmem((2, TILE, LANES), BF), vmem((2, TILE, LANES), BF),
                        vmem((PAD, WIDTH), F32), vmem((2, PAD, WIDTH), F32), vmem((2, TOKENS, WIDTH), BF), vmem((2, TOKENS, WIDTH), BF), dma((3, 2)),
                        vmem((PAD, WIDTH), BF), vmem((SUBS, WIDTH), F32), vmem((1, THREE * WIDTH), F32),
                        vmem(CUBE + rows, F32), vmem((3, 4, 4) + rows, F32), vmem((3, 4) + rows, F32),
                        vmem((3,) + rows, F32), vmem(rows, F32), dma((10,)), dma((10,))]
        + ring_scratch(ATT_SLOTS, ATT_STAGES, ATT_PARTS),
        compiler_params=pltpu.CompilerParams(vmem_limit_bytes=VMEM_CAP, collective_id=2, has_side_effects=True),
        name="attn_bwd",
    )(qkv, qkv, qkv, do, h, w_qkv, w_qkv, w_qkv, o, da, x, gr, vec, gvin, gbup, gup)


def last_kernel(z_ref, dx_ref, gq_ref, go_ref, gu_ref, gd_ref, small_ref,
                z_out, dx_out, gq_out, bq_out, go_out, gu_out, bu_out, gd_out, vec_out):
    def untiled(src, dst):
        for r in range(src.shape[0]):
            for c in range(src.shape[ONE]):
                dst[r * SUBS:r * SUBS + SUBS, c * LANES:c * LANES + LANES] = src[r, c]

    z_out[ALL] = z_ref[ALL]
    dx_out[ALL] = dx_ref[ALL]
    untiled(gq_ref, gq_out)

    @pl.when(pl.program_id(0) == 0)
    def _():
        untiled(go_ref, go_out)
        untiled(gd_ref, gd_out)
        gu_out[ALL] = gu_ref[ALL]
        vec_out[ALL] = small_ref[:, :PACK]
        bq_out[ALL] = pltpu.roll(small_ref[ALL], LANES - PACK, 1)[:1, 0:48]
        lane = iota((SUBS, LANES), ONE)
        units = jnp.zeros((ONE, LANES), F32)
        for j in range(SUBS):
            moved = pltpu.roll(small_ref[ALL], (SUBS * j + LANES - SHARDS) % LANES, ONE)
            units = jnp.where(lane[:1] // SUBS == j, moved[j:j + 1], units)
        bu_out[ALL] = units[:, :SHARDS]


def last(z, dx, gw_qkv, gw_out, gw_up, gw_down, small):
    whole = lambda dims: pl.BlockSpec(dims, lambda s: (0,) * len(dims), pipeline_mode=ONCE)
    seq = pl.BlockSpec((1, TOKENS, WIDTH), lambda s: (s, 0, 0))
    share = THREE * SUBS // SEQS
    shape = lambda *dims: jax.ShapeDtypeStruct(dims, F32)
    outs = [shape(PACK, THREE * WIDTH), shape(1, 48), shape(PACK, WIDTH), shape(PACK, HIDDEN), shape(1, SHARDS), shape(SHARDS, WIDTH), shape(SUBS, PACK)]
    return pl.pallas_call(
        last_kernel, grid=(SEQS,),
        out_shape=[jax.ShapeDtypeStruct(z.shape, BF), jax.ShapeDtypeStruct(dx.shape, BF)] + outs,
        in_specs=[seq, seq, pl.BlockSpec((2, share, SUBS, LANES), lambda s: (0, s, 0, 0))]
        + [whole(g.shape) for g in (gw_out, gw_up, gw_down, small)],
        out_specs=[seq, seq, pl.BlockSpec((PACK, share * LANES), lambda s: (0, s))] + [whole(o.shape) for o in outs[1:]],
        name="last",
    )(z, dx, gw_qkv, gw_out, gw_up, gw_down, small)


def layer(x, dz, w_qkv, b_qkv, w_out, w_up, b_up, w_down, vec_params):
    h1, qkv, o, a, h2, dm, vec, b_up, w_qkv, w_out, w_up, w_down = first(
        x, dz, (w_qkv, w_out, w_up, w_down), (b_qkv[None], b_up[None], vec_params))
    w_qkv, w_out, w_up = (w.reshape(WIDTH, -1) for w in (w_qkv, w_out, w_up))
    gw_up, gw_down, gb_up, z, gr, da, do, gvec = mlp(h2, dm, w_up, b_up, w_down, x, dz, a, w_out, vec)
    gw_qkv, gw_out, dx, small, gw_up = attn_bwd(qkv, do, h1, w_qkv, o, da, x, gr, vec, gvec, gb_up, gw_up)
    z, dx, gw_qkv, gb_qkv, gw_out, gw_up, gb_up, gw_down, gvec = last(z, dx, gw_qkv, gw_out, gw_up, gw_down, small)
    return z, dx, gw_qkv, gb_qkv[0], gw_out, gw_up, gb_up[0], gw_down, gvec


def solution(mesh):
    batch = P(("rep", "fsdp"), None, None)
    rows, flat = P("fsdp", None), P("fsdp")
    params = (rows, flat, rows, rows, flat, rows, P(None, "fsdp"))
    return jax.shard_map(layer, mesh=mesh, in_specs=(batch, batch) + params, out_specs=(batch, batch) + params, check_vma=False)
```

```python
import jax
import jax.numpy as jnp
from jax import lax
from jax.experimental import pallas as pl
from jax.experimental.pallas import tpu as pltpu
from jax.sharding import PartitionSpec as P

LN_EPS = 1e-5

ALL = ...
FIRST, ONE, PAIR, THREE = range(4)
PACK, SHARDS, FLAT, LANES, SPAN, TRIPLE, TILE = 16, 64, 192, 128, 256, 384, 512
SUBS, RING = 8, 4
CUBE, BLOCK = (RING,) * 3, (2, SUBS, LANES)
AXES, SIDES = range(3), range(2)
ONCE = pl.Buffered(ONE)
ANYWHERE = pl.BlockSpec(memory_space=pl.ANY)
VM = pltpu.VMEM
KEEP = True
UNIT, NIL = 1.0, 0.0
TILE_SHAPE = BLOCK[ONE:]


def row(ref, k):
    return ref[k:k + ONE, :]


def other(rep):
    return ONE - rep


def iota(dims, axis):
    return lax.broadcasted_iota(jnp.int32, dims, axis)


def loop(count, body, start, **options):
    return lax.fori_loop(FIRST, count, body, start, **options)


def sum_rows(t):
    return jnp.sum(t, axis=FIRST, keepdims=KEEP)


def max_rows(t):
    return jnp.max(t, axis=FIRST, keepdims=KEEP)


def sum_lanes(t):
    return jnp.sum(t, axis=-ONE, keepdims=KEEP)


def max_lanes(t):
    return jnp.max(t, axis=-ONE, keepdims=KEEP)


def mean_lanes(t):
    return jnp.mean(t, axis=-ONE, keepdims=KEEP)


SEQS, TOKENS, PAD, WIDTH, HIDDEN = 6, 197, 208, 1024, 4096
ROWS = SEQS * PAD
BF, F32 = jnp.bfloat16, jnp.float32
VMEM_CAP = 67043328


def nn(a, b):
    return lax.dot_general(a, b, (((1,), (0,)), ((), ())), preferred_element_type=F32)


def nt(a, b):
    return lax.dot_general(a, b, (((1,), (1,)), ((), ())), preferred_element_type=F32)


def tn(a, b):
    return lax.dot_general(a, b, (((0,), (0,)), ((), ())), preferred_element_type=F32)


def row_stats(t):
    mean = mean_lanes(t)
    centered = t - mean
    variance = mean_lanes(centered * centered)
    return centered, lax.rsqrt(variance + LN_EPS)


def norm_back(dt, xhat, rstd):
    return rstd * (dt - mean_lanes(dt) - xhat * mean_lanes(dt * xhat))


def head_halves(width=LANES):
    lane = iota((1, width), 1)
    return lane < SHARDS


def stack_heads(dst, rows, low):
    zero = jnp.zeros_like(rows)
    dst[:PAD] = jnp.where(low, rows, zero)
    dst[SPAN:SPAN + PAD] = jnp.where(low, zero, rows)


def padded(dst, base, rows_ref, s):
    dst[base + FLAT:base + PAD] = jnp.zeros((PACK, WIDTH), dst.dtype)
    dst[base:base + TOKENS] = rows_ref[s].astype(dst.dtype)


MESH_ID = pl.DeviceIdType.MESH
ORDERS = ((2, 1, 0), (1, 0, 2), (0, 2, 1))
HOPS = (1, 2, 3)
GREETED = 10
FAR, NEAR, DIRECT = "far", "near", "direct"
EVERY = slice(None)


def my_place():
    rep, flat = lax.axis_index("rep"), lax.axis_index("fsdp")
    return rep, (flat // PACK, (flat // RING) % RING, flat % RING)


def along(place, dim, shift):
    moved = list(place)
    moved[dim] = (place[dim] + shift) % RING
    return tuple(moved)


def flat_of(place):
    return place[0] * PACK + place[1] * RING + place[2]


def greet(sem, rep, place):
    pl.semaphore_signal(sem, inc=1, device_id=(other(rep), flat_of(place)), device_id_type=MESH_ID)
    for dim in AXES:
        for shift in HOPS:
            pl.semaphore_signal(sem, inc=1, device_id=(rep, flat_of(along(place, dim, shift))), device_id_type=MESH_ID)


def entry_barrier(rep, place):
    barrier = pltpu.get_barrier_semaphore()
    greet(barrier, rep, place)
    pl.semaphore_wait(barrier, GREETED)


def ring_scratch(slots, stages, parts):
    dma = pltpu.SemaphoreType.DMA
    block = BLOCK
    cube, square, line = CUBE, CUBE[1:], CUBE[2:]
    sides = (parts, 3)
    buffers = [(slots, parts) + cube + block, (parts,) + cube + block, (parts,) + cube + block,
               (stages, parts) + square + block,
               (slots,) + sides + square + block, (stages,) + sides + line + block, (stages,) + sides + block]
    sems = [()] * PAIR + [(slots, 2)] * PAIR + [(stages, 2)] * PAIR + [(stages,)] * THREE
    regular = pltpu.SemaphoreType.REGULAR
    return [VM(b, F32) for b in buffers] + [dma(s) for s in sems] + [regular((slots,)), regular]


class Ring:
    def __init__(self, refs, slots, steps, window):
        (self.acc, self.inbox, self.outbox, self.rest, land0, land1, land2, self.pair_send, self.pair_recv,
         self.send, self.recv, self.rest_send, self.rest_recv, self.out_sem, self.out_send, self.out_recv,
         self.free, self.emptied) = refs
        self.landing = (land0, land1, land2)
        self.slots, self.steps, self.last = slots, steps, len(steps)
        self.window = window
        self.rep, self.place = my_place()
        self.partner = (other(self.rep), flat_of(self.place))

    def across(self, ref, send, recv, into=None):
        return pltpu.make_async_remote_copy(
            src_ref=ref, dst_ref=ref if into is None else into, send_sem=send, recv_sem=recv, device_id=self.partner,
            device_id_type=MESH_ID)

    def pair(self, parts):
        some = pl.ds(FIRST, parts)
        return self.across(self.outbox.at[some], self.pair_send, self.pair_recv, self.inbox.at[some])

    def sems(self, stage, step):
        phase, kind = step
        if phase:
            at = (stage, phase - 1)
            return self.rest_send.at[at], self.rest_recv.at[at]
        at = (stage % self.slots, 1 if kind == NEAR else 0)
        return self.send.at[at], self.recv.at[at]

    def landed(self, stage, parts, step):
        phase, kind = step
        at = self.home(stage, 0, phase)[1][:1] + (pl.ds(FIRST, parts),)
        sides = {FAR: 2, NEAR: pl.ds(FIRST, 2), DIRECT: EVERY}[kind]
        return self.across(self.landing[phase].at[at + (sides,)], *self.sems(stage, step))

    def axis(self, order, phase, index):
        at = {dim: EVERY for dim in order}
        for dim in order[:phase]:
            at[dim] = self.place[dim]
        at[order[phase]] = index
        if phase:
            del at[order[0]]
        return tuple(at[dim] for dim in sorted(at))

    def home(self, stage, part, phase):
        if phase:
            return self.rest, (stage, part)
        return self.acc, (stage % self.slots, part)

    def hops(self, stage, part, order, step):
        phase, kind = step
        dim = order[phase]
        memory, at = self.home(stage, part, phase)
        send, recv = self.sems(stage, step)
        found = []
        for side, shift in enumerate((1, 3) if kind != DIRECT else HOPS):
            source, target, place = shift, 0, at + (side,)
            if kind == FAR:
                source, target = 2, shift
            src = at + self.axis(order, phase, (self.place[dim] + source) % RING)
            into = at + self.axis(order, phase, (self.place[dim] + target) % RING)
            if kind == FAR:
                src, into, place = src + (side,), into + (side,), at + (2,) + (EVERY, EVERY, side)
            copy = pltpu.make_async_remote_copy(
                src_ref=memory.at[src], dst_ref=self.landing[phase].at[place], send_sem=send, recv_sem=recv,
                device_id=(self.rep, flat_of(along(self.place, dim, shift))), device_id_type=MESH_ID)
            found.append((copy, into, place))
        return found

    def results(self, stage, orders):
        for part, order in orders.items():
            src = self.rest.at[(stage, part) + tuple(self.place[dim] for dim in sorted(order[1:]))]
            dst = self.window(stage, part)
            pltpu.make_async_copy(src, dst, self.out_sem.at[stage]).start()
            self.across(src, self.out_send.at[stage], self.out_recv.at[stage], dst).start()

    def level(self, stage, level, orders, credit, refill):
        if level == 0:
            self.pair(len(orders)).wait()
            for part in orders:
                at = (stage % self.slots, part)
                for z in range(4):
                    self.acc[at + (z,)] = self.acc[at + (z,)] + self.inbox[part, z]

            @pl.when(stage >= self.slots)
            def _():
                pl.semaphore_wait(self.free.at[stage % self.slots], GREETED)

            @pl.when(refill)
            def _():
                pl.semaphore_signal(self.emptied, inc=1, device_id=self.partner, device_id_type=MESH_ID)
        else:
            step = self.steps[level - 1]
            phase, kind = step
            self.landed(stage, len(orders), step).wait_recv()
            for part, order in orders.items():
                memory = self.home(stage, part, phase)[0]
                hops = self.hops(stage, part, order, step)
                if kind == FAR:
                    for _, into, place in hops:
                        memory[into] = memory[into] + self.landing[phase][place]
                    continue
                into = hops[0][1]
                total = memory[into]
                for _, _, place in hops:
                    total = total + self.landing[phase][place]
                if phase:
                    memory[into] = total
                else:
                    self.rest[stage, part] = total
            if phase == 0 and kind != FAR:
                self.sent(stage, orders, (0,))

                @pl.when(credit)
                def _():
                    greet(self.free.at[stage % self.slots], self.rep, self.place)
        if level < self.last:
            for part, order in orders.items():
                for copy, _, _ in self.hops(stage, part, order, self.steps[level]):
                    copy.start()
        else:
            self.results(stage, orders)
            self.sent(stage, orders, (1, 2))

    def sent(self, stage, orders, phases):
        for step in self.steps:
            if step[0] in phases:
                self.landed(stage, len(orders), step).wait_send()

    def settle(self, stage, parts):
        ref = self.rest.at[stage, pl.ds(FIRST, parts), 0, 0]
        pltpu.make_async_copy(ref, ref, self.out_sem.at[stage]).wait()
        self.across(ref, self.out_send.at[stage], self.out_recv.at[stage]).wait()

    def reopen_box(self):
        pl.semaphore_wait(self.emptied, 1)


THIRDS = 3
PIECE = TILE
QKV, OUT, UP, DOWN, SMALL = range(5)


def gather_items():
    items = [(half, QKV, 0, third * WIDTH + half * PIECE, PIECE // PAIR, PIECE // PAIR, ORDERS[third])
             for half in SIDES for third in range(THIRDS)]
    rest = [(OUT, 0, 0, PIECE)]
    rest += [(UP, 0, PIECE * j, HIDDEN // PAIR) for j in range(4)]
    rest += [(DOWN, PACK * j, 0, PIECE) for j in range(4)]
    items += [(2 + k // THREE,) + piece + (PIECE, ORDERS[k % THREE]) for k, piece in enumerate(rest)]
    return items + [(0, SMALL, 0, 0, 0, 0, ORDERS[0])]


def small_rows(table, vec, b_qkv, b_up):
    lane = iota((SUBS, LANES), ONE)

    def moved(f, half, shift):
        return pltpu.roll(table[f // PACK, f // RING % RING, f % RING, half], shift % LANES, ONE)

    def fill(ref, tile, owners, half, width, first):
        total = jnp.zeros((SUBS, LANES), F32)
        for f in owners:
            start = width * f - LANES * tile
            here = jnp.logical_and(lane >= start, lane < start + width)
            total = jnp.where(here, moved(f, half, start - first), total)
        ref[:, tile * LANES:tile * LANES + LANES] = total[:ref.shape[0]]

    for tile in range(WIDTH // LANES):
        fill(vec, tile, range(SUBS * tile, SUBS * tile + SUBS), 0, PACK, 0)
    for tile in range(TILE // LANES):
        fill(b_up, tile, range(PACK * tile, PACK * tile + PACK), 1, SUBS, 0)
    for tile in range(THREE * WIDTH // LANES):
        fill(b_qkv, tile, range(LANES * tile // 48, (LANES * tile + LANES - 1) // 48 + 1), 0, 48, PACK)


def placed(values, first, period=LANES):
    size = values.shape[ONE]
    lane = iota((size, LANES), ONE)
    row = iota((size, LANES), FIRST)
    return nn(values.astype(BF), jnp.where(lane == row % period + first, UNIT, NIL).astype(BF))


def unit_columns(j):
    column = iota((WIDTH, LANES), ONE)
    row = iota((WIDTH, LANES), FIRST)
    taken = row == SHARDS * (column // SUBS) + SUBS * j + column % SUBS
    return jnp.where(taken, UNIT, NIL).astype(BF)


def first_kernel(x_ref, dz_ref, sq_ref, so_ref, su_ref, sd_ref, bq_ref, bu_ref, sv_ref,
                 h1_hbm, qkv_ref, o_hbm, a_ref, h2_ref, dm_ref, vec_ref, bup_ref, wq_hbm, wo_hbm, wu_hbm, wd_hbm,
                 wq, wo, su, sd, packed, table, bias, xhat, kst, vst, xp,
                 own_sem, send_sem, recv_sem, pair_send, pair_recv, save_sem, h1_ref, o_ref, o_sem):
    t = pl.program_id(0)
    rep, place = my_place()
    partner = (other(rep), flat_of(place))
    items = gather_items()
    fulls = (wq, wo, wu_hbm, wd_hbm, table)

    def block(item, shards, half=None):
        _, array, row, first, step, cols, _ = items[item]
        if array == SMALL:
            return table.at[shards + ((half,) if half is not None else ())]
        col = rep * step + first
        if half is not None:
            cols = cols // PAIR
            col = col + half * cols
        return fulls[array].at[shards + (pl.ds(row, PACK), pl.ds(pl.multiple_of(col, LANES), cols))]

    def shard(item):
        _, array, row, first, step, _, _ = items[item]
        return (su, sd)[array - UP].at[pl.ds(row, PACK), pl.ds(pl.multiple_of(rep * step + first, LANES), PIECE)]

    def own(item):
        return pltpu.make_async_copy(shard(item), block(item, place), own_sem.at[item])

    def pair(item):
        everywhere = block(item, (EVERY,) * THREE)
        return pltpu.make_async_remote_copy(
            src_ref=everywhere, dst_ref=everywhere, send_sem=pair_send.at[item], recv_sem=pair_recv.at[item],
            device_id=partner, device_id_type=MESH_ID)

    def hops(item, level):
        array, order = items[item][ONE], items[item][-1]
        phase, second = level // PAIR, level % PAIR
        dim = order[phase]
        found = []
        for side, shift in enumerate((1, 3)):
            at = [EVERY] * THREE
            for later in order[phase:]:
                at[later] = place[later]
            if second:
                at[dim] = (place[dim] + 4 - shift) % RING
            dst = block(item, tuple(at), side if second else None)
            src = shard(item) if level == 0 and array in (UP, DOWN) else dst
            found.append(pltpu.make_async_remote_copy(
                src_ref=src, dst_ref=dst, send_sem=send_sem.at[item, level], recv_sem=recv_sem.at[item, level],
                device_id=(rep, flat_of(along(place, dim, shift))), device_id_type=MESH_ID))
        return found

    def both(item, level):
        order = items[item][-1]
        phase, second = level // PAIR, level % PAIR
        at = [EVERY] * THREE
        for later in order[phase:]:
            at[later] = place[later]
        if not second:
            at[order[phase]] = pl.ds(FIRST, 2)
        ref = block(item, tuple(at))
        return pltpu.make_async_remote_copy(
            src_ref=ref, dst_ref=ref, send_sem=send_sem.at[item, level], recv_sem=recv_sem.at[item, level],
            device_id=partner, device_id_type=MESH_ID)

    def advance(*todo):
        for stage, level in todo:
            for item in range(len(items)):
                if items[item][FIRST] != stage:
                    continue
                if level:
                    both(item, level - 1).wait_recv()
                if level == 2 and items[item][ONE] in (UP, DOWN):
                    own(item).wait()
                if level == 6:
                    if items[item][ONE] != SMALL:
                        pair(item).start()
                else:
                    for copy in hops(item, level):
                        copy.start()

    def arrived(*stages):
        for item in range(len(items)):
            if items[item][FIRST] in stages and items[item][ONE] != SMALL:
                pair(item).wait_recv()

    def saves():
        return (pltpu.make_async_copy(wq, wq_hbm, save_sem.at[FIRST]), pltpu.make_async_copy(wo, wo_hbm, save_sem.at[1]),
                pltpu.make_async_copy(h1_ref, h1_hbm, save_sem.at[2]))

    def heads_out(number):
        rows = pl.ds(number * (PAIR * PAD), PAIR * PAD)
        return pltpu.make_async_copy(o_ref.at[rows], o_hbm.at[rows], o_sem.at[number])

    @pl.when(t == FIRST)
    def _():
        for _, array, _, first, step, width, _ in items:
            if array in (QKV, OUT):
                cols = pl.ds(pl.multiple_of(rep * step + first, LANES), width)
                (wq, wo)[array][place + (EVERY, cols)] = (sq_ref, so_ref)[array][:, cols].astype(BF)
        for b in range(4):
            packed[b * 16:b * PACK + PACK] = su_ref[:, b * WIDTH:b * WIDTH + WIDTH].astype(BF)
        sd[ALL] = sd_ref[ALL].astype(BF)
        first_row = iota((SUBS, 48), 0) == 0
        table[place + (0,)] = placed(sv_ref[ALL], 0) + placed(jnp.where(first_row, bq_ref[ALL], NIL), PACK)
        unit = iota((SUBS, SHARDS), ONE) // SUBS == iota((SUBS, SHARDS), FIRST)
        table[place + (1,)] = placed(jnp.where(unit, bu_ref[ALL], NIL), 0, SUBS)
        entry_barrier(rep, place)
        advance((0, 0), (1, 0))
        for j in range(SUBS):
            turned = nn(packed[ALL], unit_columns(j)).astype(BF)
            for b in range(4):
                su[:, j * TILE + b * LANES:j * TILE + b * LANES + LANES] = turned[b * 16:b * PACK + PACK]
        for item in range(len(items)):
            if items[item][ONE] in (UP, DOWN):
                own(item).start()
        later = (2, 3, 4)
        advance(*((stage, 0) for stage in later))
        everything = (0, 1) + later
        for s, todo in enumerate((
                [(stage, 1) for stage in everything], [(stage, 2) for stage in everything], [(0, 3), (1, 3)],
                [(0, 4), (1, 4)] + [(stage, 3) for stage in later], [(0, 5), (2, 4)], [(0, 6), (1, 5)])):
            base = s * PAD
            xp[FLAT:PAD] = jnp.zeros((PACK, WIDTH), BF)
            xp[:TOKENS] = x_ref[s]
            centered, rstd = row_stats(xp[ALL].astype(F32))
            xhat[base:base + PAD] = centered * rstd
            advance(*todo)
        small_rows(table, vec_ref, bias, bup_ref)
        real = iota((PAD, 1), 0) < TOKENS

        def scaled(s, carry):
            here = pl.ds(pl.multiple_of(s * PAD, PACK), PAD)
            h1_ref[here, :] = jnp.where(real, xhat[here, :] * vec_ref[:1, :] + row(vec_ref, 1), NIL).astype(BF)
            return carry

        loop(SEQS, scaled, 0)
        kst[ALL] = jnp.zeros_like(kst)
        vst[ALL] = jnp.zeros_like(vst)

    half, seqs = jnp.maximum(t - ONE, FIRST) // THREE, jnp.maximum(t - ONE, FIRST) % THREE
    base = pl.multiple_of(seqs * (PAIR * PAD), PACK)

    @pl.when(t == 1)
    def _():
        arrived(0)
        saves()[2].start()

    @pl.when(t == 4)
    def _():
        arrived(1)
        saves()[0].start()

    @pl.when(t > FIRST)
    def _():
        for third in range(THIRDS):
            cols = pl.ds(pl.multiple_of(third * WIDTH + half * PIECE, PIECE), PIECE)
            weights = wq[:, :, :, :, cols].reshape(WIDTH, PIECE)
            qkv = nn(h1_ref[pl.ds(base, PAIR * PAD), :], weights) + bias[:, cols]
            qkv_ref[:, third * PIECE:third * PIECE + PIECE] = qkv.astype(BF)

    @pl.when(t == 1)
    def _():
        advance((3, 4))

    low = head_halves()
    visible = iota((1, SPAN), 1) < TOKENS

    half_cols = half * PIECE

    def head_pair(p, carry):
        def cols(third):
            return pl.ds(pl.multiple_of(third * PIECE + p * LANES, LANES), LANES)

        for s in SIDES:
            rows = pl.ds(s * PAD, PAD)
            stack_heads(kst.at[s], qkv_ref[rows, cols(1)], low)
            stack_heads(vst.at[s], qkv_ref[rows, cols(2)], low)
        for s in SIDES:
            rows = pl.ds(s * PAD, PAD)
            scores = nt(qkv_ref[rows, cols(0)], kst[s])
            probs = []
            for head in SIDES:
                part = jnp.where(visible, scores[:, head * SPAN:head * SPAN + SPAN], -jnp.inf)
                top = max_lanes(part)
                e = jnp.exp((part - top) * 0.125)
                probs.append((e * (1.0 / sum_lanes(e))).astype(BF))
            here = pl.ds(pl.multiple_of(base + s * PAD, PACK), PAD)
            heads = pl.ds(pl.multiple_of(half_cols + p * LANES, LANES), LANES)
            o_ref[here, heads] = nn(jnp.concatenate(probs, axis=1), vst[s]).astype(BF)
        return carry

    def two_pairs(i, carry):
        head_pair(PAIR * i, carry)
        head_pair(PAIR * i + 1, carry)
        for step, turn, todo in ((1, 0, (1, 6)), (1, 1, (2, 5)), (2, 0, (4, 4)), (2, 1, (3, 5)), (3, 0, (2, 6)),
                                 (4, 1, (4, 5)), (5, 0, (3, 6)), (5, 1, (4, 6))):
            @pl.when(jnp.logical_and(t == step, i == turn))
            def _(todo=todo):
                advance(todo)

        return carry

    @pl.when(t > FIRST)
    def _():
        loop(2, two_pairs, 0)

    for number in AXES:
        @pl.when(t == 4 + number)
        def _(number=number):
            heads_out(number).start()

    @pl.when(t == 4)
    def _():
        arrived(2)
        saves()[1].start()

    @pl.when(t > 3)
    def _():
        for s in SIDES:
            padded(xp, 0, x_ref, PAIR * seqs + s)
            xhat[s * PAD:s * PAD + PAD] = xp[ALL].astype(F32)
            dm_ref[s * PAD + FLAT:s * PAD + PAD] = jnp.zeros((PACK, WIDTH), BF)
            dm_ref[s * PAD:s * PAD + TOKENS] = (dz_ref[s].astype(F32) * row(vec_ref, 7)).astype(BF)
        a_ref[ALL] = nn(o_ref[pl.ds(base, PAIR * PAD), :], wo[ALL].reshape(WIDTH, WIDTH)) + row(vec_ref, 2)

        def rows(i, carry):
            at = pl.ds(pl.multiple_of(i * 32, 32), 32)
            y = xhat[at, :] + row(vec_ref, 3) * a_ref[at, :]
            centered, rstd = row_stats(y)
            h2_ref[at, :] = (centered * rstd * row(vec_ref, 4) + row(vec_ref, 5)).astype(BF)
            return carry

        loop(PAIR * PAD // 32, rows, 0, unroll=13)

    @pl.when(t == 6)
    def _():
        arrived(3, 4)
        for item in range(len(items)):
            if items[item][ONE] != SMALL:
                pair(item).wait_send()
            for level in range(6):
                both(item, level).wait_send()
        for copy in saves():
            copy.wait()
        for number in AXES:
            heads_out(number).wait()


def first(x, dz, shards, small):
    whole = lambda dims: pl.BlockSpec(dims, lambda t: (0,) * len(dims), pipeline_mode=ONCE)
    pair = lambda t: jnp.maximum(t - RING, FIRST)
    past = lambda t: jnp.maximum(t - ONE, FIRST)
    rows = pl.BlockSpec((PAIR * PAD, WIDTH), lambda t: (pair(t), 0))
    halves = pl.BlockSpec((PAIR * PAD, THREE * PIECE), lambda t: (past(t) % THREE, past(t) // THREE))
    anywhere = ANYWHERE
    shape, vmem, dma = jax.ShapeDtypeStruct, VM, pltpu.SemaphoreType.DMA
    n = len(gather_items())
    cube = CUBE
    return pl.pallas_call(
        first_kernel, grid=(7,),
        out_shape=[shape((ROWS, WIDTH), BF), shape((ROWS, THREE * WIDTH), BF), shape((ROWS, WIDTH), BF), shape((ROWS, WIDTH), F32),
                   shape((ROWS, WIDTH), BF), shape((ROWS, WIDTH), BF), shape((SUBS, WIDTH), F32), shape((SUBS, TILE), F32)]
        + [shape(cube + s.shape, BF) for s in shards],
        in_specs=[whole((SEQS, TOKENS, WIDTH)), pl.BlockSpec((2, TOKENS, WIDTH), lambda t: (pair(t), 0, 0))]
        + [whole(s.shape) for s in shards + small],
        out_specs=[anywhere, halves, anywhere, rows, rows, rows,
                   whole((SUBS, WIDTH)), whole((SUBS, TILE))] + [anywhere] * RING,
        scratch_shapes=[vmem(cube + shards[QKV].shape, BF), vmem(cube + shards[OUT].shape, BF), vmem(shards[UP].shape, BF),
                        vmem(shards[DOWN].shape, BF), vmem((SHARDS, WIDTH), BF), vmem(cube + (2, SUBS, LANES), F32), vmem((1, THREE * WIDTH), F32),
                        vmem((ROWS, WIDTH), F32), vmem((2, PIECE, LANES), BF), vmem((2, PIECE, LANES), BF),
                        vmem((PAD, WIDTH), BF),
                        dma((n,)), dma((n, 6)), dma((n, 6)), dma((n,)), dma((n,)), dma((3,)), vmem((ROWS, WIDTH), BF), vmem((ROWS, WIDTH), BF), dma((3,))],
        compiler_params=pltpu.CompilerParams(vmem_limit_bytes=VMEM_CAP, collective_id=FIRST, has_side_effects=True),
        name="first",
    )(x, dz, *shards, *small)


CHUNK = 624
TILES = HIDDEN // TILE
MLP_SLOTS, MLP_PARTS = 3, 4
MLP_STEPS = ((0, FAR), (0, NEAR), (1, DIRECT), (2, DIRECT))


def gelu_and_slope(u):
    cdf = 0.5 * (1.0 + lax.erf(u * (2.0 ** -0.5)))
    pdf = jnp.exp(u * u * -0.5) * ((2.0 * jnp.pi) ** -0.5)
    return u * cdf, cdf + u * pdf


def mlp_kernel(h_ref, dm_ref, w1_ref, w2_ref, b1_ref, x_ref, dz_ref, a_ref, wo_ref, vec_ref,
               gw1_ref, gw2_ref, gb_ref, z_ref, gr_ref, da_ref, do_ref, gv_ref,
               m_acc, dh_acc, act, dpre, turned, xp, zp, zo, *ring_refs):
    j = pl.program_id(0)

    def window(stage, part):
        if part < 2:
            return gw2_ref.at[stage, pl.ds(rep * RING + part * PAIR, 2)]
        return gw1_ref.at[:, stage * RING + rep * PAIR + part - 2]

    ring = Ring(ring_refs, MLP_SLOTS, MLP_STEPS, window)
    rep = ring.rep
    every_part = range(MLP_PARTS)

    def run(lag, level):
        stage = j - lag
        for turn in AXES:
            orders = {part: ORDERS[(turn + part) % THREE] for part in every_part}

            @pl.when(jnp.logical_and(jnp.logical_and(stage >= 0, stage < TILES), stage % THREE == turn))
            def _(orders=orders):
                ring.level(stage, level, orders, stage < TILES - MLP_SLOTS, stage < TILES - 1)

    @pl.when(j == FIRST)
    def _():
        entry_barrier(rep, ring.place)
        m_acc[ALL] = jnp.zeros_like(m_acc)
        dh_acc[ALL] = jnp.zeros_like(dh_acc)
        turned[ALL] = jnp.transpose(h_ref[ALL])

    def chunk(i, total):
        at = pl.ds(pl.multiple_of(i * CHUNK, PACK), CHUNK)
        w1, w2 = w1_ref[ALL], w2_ref[ALL].reshape(TILE, WIDTH)
        u = nn(h_ref[at, :], w1) + b1_ref[pl.ds(j, 1), :]
        value, slope = gelu_and_slope(u)
        act[at, :] = value.astype(BF)
        d = nt(dm_ref[at, :], w2) * slope
        dpre[at, :] = d.astype(BF)
        return sum_rows(d) + total

    def onward(i, carry):
        at = pl.ds(pl.multiple_of(i * CHUNK, PACK), CHUNK)
        m_acc[at, :] += nn(act[at, :], w2_ref[ALL].reshape(TILE, WIDTH))
        dh_acc[at, :] += nt(dpre[at, :], w1_ref[ALL])
        return carry

    def grads(core, target):
        cols = pl.ds(pl.multiple_of(core * TILE, TILE), TILE)
        g = tn(act[ALL], dm_ref[:, cols])
        for part in SIDES:
            for half in SIDES:
                first = (part * PAIR + half) * LANES
                target(part, half, g[:, first:first + LANES].reshape(CUBE + TILE_SHAPE))

    def grads_up(core, target):
        g = nn(turned[ALL], dpre[:, pl.ds(pl.multiple_of(core * SPAN, SPAN), SPAN)])
        for part in SIDES:
            target(part + 2, EVERY, g[:, part * LANES:part * LANES + LANES].reshape(CUBE + BLOCK))

    for lag in range(ONE, ring.last + 2):
        run(lag, lag - 1)

    @pl.when(j < TILES)
    def _():
        gb_ref[pl.ds(j, 1), :] = loop(ROWS // CHUNK, chunk, jnp.zeros((1, TILE), F32))

    @pl.when(j == TILES)
    def _():
        gv_ref[ALL] = jnp.zeros_like(gv_ref)

    @pl.when(j >= TILES)
    def _():
        padded(xp, 0, x_ref, 0)
        padded(zp, 0, dz_ref, 0)
        s1, g2, b2, s2 = (vec_ref[k:k + 1, :] for k in (3, 4, 6, 7))
        here = pl.ds(pl.multiple_of((j - TILES) * PAD, PACK), PAD)
        a = a_ref[ALL]
        y = xp[ALL].astype(F32) + s1 * a
        mlp_out = m_acc[here, :] + b2
        g_out = zp[ALL].astype(F32)
        zo[ALL] = (y + s2 * mlp_out).astype(BF)
        centered, rstd = row_stats(y)
        xhat = centered * rstd
        dh = dh_acc[here, :]
        g_resid = g_out + norm_back(dh * g2, xhat, rstd)
        d_att = g_resid * s1
        gr_ref[ALL] = g_resid
        da_ref[ALL] = d_att.astype(BF)
        for k, total in enumerate((d_att, g_resid * a, dh * xhat, dh, g_out * s2, g_out * mlp_out)):
            gv_ref[2 + k:3 + k, :] += sum_rows(total)
        z_ref[0] = zo[:TOKENS]
        do_ref[ALL] = nt(da_ref[ALL], wo_ref[ALL]).astype(BF)

    @pl.when(j < TILES)
    def _():
        slot = j % MLP_SLOTS

        def out(part, half, value):
            ring.outbox[part, :, :, :, half] = value

        def own(part, half, value):
            ring.acc[slot, part, :, :, :, half] = value

        grads(other(rep), out)
        grads_up(other(rep), out)

        @pl.when(j >= 1)
        def _():
            ring.reopen_box()

        ring.pair(MLP_PARTS).start()
        grads(rep, own)
        grads_up(rep, own)
        loop(ROWS // CHUNK, onward, 0)

    @pl.when(j == TILES + SEQS - 1)
    def _():
        for stage in range(TILES):
            ring.settle(stage, MLP_PARTS)


def mlp(h, dm, w1, b1, w2, x, dz, a, w_out, vec):
    whole = lambda shape: pl.BlockSpec(shape, lambda j: (0, 0), pipeline_mode=ONCE)
    tile = lambda j: jnp.minimum(j, TILES - 1)
    seq = lambda j: jnp.maximum(j - TILES, FIRST)
    b1_spec = whole((SUBS, TILE))
    seqs = pl.BlockSpec((1, TOKENS, WIDTH), lambda j: (seq(j), 0, 0))
    rows = pl.BlockSpec((PAD, WIDTH), lambda j: (seq(j), 0))
    anywhere = ANYWHERE
    shape = jax.ShapeDtypeStruct
    return pl.pallas_call(
        mlp_kernel, grid=(TILES + SEQS,),
        out_shape=[shape((2, HIDDEN // LANES, SUBS, LANES), F32), shape((SUBS, SUBS, SUBS, LANES), F32), shape((SUBS, TILE), F32),
                   shape((SEQS, TOKENS, WIDTH), BF), shape((ROWS, WIDTH), F32), shape((ROWS, WIDTH), BF),
                   shape((ROWS, WIDTH), BF), shape((8, WIDTH), F32)],
        in_specs=[whole((ROWS, WIDTH)), whole((ROWS, WIDTH)), pl.BlockSpec((WIDTH, TILE), lambda j: (0, tile(j))),
                  pl.BlockSpec((SHARDS, SUBS, WIDTH), lambda j: (0, tile(j), 0)), b1_spec, seqs, seqs, rows,
                  whole((WIDTH, WIDTH)), whole((8, WIDTH))],
        out_specs=[anywhere, anywhere, whole((SUBS, TILE)), seqs, rows, rows, rows, whole((8, WIDTH))],
        scratch_shapes=[VM((ROWS, WIDTH), F32), VM((ROWS, WIDTH), F32), VM((ROWS, TILE), BF),
                        VM((ROWS, TILE), BF), VM((WIDTH, ROWS), BF), VM((PAD, WIDTH), BF),
                        VM((PAD, WIDTH), BF), VM((PAD, WIDTH), BF)] + ring_scratch(MLP_SLOTS, TILES, MLP_PARTS),
        compiler_params=pltpu.CompilerParams(vmem_limit_bytes=VMEM_CAP, collective_id=1, has_side_effects=True),
        name="mlp",
    )(h, dm, w1, w2.reshape(SHARDS, SHARDS, WIDTH), b1, x, dz, a, w_out, vec)


GROUP = SPAN
GROUPS = WIDTH // GROUP
ATT_SLOTS, ATT_STAGES, ATT_PARTS = 2, GROUPS + 1, 4
ATT_STEPS = tuple((phase, DIRECT) for phase in AXES)


def small_blocks(target, vec, b_qkv, b_up):
    lane = iota((SUBS, LANES), ONE)

    def turned(ref, tile, first, to):
        return pltpu.roll(ref[:, tile * LANES:tile * LANES + LANES], (to - first) % LANES, ONE)

    for f in range(SHARDS):
        tile, first = divmod(48 * f, LANES)
        bias = turned(b_qkv, tile, first, PACK)
        if first + 48 > LANES:
            bias = jnp.where(lane[:1] < PACK + LANES - first, bias, turned(b_qkv, tile + 1, first, PACK))
        rows = turned(vec, f // SUBS, PACK * (f % SUBS), 0)
        up = turned(b_up, f // PACK, SUBS * (f % PACK), SHARDS)
        target[f // PACK, f // RING % RING, f % RING] = jnp.where(lane < PACK, rows, jnp.where(lane < SHARDS, bias, up))


def attn_bwd_kernel(q_ref, k_ref, v_ref, do_ref, h_ref, wq_ref, wk_ref, wv_ref, o_ref, da_ref, x_ref, gr_ref, vec_ref,
                    gvin_ref, gbup_ref, gup_ref, gw_ref, gwo_ref, dx_ref, small_ref, up_ref,
                    dh, grads, by_core, turned, qst, dst, xp, gr, xs, dxs, seq_sem, dxp, sums, biases, blocks, from_x, from_y, from_z, from_pair,
                    small_send, small_recv, *ring_refs):
    g = pl.program_id(0)

    def window(stage, part):
        if isinstance(stage, int) and stage == 0:
            return gwo_ref.at[:, rep * RING + part]
        return gw_ref.at[:, part * SUBS + (stage - 1) * PAIR + rep]

    ring = Ring(ring_refs, ATT_SLOTS, ATT_STEPS, window)
    rep, place = ring.rep, ring.place
    first_orders = {part: ORDERS[part % THREE] for part in range(ATT_PARTS)}
    orders = {part: ORDERS[part] for part in range(THIRDS)}

    def level(stage, which, at):
        ring.level(stage, at, which, stage < ATT_STAGES - ATT_SLOTS, stage < ATT_STAGES - 1)

    def poll(todo):
        for lag, at in todo:
            @pl.when(g - lag >= 1)
            def _(lag=lag, at=at):
                level(g - lag, orders, at)

            @pl.when(g == lag)
            def _(at=at):
                level(0, first_orders, at)

    @pl.when(g == FIRST)
    def _():
        entry_barrier(rep, place)
        dh[ALL] = jnp.zeros_like(dh)
        qst[ALL] = jnp.zeros_like(qst)
        dst[ALL] = jnp.zeros_like(dst)
        turned[ALL] = jnp.transpose(h_ref[ALL])
        for core, box in ((other(rep), ring.outbox), (rep, ring.acc.at[FIRST])):
            w = tn(o_ref[ALL], da_ref[:, pl.ds(pl.multiple_of(core * TILE, TILE), TILE)])
            for part in range(ATT_PARTS):
                box[part] = w[:, part * LANES:part * LANES + LANES].reshape(CUBE + BLOCK)
            if box is ring.outbox:
                ring.pair(ATT_PARTS).start()

    poll(((2, 2),))
    low = head_halves()
    low_rows = iota((LANES, ONE), 0) < SHARDS
    hidden = iota((PAD, 1), 0) >= TOKENS

    def seq(s, sums):
        rows = pl.ds(pl.multiple_of(s * PAD, PACK), PAD)
        out = []
        for p in SIDES:
            cols = slice(p * LANES, p * LANES + LANES)
            qs, ds = qst.at[p], dst.at[p]
            k_rows, v_rows = k_ref[rows, cols], v_ref[rows, cols]
            stack_heads(qs, q_ref[rows, cols], low)
            stack_heads(ds, do_ref[rows, cols], low)
            scores = jnp.where(hidden, -jnp.inf, nt(k_rows, qs[ALL]))
            top = max_rows(scores)
            e = jnp.exp((scores - top) * 0.125)
            probs = e * (1.0 / sum_rows(e))
            d_probs = nt(v_rows, ds[ALL])
            inner = sum_rows(d_probs * probs)
            d_scores = (probs * (d_probs - inner) * 0.125).astype(BF)
            grad_v = nn(probs.astype(BF), ds[ALL])
            grad_k = nn(d_scores, qs[ALL])
            folded = nn(jnp.transpose(k_rows), d_scores)
            grad_q = jnp.transpose(jnp.where(low_rows, folded[:, :SPAN], folded[:, SPAN:TILE]))[:PAD]
            for third, value in enumerate((grad_q, grad_k, grad_v)):
                rounded = value.astype(BF)
                grads[third, rows, cols] = rounded
                by_core[rows, p * TRIPLE + third * LANES:p * TRIPLE + third * LANES + LANES] = rounded
                out.append(sum_rows(value))
        return tuple(t + n for t, n in zip(sums, out))

    zero = jnp.zeros((ONE, LANES), F32)
    bias_sums = loop(SEQS, seq, (zero,) * 6, unroll=3)
    for p in SIDES:
        for third in range(THIRDS):
            at = pl.multiple_of(third * WIDTH + g * GROUP + p * LANES, LANES)
            biases[:, pl.ds(at, LANES)] = bias_sums[THREE * p + third]
    poll(((2, 3), (1, 1), (0, 0)))
    stage = g + 1

    ring.reopen_box()

    w = nn(turned[ALL], by_core[ALL])
    for part in range(THIRDS):
        both = [w[:, at:at + LANES].reshape(CUBE + BLOCK) for at in (part * LANES, TRIPLE + part * LANES)]
        ring.outbox[part] = jnp.where(rep == 0, both[1], both[0])
        ring.acc[stage % ATT_SLOTS, part] = jnp.where(rep == 0, both[0], both[1])
    ring.pair(THIRDS).start()

    def chunk(i, carry):
        at = pl.ds(pl.multiple_of(i * CHUNK, PACK), CHUNK)
        dh[at, :] += nt(grads[0, at, :], wq_ref[ALL]) + nt(grads[1, at, :], wk_ref[ALL]) + nt(grads[2, at, :], wv_ref[ALL])
        return carry

    loop(ROWS // CHUNK, chunk, 0)

    def exchange(dim, landing, at, number):
        copies = []
        for hops in range(ONE, 4):
            index = list(at)
            index[dim] = (place[dim] + hops) % RING
            copies.append(pltpu.make_async_remote_copy(
                src_ref=blocks.at[tuple(index)], dst_ref=landing.at[hops - 1], send_sem=small_send.at[number + hops],
                recv_sem=small_recv.at[number + hops], device_id=(rep, flat_of(along(place, dim, hops))),
                device_id_type=MESH_ID))
        return copies

    def start(copies):
        for copy in copies:
            copy.start()
        return copies

    def collect(copies, dim, landing, at):
        for copy in copies:
            copy.wait()
        index = list(at)
        index[dim] = place[dim]
        index = tuple(index)
        blocks[index] = blocks[index] + landing[0] + landing[1] + landing[2]

    @pl.when(g == GROUPS - 1)
    def _():
        def tail(*todo):
            for stage, at in todo:
                level(stage, orders, at)

        def fetch(s):
            rows, box = pl.ds(pl.multiple_of(s * PAD, PACK), PAD), s % PAIR
            return (pltpu.make_async_copy(gr_ref.at[rows], gr.at[box], seq_sem.at[0, box]),
                    pltpu.make_async_copy(x_ref.at[s], xs.at[box], seq_sem.at[1, box]))

        def dx_out(s):
            return pltpu.make_async_copy(dxs.at[s % PAIR], dx_ref.at[s], seq_sem.at[2, s % PAIR])

        for copy in fetch(0):
            copy.start()
        gain = vec_ref[:1, :]
        tail((2, 2), (3, 1), (4, 0))
        sums[ALL] = gvin_ref[ALL]
        def norm_one(s, carry):
            @pl.when(s + 1 < SEQS)
            def _():
                for copy in fetch(s + 1):
                    copy.start()

            for copy in fetch(s):
                copy.wait()
            padded(xp, 0, xs, s % PAIR)
            here = pl.ds(pl.multiple_of(s * PAD, PACK), PAD)
            centered, rstd = row_stats(xp[ALL])
            xhat = centered * rstd
            d = dh[here, :]
            dxp[ALL] = (gr[s % PAIR] + norm_back(d * gain, xhat, rstd)).astype(BF)
            for k, value in enumerate((d * xhat, d)):
                sums[k:k + 1, :] += sum_rows(value)

            @pl.when(s >= 2)
            def _():
                dx_out(s - 2).wait()

            dxs[s % PAIR] = dxp[:TOKENS]
            dx_out(s).start()

            @pl.when(s == 3)
            def _():
                tail((2, 3), (3, 2))

            return carry

        loop(SEQS, norm_one, 0)
        for s in (SEQS - 2, SEQS - 1):
            dx_out(s).wait()
        small_blocks(blocks, sums, biases, gbup_ref)
        at = [EVERY] * THREE
        number = 0
        def shard_order():
            for j in range(SUBS):
                turned[:, j * LANES:j * LANES + LANES] = unit_columns(j)
                for b in range(4):
                    for h in SIDES:
                        xp[b * PACK + h * SUBS:b * PACK + h * SUBS + SUBS, j * LANES:j * LANES + LANES] = gup_ref[h, j * RING + b]
            left = xp[:SHARDS]
            total = jnp.zeros_like(left)
            for _ in AXES:
                piece = left.astype(BF)
                total = total + nt(piece, turned[:, :WIDTH])
                left = left - piece.astype(F32)
            for b in range(4):
                up_ref[:, b * WIDTH:b * WIDTH + WIDTH] = total[b * 16:b * PACK + PACK]

        for dim, landing, todo in ((2, from_x, ((4, 1),)), (1, from_y, ((3, 3),)), (0, from_z, ((4, 2),))):
            copies = start(exchange(dim, landing, at, number))
            if dim == 1:
                shard_order()
            tail(*todo)
            collect(copies, dim, landing, at)
            at[dim] = place[dim]
            number += 3
        last = pltpu.make_async_remote_copy(
            src_ref=blocks.at[place], dst_ref=from_pair, send_sem=small_send.at[FIRST], recv_sem=small_recv.at[FIRST],
            device_id=ring.partner, device_id_type=MESH_ID)
        last.start()
        tail((4, 3))
        last.wait()
        small_ref[ALL] = blocks[place] + from_pair[ALL]
        ring.settle(0, ATT_PARTS)
        for stage in range(ONE, ATT_STAGES):
            ring.settle(stage, THIRDS)


def attn_bwd(qkv, do, h, w_qkv, o, da, x, gr, vec, gvin, gbup, gup):
    one = lambda shape: pl.BlockSpec(shape, lambda g: (0,) * len(shape), pipeline_mode=ONCE)
    third = lambda t: pl.BlockSpec((ROWS, GROUP), lambda g: (0, g // PAIR * 6 + t * PAIR + g % PAIR))
    wthird = lambda t: pl.BlockSpec((WIDTH, GROUP), lambda g: (0, t * GROUPS + g))
    col = pl.BlockSpec((ROWS, GROUP), lambda g: (0, g))
    anywhere = ANYWHERE
    shape = jax.ShapeDtypeStruct
    rows = (SUBS, LANES)
    vmem, dma = VM, pltpu.SemaphoreType.DMA
    return pl.pallas_call(
        attn_bwd_kernel, grid=(GROUPS,),
        out_shape=[shape((2, THREE * SUBS) + rows, F32), shape((2, SUBS) + rows, F32), shape((SEQS, TOKENS, WIDTH), BF), shape(rows, F32), shape((PACK, HIDDEN), F32)],
        in_specs=[third(0), third(1), third(2), col, one((ROWS, WIDTH)), wthird(0), wthird(1), wthird(2),
                  one((ROWS, WIDTH)), one((ROWS, WIDTH)), anywhere, anywhere,
                  one((SUBS, WIDTH)), one((SUBS, WIDTH)), one((SUBS, TILE)), one(gup.shape)],
        out_specs=[anywhere, anywhere, anywhere, one(rows), one((PACK, HIDDEN))],
        scratch_shapes=[vmem((ROWS, WIDTH), F32), vmem((THIRDS, ROWS, GROUP), BF), vmem((ROWS, THREE * GROUP), BF),
                        vmem((WIDTH, ROWS), BF), vmem((2, TILE, LANES), BF), vmem((2, TILE, LANES), BF),
                        vmem((PAD, WIDTH), F32), vmem((2, PAD, WIDTH), F32), vmem((2, TOKENS, WIDTH), BF), vmem((2, TOKENS, WIDTH), BF), dma((3, 2)),
                        vmem((PAD, WIDTH), BF), vmem((SUBS, WIDTH), F32), vmem((1, THREE * WIDTH), F32),
                        vmem(CUBE + rows, F32), vmem((3, 4, 4) + rows, F32), vmem((3, 4) + rows, F32),
                        vmem((3,) + rows, F32), vmem(rows, F32), dma((10,)), dma((10,))]
        + ring_scratch(ATT_SLOTS, ATT_STAGES, ATT_PARTS),
        compiler_params=pltpu.CompilerParams(vmem_limit_bytes=VMEM_CAP, collective_id=2, has_side_effects=True),
        name="attn_bwd",
    )(qkv, qkv, qkv, do, h, w_qkv, w_qkv, w_qkv, o, da, x, gr, vec, gvin, gbup, gup)


def last_kernel(z_ref, dx_ref, gq_ref, go_ref, gu_ref, gd_ref, small_ref,
                z_out, dx_out, gq_out, bq_out, go_out, gu_out, bu_out, gd_out, vec_out):
    def untiled(src, dst):
        for r in range(src.shape[0]):
            for c in range(src.shape[ONE]):
                dst[r * SUBS:r * SUBS + SUBS, c * LANES:c * LANES + LANES] = src[r, c]

    z_out[ALL] = z_ref[ALL]
    dx_out[ALL] = dx_ref[ALL]
    untiled(gq_ref, gq_out)

    @pl.when(pl.program_id(0) == 0)
    def _():
        untiled(go_ref, go_out)
        untiled(gd_ref, gd_out)
        gu_out[ALL] = gu_ref[ALL]
        vec_out[ALL] = small_ref[:, :PACK]
        bq_out[ALL] = pltpu.roll(small_ref[ALL], LANES - PACK, 1)[:1, 0:48]
        lane = iota((SUBS, LANES), ONE)
        units = jnp.zeros((ONE, LANES), F32)
        for j in range(SUBS):
            moved = pltpu.roll(small_ref[ALL], (SUBS * j + LANES - SHARDS) % LANES, ONE)
            units = jnp.where(lane[:1] // SUBS == j, moved[j:j + 1], units)
        bu_out[ALL] = units[:, :SHARDS]


def last(z, dx, gw_qkv, gw_out, gw_up, gw_down, small):
    whole = lambda dims: pl.BlockSpec(dims, lambda s: (0,) * len(dims), pipeline_mode=ONCE)
    seq = pl.BlockSpec((2, TOKENS, WIDTH), lambda s: (s, 0, 0))
    share = SUBS
    shape = lambda *dims: jax.ShapeDtypeStruct(dims, F32)
    outs = [shape(PACK, THREE * WIDTH), shape(1, 48), shape(PACK, WIDTH), shape(PACK, HIDDEN), shape(1, SHARDS), shape(SHARDS, WIDTH), shape(SUBS, PACK)]
    return pl.pallas_call(
        last_kernel, grid=(3,),
        out_shape=[jax.ShapeDtypeStruct(z.shape, BF), jax.ShapeDtypeStruct(dx.shape, BF)] + outs,
        in_specs=[seq, seq, pl.BlockSpec((2, share, SUBS, LANES), lambda s: (0, s, 0, 0))]
        + [whole(g.shape) for g in (gw_out, gw_up, gw_down, small)],
        out_specs=[seq, seq, pl.BlockSpec((PACK, share * LANES), lambda s: (0, s))] + [whole(o.shape) for o in outs[1:]],
        name="last",
    )(z, dx, gw_qkv, gw_out, gw_up, gw_down, small)


def layer(x, dz, w_qkv, b_qkv, w_out, w_up, b_up, w_down, vec_params):
    h1, qkv, o, a, h2, dm, vec, b_up, w_qkv, w_out, w_up, w_down = first(
        x, dz, (w_qkv, w_out, w_up, w_down), (b_qkv[None], b_up[None], vec_params))
    w_qkv, w_out, w_up = (w.reshape(WIDTH, -1) for w in (w_qkv, w_out, w_up))
    gw_up, gw_down, gb_up, z, gr, da, do, gvec = mlp(h2, dm, w_up, b_up, w_down, x, dz, a, w_out, vec)
    gw_qkv, gw_out, dx, small, gw_up = attn_bwd(qkv, do, h1, w_qkv, o, da, x, gr, vec, gvec, gb_up, gw_up)
    z, dx, gw_qkv, gb_qkv, gw_out, gw_up, gb_up, gw_down, gvec = last(z, dx, gw_qkv, gw_out, gw_up, gw_down, small)
    return z, dx, gw_qkv, gb_qkv[0], gw_out, gw_up, gb_up[0], gw_down, gvec


def solution(mesh):
    batch = P(("rep", "fsdp"), None, None)
    rows, flat = P("fsdp", None), P("fsdp")
    params = (rows, flat, rows, rows, flat, rows, P(None, "fsdp"))
    return jax.shard_map(layer, mesh=mesh, in_specs=(batch, batch) + params, out_specs=(batch, batch) + params, check_vma=False)
```
